32 devices in a mesh: trial: 4 (over z), lat: 2 (over x), lon: 2 (over core), lev: 2 (over y).
Axes of the slice: x: 2, y: 2, z: 4, core: 2. Of those that a mesh axis runs over, the one named last changes fastest.
Arguments:
- density: float32 [32, 32, 256, 128], P(('trial', 'lat'), 'lon', 'lev'), parts along dimension 0, may hold values from 0.5 to 2
- crowding: float32 [32, 32, 256, 128], P(('trial', 'lat'), 'lon', 'lev'), parts along dimension 0, may hold values from 0.5 to 2
Outputs:
- scaled_field: float32 [32, 32, 256, 128], P(('trial', 'lat'), 'lon', 'lev'), parts along dimension 0
- density_end: float32 [32, 32, 256, 128], P(('trial', 'lat'), 'lon', 'lev'), parts along dimension 0
The draws below stay inside these ranges and needn't reach their ends.
There are 4 independent parts, one for each index of `trial`. The reference program is written for one: setup_inputs(seed, part) draws one part's arguments, and reference() takes and returns one part's arrays. A program takes and returns all parts, laid end to end along the dimension named above; each array names one. Nothing has to cross between parts.
All inputs are finite; a program needn't handle non-finite values.
Results may differ from the reference program's by a relative error of at most 0.000058.
Values sent between devices are 32-bit elements; how exact they have to be, the bound alone decides.
A program may use at most 64 MiB of HBM per device.

```python
import jax
import jax.numpy as jnp
from jax import lax

GRID_Y = 8
GRID_X = 32
GRID_Z = 256
SPECIES = 128
STEPS = 4


def shard_levels(stream_key, extent, cuts, least, largest):
    level, own = 1.0, jax.random.fold_in(stream_key, 6)
    for dim, blocks in cuts:
        draws = jnp.exp(jax.random.uniform(jax.random.fold_in(own, dim), (blocks,), jnp.float32, least / len(cuts), largest / len(cuts)))
        level = level * jnp.repeat(draws, extent[dim] // blocks).reshape([-1 if axis == dim else 1 for axis in range(len(extent))])
    return level


def setup_inputs(seed: int = 0, part: int = 0) -> dict:
    arg_keys = jax.random.split(jax.random.key(seed), 3)
    own_keys = jax.random.split(jax.random.fold_in(arg_keys[2], part), 3)
    density = jnp.clip(0.5 + 1.5 * jax.random.uniform(own_keys[0], (GRID_Y, GRID_X, GRID_Z, SPECIES), jnp.float32) ** shard_levels(own_keys[0], (GRID_Y, GRID_X, GRID_Z, SPECIES), ((0, 2), (1, 2), (2, 2)), -0.2, 0.2), 0.5, 2.0)
    crowding = jnp.clip(0.5 + 1.5 * jax.random.uniform(own_keys[1], (GRID_Y, GRID_X, GRID_Z, SPECIES), jnp.float32) ** shard_levels(own_keys[1], (GRID_Y, GRID_X, GRID_Z, SPECIES), ((0, 2), (1, 2), (2, 2)), -0.2, 0.2), 0.5, 2.0)
    return dict(density=density, crowding=crowding)


def inner_cells(values, dims):
    for dim in dims:
        values = lax.slice_in_dim(values, 1, values.shape[dim] - 1, axis=dim)
    return values

def side_cells(values, dim, start, dims):
    others = [other for other in dims if other != dim]
    values = inner_cells(values, others)
    return lax.slice_in_dim(values, start, start + values.shape[dim] - 2, axis=dim)

def advance(padded, crowding):
    middle = inner_cells(padded, (0, 1, 2))
    lower = [side_cells(padded, dim, 0, (0, 1, 2)) for dim in (0, 1, 2)]
    upper = [side_cells(padded, dim, 2, (0, 1, 2)) for dim in (0, 1, 2)]
    spread = lower[0] + upper[0] + lower[1] + upper[1] + lower[2] + upper[2] - 6.0 * middle
    return middle + 0.1 * spread + 0.2 * middle * (1.0 - middle * crowding)

def reference(density, crowding):
    for step in range(STEPS):
        density = advance(jnp.pad(density, ((1, 1), (1, 1), (1, 1), (0, 0)), mode='constant'), crowding)
    line_mean = lax.optimization_barrier(jnp.mean(density, axis=1, keepdims=True))
    centred = density - line_mean
    line_variance = lax.optimization_barrier(jnp.mean(centred * centred, axis=1, keepdims=True))
    scaled_field = centred * lax.rsqrt(line_variance + 0.0001)
    return (scaled_field, density)
```

```python
import functools

import jax
import jax.numpy as jnp
from jax import lax
from jax.experimental import pallas as pl
from jax.experimental.pallas import tpu as pltpu
from jax.sharding import PartitionSpec as P

STEPS = 4
PAD = 8
MESH = pl.DeviceIdType.MESH


def with_halo(cells, sides, width):
    for axis, dim in sides:
        count = lax.axis_size(axis)
        ends = count - 1
        head = lax.slice_in_dim(cells, 0, width, axis=dim)
        tail = lax.slice_in_dim(cells, cells.shape[dim] - width, cells.shape[dim], axis=dim)
        cells = jnp.concatenate(
            [
                lax.ppermute(tail, axis, [(i, (i + 1) % count) for i in range(ends)]),
                cells,
                lax.ppermute(head, axis, [((i + 1) % count, i) for i in range(ends)]),
            ],
            axis=dim,
        )
    return cells


def inner_cells(values, dims):
    for dim in dims:
        values = lax.slice_in_dim(values, 1, values.shape[dim] - 1, axis=dim)
    return values


def side_cells(values, dim, start, dims):
    others = [other for other in dims if other != dim]
    values = inner_cells(values, others)
    return lax.slice_in_dim(values, start, start + values.shape[dim] - 2, axis=dim)


def advance(padded, crowding):
    middle = inner_cells(padded, (0, 1, 2))
    lower = [side_cells(padded, dim, 0, (0, 1, 2)) for dim in (0, 1, 2)]
    upper = [side_cells(padded, dim, 2, (0, 1, 2)) for dim in (0, 1, 2)]
    spread = lower[0] + upper[0] + lower[1] + upper[1] + lower[2] + upper[2] - 6.0 * middle
    return middle + 0.1 * spread + 0.2 * middle * (1.0 - middle * crowding)


def general(density, crowding):
    for step in range(STEPS):
        padded = with_halo(density, (("lat", 0), ("lon", 1), ("lev", 2)), 1)
        density = advance(padded, crowding)
    count = density.shape[1] * lax.axis_size("lon")
    moved = density - 1.0
    totals, squares = lax.psum(
        (jnp.sum(moved, axis=1, keepdims=True), jnp.sum(moved * moved, axis=1, keepdims=True)),
        "lon",
    )
    line_mean = 1.0 + totals / count
    centred = density - line_mean
    line_variance = squares / count - totals / count * (totals / count)
    return (centred * lax.rsqrt(line_variance + 0.0001), density)


def tree_sum(terms):
    terms = list(terms)
    while len(terms) > 1:
        terms = [sum(terms[i : i + 2][1:], terms[i]) for i in range(0, len(terms), 2)]
    return terms[0]


def signal(sem, where):
    pl.semaphore_signal(sem, inc=1, device_id=where, device_id_type=MESH)


def split(deep):
    half, first = deep // 2, max(8, deep // 32 * 8)
    coarse = [(0, half), (half, half)]
    fine = [(0, first), (first, half - first), (half, half - 8), (deep - 8, 8)]
    return coarse, fine


def place(r, rows):
    lat = lax.axis_index("lat")
    return (1 - lat) * (rows - r) + lat * (r - 1)


def tiles(first, many, act):
    def tile(i, _):
        act(pl.multiple_of(i * 8, 8))
        return 0
    lax.fori_loop(first // 8, (first + many) // 8, tile, 0)


def line_sums(values):
    cols = len(values)
    total = tree_sum(values)
    mean = total * (1.0 / cols)
    return total, tree_sum([(v - mean) * (v - mean) for v in values])


def line_scale(pair, cols):
    count = cols * len(pair)
    mean = tree_sum([p[0] for p in pair]) * (1.0 / count)
    square = tree_sum([p[1] + cols * (p[0] * (1.0 / cols) - mean) ** 2 for p in pair])
    return mean, lax.rsqrt(square * (1.0 / count) + 0.0001)


def kernel(lons, levs, dens, crowd, out_scaled, out_dens, edge, front,
           field, cap, stats, peers, load_sem, edge_sem, face_send, face_recv,
           lon_send, lon_recv, lev_send, lev_recv, stat_send, stat_recv):
    rows, cols, deep, lanes = dens.shape
    coarse, fine = split(deep)
    lat, lon, lev = lax.axis_index("lat"), lax.axis_index("lon"), lax.axis_index("lev")
    has_left, has_right = lon > 0, lon < lons - 1
    has_down, has_up = lev > 0, lev < levs - 1
    late = lax.rem(lon, 2) == 1

    first = [
        pltpu.make_async_copy(
            dens.at[place(1, rows), :, pl.ds(at, span)],
            field.at[0, 1, pl.ds(1, cols), pl.ds(PAD + at, span)],
            edge_sem.at[k])
        for k, (at, span) in enumerate(coarse)
    ]
    loads = []
    for r in range(1, rows + 1):
        if r > 1:
            loads.append(pltpu.make_async_copy(
                dens.at[place(r, rows)],
                field.at[0, r, pl.ds(1, cols), pl.ds(PAD, deep)],
                load_sem.at[0, r - 1]))
        loads.append(pltpu.make_async_copy(
            crowd.at[place(r, rows)], cap.at[r - 1], load_sem.at[1, r - 1]))

    barrier = pltpu.get_barrier_semaphore()
    signal(barrier, {"lat": 1 - lat})
    for j in range(1, lons):
        signal(barrier, {"lon": lax.rem(lon + j, lons)})
    if levs > 1:
        pl.when(has_down)(lambda: signal(barrier, {"lev": lev - 1}))
        pl.when(has_up)(lambda: signal(barrier, {"lev": lev + 1}))
    for copy in first + loads:
        copy.start()
    pl.semaphore_wait(barrier, lons + has_down.astype(jnp.int32) + has_up.astype(jnp.int32))

    def chunks(t):
        return fine if t == STEPS - 1 else coarse

    def face(t, k):
        at, span = chunks(t)[k]
        return pltpu.make_async_remote_copy(
            src_ref=field.at[t, 1, pl.ds(1, cols), pl.ds(PAD + at, span)],
            dst_ref=field.at[t, 0, pl.ds(1, cols), pl.ds(PAD + at, span)],
            send_sem=face_send.at[t, k],
            recv_sem=face_recv.at[t, k],
            device_id={"lat": 1 - lat},
            device_id_type=MESH,
        )

    def lon_side(t, right):
        own, theirs = (cols, 0) if right else (1, cols + 1)
        span = pl.ds(1, rows)
        return pltpu.make_async_remote_copy(
            src_ref=field.at[t, span, own, pl.ds(PAD, deep)],
            dst_ref=field.at[t, span, theirs, pl.ds(PAD, deep)],
            send_sem=lon_send.at[t, int(right)],
            recv_sem=lon_recv.at[t, int(right)],
            device_id={"lon": lon + 1 if right else lon - 1},
            device_id_type=MESH,
        )

    def lev_side(t, up):
        own, theirs = (PAD + deep - 1, PAD - 1) if up else (PAD, PAD + deep)
        span = (pl.ds(1, rows), pl.ds(1, cols))
        return pltpu.make_async_remote_copy(
            src_ref=field.at[t, span[0], span[1], pl.ds(own, 1)],
            dst_ref=field.at[t, span[0], span[1], pl.ds(theirs, 1)],
            send_sem=lev_send.at[t, int(up)],
            recv_sem=lev_recv.at[t, int(up)],
            device_id={"lev": lev + 1 if up else lev - 1},
            device_id_type=MESH,
        )

    def sides(t, act):
        if lons > 1:
            pl.when(has_right)(lambda: act(lon_side(t, True), 1))
            pl.when(has_left)(lambda: act(lon_side(t, False), 0))
        if levs > 1:
            pl.when(has_up)(lambda: act(lev_side(t, True), 1))
            pl.when(has_down)(lambda: act(lev_side(t, False), 0))

    def start_sides(t):
        sides(t, lambda copy, _: copy.start())

    def wait_sides_sent(t):
        sides(t, lambda copy, _: copy.wait_send())

    def wait_sides(t):
        if lons > 1:
            pl.when(has_left)(lambda: lon_side(t, True).wait_recv())
            pl.when(has_right)(lambda: lon_side(t, False).wait_recv())
        if levs > 1:
            pl.when(has_down)(lambda: lev_side(t, True).wait_recv())
            pl.when(has_up)(lambda: lev_side(t, False).wait_recv())

    def stat(j):
        return pltpu.make_async_remote_copy(
            src_ref=stats,
            dst_ref=peers.at[j - 1],
            send_sem=stat_send.at[j - 1],
            recv_sem=stat_recv.at[j - 1],
            device_id={"lon": lax.rem(lon + j, lons)},
            device_id_type=MESH,
        )

    for k in range(len(coarse)):
        first[k].wait()
        face(0, k).start()

    def clear_cols(at):
        for t in range(STEPS):
            def row(i, _, t=t):
                field[t, i, at, pl.ds(PAD, deep)] = jnp.zeros((deep, lanes), jnp.float32)
                return 0
            lax.fori_loop(1, rows + 1, row, 0)

    def clear_level(at):
        for t in range(STEPS):
            def row(i, _, t=t):
                def col(c, _):
                    field[t, i, c, pl.ds(at, PAD)] = jnp.zeros((PAD, lanes), jnp.float32)
                    return 0
                return lax.fori_loop(1, cols + 1, col, 0)
            lax.fori_loop(1, rows + 1, row, 0)

    pl.when(jnp.logical_not(has_left))(lambda: clear_cols(0))
    pl.when(jnp.logical_not(has_right))(lambda: clear_cols(cols + 1))
    pl.when(jnp.logical_not(has_down))(lambda: clear_level(0))
    pl.when(jnp.logical_not(has_up))(lambda: clear_level(PAD + deep))

    for copy in loads:
        copy.wait()
    start_sides(0)

    def cell(t, r, c, at, span, below, above):
        here = field[t, r, c, pl.ds(PAD + at, span)]
        near = (field[t, r, c - 1, pl.ds(PAD + at, span)] + field[t, r, c + 1, pl.ds(PAD + at, span)])
        near += (field[t, r, c, pl.ds(PAD - 1 + at, span)] + field[t, r, c, pl.ds(PAD + 1 + at, span)])
        if below:
            near += field[t, r - 1, c, pl.ds(PAD + at, span)]
        if above:
            near += field[t, r + 1, c, pl.ds(PAD + at, span)]
        limit = cap[r - 1, c - 1, pl.ds(at, span)]
        return here * (0.6 - 0.2 * (here * limit)) + 0.1 * near

    def advance_row(t, r, at, span, last):
        def col(c, _):
            value = cell(t, r, c, at, span, True, not last)
            field[t + 1, r, c, pl.ds(PAD + at, span)] = value
            if t == STEPS - 2 and isinstance(r, int) and r == 1:
                front[c - 1, pl.ds(at, span)] = value
            return 0
        lax.fori_loop(1, cols + 1, col, 0)

    def start_face(t, k):
        if t == STEPS - 1 and k == len(fine) - 1:
            return
        if t == STEPS - 1 and k > 0:
            pl.when(late)(lambda: face(t, k).start())
        else:
            face(t, k).start()

    for t in range(STEPS - 1):
        wait_sides(t)

        def inner(r, _, t=t):
            advance_row(t, r, 0, deep, False)
            return 0

        lax.fori_loop(2, rows, inner, 0)
        advance_row(t, rows, 0, deep, True)
        for k in range(len(coarse)):
            face(t, k).wait_recv()
            advance_row(t, 1, *coarse[k], False)
            for j, (at, _) in enumerate(chunks(t + 1)):
                if coarse[k][0] <= at < sum(coarse[k]):
                    start_face(t + 1, j)
        start_sides(t + 1)

    t = STEPS - 1
    wait_sides(t)

    def finish(r, at, last):
        values = [cell(t, r, c, at, 8, True, not last) for c in range(1, cols + 1)]
        for c in range(cols):
            out_dens[r - 2, c, pl.ds(at, 8)] = values[c]
        total, square = line_sums(values)
        stats[r - 2, 0, pl.ds(at, 8)] = total
        stats[r - 2, 1, pl.ds(at, 8)] = square

    def scale(r, at):
        pair = [(stats[r - 2, 0, pl.ds(at, 8)], stats[r - 2, 1, pl.ds(at, 8)])]
        for j in range(lons - 1):
            pair.append((peers[j, r - 2, 0, pl.ds(at, 8)], peers[j, r - 2, 1, pl.ds(at, 8)]))
        mean, gain = line_scale(pair, cols)
        for c in range(cols):
            out_scaled[r - 2, c, pl.ds(at, 8)] = (out_dens[r - 2, c, pl.ds(at, 8)] - mean) * gain

    def each_inner(act):
        def row(r, _):
            tiles(0, deep, lambda at: act(r, at))
            return 0
        lax.fori_loop(2, rows, row, 0)

    each_inner(lambda r, at: finish(r, at, False))
    tiles(0, deep, lambda at: finish(rows, at, True))
    for j in range(1, lons):
        stat(j).start()

    def base(c, _):
        edge[c - 1] = cell(t, 1, c, 0, deep, False, True)
        return 0

    lax.fori_loop(1, cols + 1, base, 0)
    for j in range(1, lons):
        stat(j).wait_recv()
    each_inner(scale)
    tiles(0, deep, lambda at: scale(rows, at))

    def add_face(k):
        at, span = fine[k]
        face(t, k).wait_recv()

        def col(c, _):
            edge[c, pl.ds(at, span)] += 0.1 * field[t, 0, c + 1, pl.ds(PAD + at, span)]
            return 0
        lax.fori_loop(0, cols, col, 0)

    for s in range(STEPS - 1):
        for k in range(len(coarse)):
            face(s, k).wait_send()
    for s in range(STEPS):
        wait_sides_sent(s)
    for j in range(1, lons):
        stat(j).wait_send()
    add_face(0)
    face(t, 0).wait_send()

    @pl.when(late)
    def _():
        for k in range(1, len(fine) - 1):
            add_face(k)
        for k in range(1, len(fine) - 1):
            face(t, k).wait_send()


def write_inner(scaled, dens, out_scaled, out_dens, token, sems):
    inner, cols, _, _ = scaled.shape
    copies = []
    for i, (src, dst) in enumerate(((scaled, out_scaled), (dens, out_dens))):
        for r in range(inner):
            copies.append(pltpu.make_async_copy(
                src.at[r], dst.at[place(r + 2, inner + 1)], sems.at[i, r]))
    for copy in copies:
        copy.start()
    token[...] = jnp.zeros(token.shape, jnp.float32)
    for copy in copies:
        copy.wait()


def last_row(lons, edge, front, token, out_scaled, out_dens, other, stats, peers,
             entered, face_send, face_recv, stat_send, stat_recv):
    cols, deep, lanes = edge.shape
    _, fine = split(deep)
    end = len(fine) - 1
    lat, lon = lax.axis_index("lat"), lax.axis_index("lon")
    late = lax.rem(lon, 2)
    early = 1 - late
    order = late * lons + lon

    barrier = pltpu.get_barrier_semaphore()
    signal(barrier, {"lat": 1 - lat})
    before = 0
    for j in range(1, lons):
        there = lax.rem(lon + j, lons)
        ahead = lax.rem(there, 2) * lons + there < order
        before += ahead.astype(jnp.int32)
        pl.when(jnp.logical_not(ahead))(lambda: signal(barrier, {"lon": there}))
    pl.semaphore_wait(barrier, 1 + before)

    def face(k):
        at, span = fine[k]
        return pltpu.make_async_remote_copy(
            src_ref=front.at[:, pl.ds(at, span)],
            dst_ref=other.at[:, pl.ds(at, span)],
            send_sem=face_send.at[k],
            recv_sem=face_recv.at[k],
            device_id={"lat": 1 - lat},
            device_id_type=MESH,
        )

    def stat(part, j):
        pick = (slice(None), pl.ds(deep - 8, 8) if part else pl.ds(0, deep - 8))
        return pltpu.make_async_remote_copy(
            src_ref=stats.at[pick],
            dst_ref=peers.at[(j - 1,) + pick],
            send_sem=stat_send.at[part, j - 1],
            recv_sem=stat_recv.at[part, j - 1],
            device_id={"lon": lax.rem(lon + j, lons)},
            device_id_type=MESH,
        )

    for k in range(1, end):
        pl.when(early == 1)(lambda: face(k).start())
    face(end).start()
    for j in range(1, lons):
        there = lax.rem(lon + j, lons)
        ahead = lax.rem(there, 2) * lons + there < order
        pl.when(ahead)(lambda: signal(entered, {"lon": there}))

    def finish(at, add):
        values = [edge[c, pl.ds(at, 8)] for c in range(cols)]
        if add:
            values = [v + 0.1 * other[c, pl.ds(at, 8)] for c, v in enumerate(values)]
        for c in range(cols):
            out_dens[c, pl.ds(at, 8)] = values[c]
        total, square = line_sums(values)
        stats[0, pl.ds(at, 8)] = total
        stats[1, pl.ds(at, 8)] = square

    def scale(at):
        pair = [(stats[0, pl.ds(at, 8)], stats[1, pl.ds(at, 8)])]
        for j in range(lons - 1):
            pair.append((peers[j, 0, pl.ds(at, 8)], peers[j, 1, pl.ds(at, 8)]))
        mean, gain = line_scale(pair, cols)
        for c in range(cols):
            out_scaled[c, pl.ds(at, 8)] = (out_dens[c, pl.ds(at, 8)] - mean) * gain

    tiles(*fine[0], lambda at: finish(at, False))

    @pl.when(early == 0)
    def _():
        for k in range(1, end):
            tiles(*fine[k], lambda at: finish(at, False))

    @pl.when(early == 1)
    def _():
        for k in range(1, end):
            face(k).wait_recv()
            tiles(*fine[k], lambda at: finish(at, True))

    pl.when(before < lons - 1)(lambda: pl.semaphore_wait(entered, lons - 1 - before))
    for j in range(1, lons):
        stat(0, j).start()
    face(end).wait_recv()
    tiles(*fine[end], lambda at: finish(at, True))
    for j in range(1, lons):
        stat(1, j).start()
    for j in range(1, lons):
        stat(0, j).wait_recv()
    tiles(0, deep - 8, scale)
    for k in range(1, end):
        pl.when(early == 1)(lambda: face(k).wait_send())
    face(end).wait_send()
    for j in range(1, lons):
        stat(1, j).wait_recv()
    tiles(*fine[end], scale)
    for part in range(2):
        for j in range(1, lons):
            stat(part, j).wait_send()


def write_last(scaled, dens, in_scaled, in_dens, out_scaled, out_dens, sems):
    del in_scaled, in_dens
    rows, many = out_dens.shape[0], sems.shape[1]
    step = dens.shape[0] // many
    copies = []
    for i, (src, dst) in enumerate(((scaled, out_scaled), (dens, out_dens))):
        for part in range(many):
            span = pl.ds(part * step, step)
            copies.append(pltpu.make_async_copy(
                src.at[span], dst.at[place(1, rows), span], sems.at[i, part]))
    for copy in copies:
        copy.start()
    for copy in copies:
        copy.wait()


def in_vmem(*arrays):
    return [pltpu.with_memory_space_constraint(a, pltpu.VMEM) for a in arrays]


def all_steps(lons, levs, density, crowding):
    rows, cols, deep, lanes = density.shape
    coarse, fine = split(deep)
    sem = pltpu.SemaphoreType.DMA
    peers = max(lons - 1, 1)
    inner = pltpu.VMEM((rows - 1, cols, deep, lanes), jnp.float32)
    row = pltpu.VMEM((cols, deep, lanes), jnp.float32)
    any_space = pl.BlockSpec(memory_space=pl.ANY)
    vmem = pl.BlockSpec(memory_space=pltpu.VMEM)
    scaled, dens, edge, front = pl.pallas_call(
        functools.partial(kernel, lons, levs),
        out_shape=(inner, inner, row, row),
        in_specs=[any_space] * 2,
        out_specs=[vmem] * 4,
        scratch_shapes=[
            pltpu.VMEM((STEPS, rows + 1, cols + 2, deep + 2 * PAD, lanes), jnp.float32),
            pltpu.VMEM((rows, cols, deep, lanes), jnp.float32),
            pltpu.VMEM((rows - 1, 2, deep, lanes), jnp.float32),
            pltpu.VMEM((peers, rows - 1, 2, deep, lanes), jnp.float32),
            sem((2, rows)),
            sem((len(coarse),)),
            sem((STEPS, len(fine))),
            sem((STEPS, len(fine))),
            sem((STEPS, 2)),
            sem((STEPS, 2)),
            sem((STEPS, 2)),
            sem((STEPS, 2)),
            sem((peers,)),
            sem((peers,)),
        ],
        compiler_params=pltpu.CompilerParams(
            collective_id=0, has_side_effects=True, vmem_limit_bytes=VMEM_LIMIT
        ),
    )(density, crowding)

    out = jax.ShapeDtypeStruct(density.shape, density.dtype)
    out_scaled, out_dens, token = pl.pallas_call(
        write_inner,
        out_shape=(out, out, pltpu.VMEM((8, lanes), jnp.float32)),
        in_specs=[vmem] * 2,
        out_specs=[pl.BlockSpec(memory_space=pltpu.HBM)] * 2 + [vmem],
        scratch_shapes=[sem((2, rows - 1))],
        compiler_params=pltpu.CompilerParams(vmem_limit_bytes=2**20),
    )(*in_vmem(scaled, dens))

    row_scaled, row_dens = pl.pallas_call(
        functools.partial(last_row, lons),
        out_shape=(row, row),
        in_specs=[vmem] * 3,
        out_specs=[vmem] * 2,
        scratch_shapes=[
            pltpu.VMEM((cols, deep, lanes), jnp.float32),
            pltpu.VMEM((2, deep, lanes), jnp.float32),
            pltpu.VMEM((peers, 2, deep, lanes), jnp.float32),
            pltpu.SemaphoreType.REGULAR,
            sem((len(fine),)),
            sem((len(fine),)),
            sem((2, peers)),
            sem((2, peers)),
        ],
        compiler_params=pltpu.CompilerParams(
            collective_id=1, has_side_effects=True, vmem_limit_bytes=8 * 2**20
        ),
    )(*in_vmem(edge, front, token))

    hbm = pl.BlockSpec(memory_space=pltpu.HBM)
    return pl.pallas_call(
        write_last,
        out_shape=(out, out),
        in_specs=[vmem] * 2 + [hbm] * 2,
        out_specs=[hbm] * 2,
        input_output_aliases={2: 0, 3: 1},
        scratch_shapes=[sem((2, 4 if cols % 4 == 0 else 1))],
        compiler_params=pltpu.CompilerParams(vmem_limit_bytes=2**20),
    )(*in_vmem(row_scaled, row_dens), out_scaled, out_dens)


VMEM_LIMIT = 44 * 2**20


def solution(mesh):
    lats, lons, levs = mesh.shape["lat"], mesh.shape["lon"], mesh.shape["lev"]

    def shards(density, crowding):
        rows, cols, deep, lanes = density.shape
        words = lanes * (
            STEPS * (rows + 1) * (cols + 2) * (deep + 2 * PAD)
            + 3 * rows * cols * deep
            + 2 * lons * rows * deep
        )
        fits = lats == 2 and rows > 1 and lanes == 128 and deep % 32 == 0 and 4 * words < VMEM_LIMIT
        if fits:
            return tuple(all_steps(lons, levs, density, crowding))
        return general(density, crowding)

    spec = P(("trial", "lat"), "lon", "lev", None)
    return jax.shard_map(
        shards, mesh=mesh, in_specs=(spec, spec), out_specs=(spec, spec), check_vma=False
    )
```

```python
import functools

import jax
import jax.numpy as jnp
from jax import lax
from jax.experimental import pallas as pl
from jax.experimental.pallas import tpu as pltpu
from jax.sharding import PartitionSpec as P

STEPS = 4
PAD = 8
MESH = pl.DeviceIdType.MESH


def with_halo(cells, sides, width):
    for axis, dim in sides:
        count = lax.axis_size(axis)
        ends = count - 1
        head = lax.slice_in_dim(cells, 0, width, axis=dim)
        tail = lax.slice_in_dim(cells, cells.shape[dim] - width, cells.shape[dim], axis=dim)
        cells = jnp.concatenate(
            [
                lax.ppermute(tail, axis, [(i, (i + 1) % count) for i in range(ends)]),
                cells,
                lax.ppermute(head, axis, [((i + 1) % count, i) for i in range(ends)]),
            ],
            axis=dim,
        )
    return cells


def inner_cells(values, dims):
    for dim in dims:
        values = lax.slice_in_dim(values, 1, values.shape[dim] - 1, axis=dim)
    return values


def side_cells(values, dim, start, dims):
    others = [other for other in dims if other != dim]
    values = inner_cells(values, others)
    return lax.slice_in_dim(values, start, start + values.shape[dim] - 2, axis=dim)


def advance(padded, crowding):
    middle = inner_cells(padded, (0, 1, 2))
    lower = [side_cells(padded, dim, 0, (0, 1, 2)) for dim in (0, 1, 2)]
    upper = [side_cells(padded, dim, 2, (0, 1, 2)) for dim in (0, 1, 2)]
    spread = lower[0] + upper[0] + lower[1] + upper[1] + lower[2] + upper[2] - 6.0 * middle
    return middle + 0.1 * spread + 0.2 * middle * (1.0 - middle * crowding)


def general(density, crowding):
    for step in range(STEPS):
        padded = with_halo(density, (("lat", 0), ("lon", 1), ("lev", 2)), 1)
        density = advance(padded, crowding)
    count = density.shape[1] * lax.axis_size("lon")
    moved = density - 1.0
    totals, squares = lax.psum(
        (jnp.sum(moved, axis=1, keepdims=True), jnp.sum(moved * moved, axis=1, keepdims=True)),
        "lon",
    )
    line_mean = 1.0 + totals / count
    centred = density - line_mean
    line_variance = squares / count - totals / count * (totals / count)
    return (centred * lax.rsqrt(line_variance + 0.0001), density)


def tree_sum(terms):
    terms = list(terms)
    while len(terms) > 1:
        terms = [sum(terms[i : i + 2][1:], terms[i]) for i in range(0, len(terms), 2)]
    return terms[0]


def signal(sem, where):
    pl.semaphore_signal(sem, inc=1, device_id=where, device_id_type=MESH)


def split(deep):
    half, first, late = deep // 2, max(8, 3 * deep // 64 * 8), max(8, 3 * deep // 128 * 8)
    coarse = [(0, half), (half, half)]
    fine = [(0, first), (first, deep - 8 - late - first), (deep - 8 - late, late), (deep - 8, 8)]
    return coarse, fine


def place(r, rows):
    lat = lax.axis_index("lat")
    return (1 - lat) * (rows - r) + lat * (r - 1)


def tiles(first, many, act):
    def tile(i, _):
        act(pl.multiple_of(i * 8, 8))
        return 0
    lax.fori_loop(first // 8, (first + many) // 8, tile, 0)


def line_sums(values):
    cols = len(values)
    total = tree_sum(values)
    mean = total * (1.0 / cols)
    return total, tree_sum([(v - mean) * (v - mean) for v in values])


def line_scale(pair, cols):
    count = cols * len(pair)
    mean = tree_sum([p[0] for p in pair]) * (1.0 / count)
    square = tree_sum([p[1] + cols * (p[0] * (1.0 / cols) - mean) ** 2 for p in pair])
    return mean, lax.rsqrt(square * (1.0 / count) + 0.0001)


def kernel(lons, levs, dens, crowd, out_scaled, out_dens, edge, front,
           field, cap, stats, peers, load_sem, edge_sem, face_send, face_recv,
           lon_send, lon_recv, lev_send, lev_recv, stat_send, stat_recv):
    rows, cols, deep, lanes = dens.shape
    coarse, fine = split(deep)
    lat, lon, lev = lax.axis_index("lat"), lax.axis_index("lon"), lax.axis_index("lev")
    has_left, has_right = lon > 0, lon < lons - 1
    has_down, has_up = lev > 0, lev < levs - 1
    late = lax.rem(lon, 2) == 1

    first = [
        pltpu.make_async_copy(
            dens.at[place(1, rows), :, pl.ds(at, span)],
            field.at[0, 1, pl.ds(1, cols), pl.ds(PAD + at, span)],
            edge_sem.at[k])
        for k, (at, span) in enumerate(coarse)
    ]
    loads = []
    for r in range(1, rows + 1):
        if r > 1:
            loads.append(pltpu.make_async_copy(
                dens.at[place(r, rows)],
                field.at[0, r, pl.ds(1, cols), pl.ds(PAD, deep)],
                load_sem.at[0, r - 1]))
        loads.append(pltpu.make_async_copy(
            crowd.at[place(r, rows)], cap.at[r - 1], load_sem.at[1, r - 1]))

    barrier = pltpu.get_barrier_semaphore()
    signal(barrier, {"lat": 1 - lat})
    for j in range(1, lons):
        signal(barrier, {"lon": lax.rem(lon + j, lons)})
    if levs > 1:
        pl.when(has_down)(lambda: signal(barrier, {"lev": lev - 1}))
        pl.when(has_up)(lambda: signal(barrier, {"lev": lev + 1}))
    for copy in first + loads:
        copy.start()
    pl.semaphore_wait(barrier, lons + has_down.astype(jnp.int32) + has_up.astype(jnp.int32))

    def chunks(t):
        return fine if t == STEPS - 1 else coarse

    def face(t, k):
        at, span = chunks(t)[k]
        return pltpu.make_async_remote_copy(
            src_ref=field.at[t, 1, pl.ds(1, cols), pl.ds(PAD + at, span)],
            dst_ref=field.at[t, 0, pl.ds(1, cols), pl.ds(PAD + at, span)],
            send_sem=face_send.at[t, k],
            recv_sem=face_recv.at[t, k],
            device_id={"lat": 1 - lat},
            device_id_type=MESH,
        )

    def lon_side(t, right):
        own, theirs = (cols, 0) if right else (1, cols + 1)
        span = pl.ds(1, rows)
        return pltpu.make_async_remote_copy(
            src_ref=field.at[t, span, own, pl.ds(PAD, deep)],
            dst_ref=field.at[t, span, theirs, pl.ds(PAD, deep)],
            send_sem=lon_send.at[t, int(right)],
            recv_sem=lon_recv.at[t, int(right)],
            device_id={"lon": lon + 1 if right else lon - 1},
            device_id_type=MESH,
        )

    def lev_side(t, up):
        own, theirs = (PAD + deep - 1, PAD - 1) if up else (PAD, PAD + deep)
        span = (pl.ds(1, rows), pl.ds(1, cols))
        return pltpu.make_async_remote_copy(
            src_ref=field.at[t, span[0], span[1], pl.ds(own, 1)],
            dst_ref=field.at[t, span[0], span[1], pl.ds(theirs, 1)],
            send_sem=lev_send.at[t, int(up)],
            recv_sem=lev_recv.at[t, int(up)],
            device_id={"lev": lev + 1 if up else lev - 1},
            device_id_type=MESH,
        )

    def sides(t, act):
        if lons > 1:
            pl.when(has_right)(lambda: act(lon_side(t, True), 1))
            pl.when(has_left)(lambda: act(lon_side(t, False), 0))
        if levs > 1:
            pl.when(has_up)(lambda: act(lev_side(t, True), 1))
            pl.when(has_down)(lambda: act(lev_side(t, False), 0))

    def start_sides(t):
        sides(t, lambda copy, _: copy.start())

    def wait_sides_sent(t):
        sides(t, lambda copy, _: copy.wait_send())

    def wait_sides(t):
        if lons > 1:
            pl.when(has_left)(lambda: lon_side(t, True).wait_recv())
            pl.when(has_right)(lambda: lon_side(t, False).wait_recv())
        if levs > 1:
            pl.when(has_down)(lambda: lev_side(t, True).wait_recv())
            pl.when(has_up)(lambda: lev_side(t, False).wait_recv())

    def stat(j):
        return pltpu.make_async_remote_copy(
            src_ref=stats,
            dst_ref=peers.at[j - 1],
            send_sem=stat_send.at[j - 1],
            recv_sem=stat_recv.at[j - 1],
            device_id={"lon": lax.rem(lon + j, lons)},
            device_id_type=MESH,
        )

    for k in range(len(coarse)):
        first[k].wait()
        face(0, k).start()

    def clear_cols(at):
        for t in range(STEPS):
            def row(i, _, t=t):
                field[t, i, at, pl.ds(PAD, deep)] = jnp.zeros((deep, lanes), jnp.float32)
                return 0
            lax.fori_loop(1, rows + 1, row, 0)

    def clear_level(at):
        for t in range(STEPS):
            def row(i, _, t=t):
                def col(c, _):
                    field[t, i, c, pl.ds(at, PAD)] = jnp.zeros((PAD, lanes), jnp.float32)
                    return 0
                return lax.fori_loop(1, cols + 1, col, 0)
            lax.fori_loop(1, rows + 1, row, 0)

    pl.when(jnp.logical_not(has_left))(lambda: clear_cols(0))
    pl.when(jnp.logical_not(has_right))(lambda: clear_cols(cols + 1))
    pl.when(jnp.logical_not(has_down))(lambda: clear_level(0))
    pl.when(jnp.logical_not(has_up))(lambda: clear_level(PAD + deep))

    for copy in loads:
        copy.wait()
    start_sides(0)

    def cell(t, r, c, at, span, below, above):
        here = field[t, r, c, pl.ds(PAD + at, span)]
        near = (field[t, r, c - 1, pl.ds(PAD + at, span)] + field[t, r, c + 1, pl.ds(PAD + at, span)])
        near += (field[t, r, c, pl.ds(PAD - 1 + at, span)] + field[t, r, c, pl.ds(PAD + 1 + at, span)])
        if below:
            near += field[t, r - 1, c, pl.ds(PAD + at, span)]
        if above:
            near += field[t, r + 1, c, pl.ds(PAD + at, span)]
        limit = cap[r - 1, c - 1, pl.ds(at, span)]
        return here * (0.6 - 0.2 * (here * limit)) + 0.1 * near

    def advance_row(t, r, at, span, last):
        def col(c, _):
            value = cell(t, r, c, at, span, True, not last)
            field[t + 1, r, c, pl.ds(PAD + at, span)] = value
            if t == STEPS - 2 and isinstance(r, int) and r == 1:
                front[c - 1, pl.ds(at, span)] = value
            return 0
        lax.fori_loop(1, cols + 1, col, 0)

    def start_face(t, k):
        if t == STEPS - 1 and k == len(fine) - 1:
            return
        if t == STEPS - 1 and k > 0:
            pl.when(late)(lambda: face(t, k).start())
        else:
            face(t, k).start()

    for t in range(STEPS - 1):
        wait_sides(t)

        def inner(r, _, t=t):
            advance_row(t, r, 0, deep, False)
            return 0

        lax.fori_loop(2, rows, inner, 0)
        advance_row(t, rows, 0, deep, True)
        for k in range(len(coarse)):
            face(t, k).wait_recv()
            advance_row(t, 1, *coarse[k], False)
            for j, chunk in enumerate(chunks(t + 1)):
                if coarse[k][0] < sum(chunk) <= sum(coarse[k]):
                    start_face(t + 1, j)
        start_sides(t + 1)

    t = STEPS - 1
    wait_sides(t)

    def finish(r, at, last):
        values = [cell(t, r, c, at, 8, True, not last) for c in range(1, cols + 1)]
        for c in range(cols):
            out_dens[r - 2, c, pl.ds(at, 8)] = values[c]
        total, square = line_sums(values)
        stats[r - 2, 0, pl.ds(at, 8)] = total
        stats[r - 2, 1, pl.ds(at, 8)] = square

    def scale(r, at):
        pair = [(stats[r - 2, 0, pl.ds(at, 8)], stats[r - 2, 1, pl.ds(at, 8)])]
        for j in range(lons - 1):
            pair.append((peers[j, r - 2, 0, pl.ds(at, 8)], peers[j, r - 2, 1, pl.ds(at, 8)]))
        mean, gain = line_scale(pair, cols)
        for c in range(cols):
            out_scaled[r - 2, c, pl.ds(at, 8)] = (out_dens[r - 2, c, pl.ds(at, 8)] - mean) * gain

    def each_inner(act):
        def row(r, _):
            tiles(0, deep, lambda at: act(r, at))
            return 0
        lax.fori_loop(2, rows, row, 0)

    each_inner(lambda r, at: finish(r, at, False))
    tiles(0, deep, lambda at: finish(rows, at, True))
    for j in range(1, lons):
        stat(j).start()

    def base(c, _):
        edge[c - 1] = cell(t, 1, c, 0, deep, False, True)
        return 0

    lax.fori_loop(1, cols + 1, base, 0)
    for j in range(1, lons):
        stat(j).wait_recv()
    each_inner(scale)
    tiles(0, deep, lambda at: scale(rows, at))

    def add_face(k):
        at, span = fine[k]
        face(t, k).wait_recv()

        def col(c, _):
            edge[c, pl.ds(at, span)] += 0.1 * field[t, 0, c + 1, pl.ds(PAD + at, span)]
            return 0
        lax.fori_loop(0, cols, col, 0)

    for s in range(STEPS - 1):
        for k in range(len(coarse)):
            face(s, k).wait_send()
    for s in range(STEPS):
        wait_sides_sent(s)
    for j in range(1, lons):
        stat(j).wait_send()
    add_face(0)
    face(t, 0).wait_send()

    @pl.when(late)
    def _():
        for k in range(1, len(fine) - 1):
            add_face(k)
        for k in range(1, len(fine) - 1):
            face(t, k).wait_send()


def write_inner(scaled, dens, out_scaled, out_dens, token, sems):
    inner, cols, _, _ = scaled.shape
    copies = []
    for i, (src, dst) in enumerate(((scaled, out_scaled), (dens, out_dens))):
        for r in range(inner):
            copies.append(pltpu.make_async_copy(
                src.at[r], dst.at[place(r + 2, inner + 1)], sems.at[i, r]))
    for copy in copies:
        copy.start()
    token[...] = jnp.zeros(token.shape, jnp.float32)
    for copy in copies:
        copy.wait()


def last_row(lons, edge, front, token, out_scaled, out_dens, other, stats, peers,
             entered, face_send, face_recv, stat_send, stat_recv):
    cols, deep, lanes = edge.shape
    _, fine = split(deep)
    end = len(fine) - 1
    spans = [(0, sum(fine[1]))] + fine[2:]
    lat, lon = lax.axis_index("lat"), lax.axis_index("lon")
    late = lax.rem(lon, 2)
    early = 1 - late
    order = late * lons + lon

    barrier = pltpu.get_barrier_semaphore()
    signal(barrier, {"lat": 1 - lat})
    before = 0
    for j in range(1, lons):
        there = lax.rem(lon + j, lons)
        ahead = lax.rem(there, 2) * lons + there < order
        before += ahead.astype(jnp.int32)
        pl.when(jnp.logical_not(ahead))(lambda: signal(barrier, {"lon": there}))
    pl.semaphore_wait(barrier, 1 + before)

    def face(k):
        at, span = fine[k]
        return pltpu.make_async_remote_copy(
            src_ref=front.at[:, pl.ds(at, span)],
            dst_ref=other.at[:, pl.ds(at, span)],
            send_sem=face_send.at[k],
            recv_sem=face_recv.at[k],
            device_id={"lat": 1 - lat},
            device_id_type=MESH,
        )

    def stat(part, j):
        pick = (slice(None), pl.ds(*spans[part]))
        return pltpu.make_async_remote_copy(
            src_ref=stats.at[pick],
            dst_ref=peers.at[(j - 1,) + pick],
            send_sem=stat_send.at[part, j - 1],
            recv_sem=stat_recv.at[part, j - 1],
            device_id={"lon": lax.rem(lon + j, lons)},
            device_id_type=MESH,
        )

    for k in range(1, end):
        pl.when(early == 1)(lambda: face(k).start())
    face(end).start()
    for j in range(1, lons):
        there = lax.rem(lon + j, lons)
        ahead = lax.rem(there, 2) * lons + there < order
        pl.when(ahead)(lambda: signal(entered, {"lon": there}))

    def finish(at, add):
        values = [edge[c, pl.ds(at, 8)] for c in range(cols)]
        if add:
            values = [v + 0.1 * other[c, pl.ds(at, 8)] for c, v in enumerate(values)]
        for c in range(cols):
            out_dens[c, pl.ds(at, 8)] = values[c]
        total, square = line_sums(values)
        stats[0, pl.ds(at, 8)] = total
        stats[1, pl.ds(at, 8)] = square

    def scale(at):
        pair = [(stats[0, pl.ds(at, 8)], stats[1, pl.ds(at, 8)])]
        for j in range(lons - 1):
            pair.append((peers[j, 0, pl.ds(at, 8)], peers[j, 1, pl.ds(at, 8)]))
        mean, gain = line_scale(pair, cols)
        for c in range(cols):
            out_scaled[c, pl.ds(at, 8)] = (out_dens[c, pl.ds(at, 8)] - mean) * gain

    tiles(*fine[0], lambda at: finish(at, False))
    for k in range(1, end + 1):
        if k < end:
            pl.when(early == 0)(lambda: tiles(*fine[k], lambda at: finish(at, False)))

            @pl.when(early == 1)
            def _():
                face(k).wait_recv()
                tiles(*fine[k], lambda at: finish(at, True))
        else:
            face(k).wait_recv()
            tiles(*fine[k], lambda at: finish(at, True))
        if k == 1:
            pl.when(before < lons - 1)(lambda: pl.semaphore_wait(entered, lons - 1 - before))
        for j in range(1, lons):
            stat(k - 1, j).start()
        if k > 1:
            for j in range(1, lons):
                stat(k - 2, j).wait_recv()
            tiles(*spans[k - 2], scale)
    for k in range(1, end):
        pl.when(early == 1)(lambda: face(k).wait_send())
    face(end).wait_send()
    for j in range(1, lons):
        stat(end - 1, j).wait_recv()
    tiles(*spans[end - 1], scale)
    for part in range(len(spans)):
        for j in range(1, lons):
            stat(part, j).wait_send()


def write_last(scaled, dens, in_scaled, in_dens, out_scaled, out_dens, sems):
    del in_scaled, in_dens
    rows, many = out_dens.shape[0], sems.shape[1]
    step = dens.shape[0] // many
    copies = []
    for i, (src, dst) in enumerate(((scaled, out_scaled), (dens, out_dens))):
        for part in range(many):
            span = pl.ds(part * step, step)
            copies.append(pltpu.make_async_copy(
                src.at[span], dst.at[place(1, rows), span], sems.at[i, part]))
    for copy in copies:
        copy.start()
    for copy in copies:
        copy.wait()


def in_vmem(*arrays):
    return [pltpu.with_memory_space_constraint(a, pltpu.VMEM) for a in arrays]


def all_steps(lons, levs, density, crowding):
    rows, cols, deep, lanes = density.shape
    coarse, fine = split(deep)
    sem = pltpu.SemaphoreType.DMA
    peers = max(lons - 1, 1)
    inner = pltpu.VMEM((rows - 1, cols, deep, lanes), jnp.float32)
    row = pltpu.VMEM((cols, deep, lanes), jnp.float32)
    any_space = pl.BlockSpec(memory_space=pl.ANY)
    vmem = pl.BlockSpec(memory_space=pltpu.VMEM)
    scaled, dens, edge, front = pl.pallas_call(
        functools.partial(kernel, lons, levs),
        out_shape=(inner, inner, row, row),
        in_specs=[any_space] * 2,
        out_specs=[vmem] * 4,
        scratch_shapes=[
            pltpu.VMEM((STEPS, rows + 1, cols + 2, deep + 2 * PAD, lanes), jnp.float32),
            pltpu.VMEM((rows, cols, deep, lanes), jnp.float32),
            pltpu.VMEM((rows - 1, 2, deep, lanes), jnp.float32),
            pltpu.VMEM((peers, rows - 1, 2, deep, lanes), jnp.float32),
            sem((2, rows)),
            sem((len(coarse),)),
            sem((STEPS, len(fine))),
            sem((STEPS, len(fine))),
            sem((STEPS, 2)),
            sem((STEPS, 2)),
            sem((STEPS, 2)),
            sem((STEPS, 2)),
            sem((peers,)),
            sem((peers,)),
        ],
        compiler_params=pltpu.CompilerParams(
            collective_id=0, has_side_effects=True, vmem_limit_bytes=VMEM_LIMIT
        ),
    )(density, crowding)

    out = jax.ShapeDtypeStruct(density.shape, density.dtype)
    out_scaled, out_dens, token = pl.pallas_call(
        write_inner,
        out_shape=(out, out, pltpu.VMEM((8, lanes), jnp.float32)),
        in_specs=[vmem] * 2,
        out_specs=[pl.BlockSpec(memory_space=pltpu.HBM)] * 2 + [vmem],
        scratch_shapes=[sem((2, rows - 1))],
        compiler_params=pltpu.CompilerParams(vmem_limit_bytes=2**20),
    )(*in_vmem(scaled, dens))

    row_scaled, row_dens = pl.pallas_call(
        functools.partial(last_row, lons),
        out_shape=(row, row),
        in_specs=[vmem] * 3,
        out_specs=[vmem] * 2,
        scratch_shapes=[
            pltpu.VMEM((cols, deep, lanes), jnp.float32),
            pltpu.VMEM((2, deep, lanes), jnp.float32),
            pltpu.VMEM((peers, 2, deep, lanes), jnp.float32),
            pltpu.SemaphoreType.REGULAR,
            sem((len(fine),)),
            sem((len(fine),)),
            sem((len(fine) - 1, peers)),
            sem((len(fine) - 1, peers)),
        ],
        compiler_params=pltpu.CompilerParams(
            collective_id=1, has_side_effects=True, vmem_limit_bytes=8 * 2**20
        ),
    )(*in_vmem(edge, front, token))

    hbm = pl.BlockSpec(memory_space=pltpu.HBM)
    return pl.pallas_call(
        write_last,
        out_shape=(out, out),
        in_specs=[vmem] * 2 + [hbm] * 2,
        out_specs=[hbm] * 2,
        input_output_aliases={2: 0, 3: 1},
        scratch_shapes=[sem((2, 4 if cols % 4 == 0 else 1))],
        compiler_params=pltpu.CompilerParams(vmem_limit_bytes=2**20),
    )(*in_vmem(row_scaled, row_dens), out_scaled, out_dens)


VMEM_LIMIT = 44 * 2**20


def solution(mesh):
    lats, lons, levs = mesh.shape["lat"], mesh.shape["lon"], mesh.shape["lev"]

    def shards(density, crowding):
        rows, cols, deep, lanes = density.shape
        words = lanes * (
            STEPS * (rows + 1) * (cols + 2) * (deep + 2 * PAD)
            + 3 * rows * cols * deep
            + 2 * lons * rows * deep
        )
        fits = lats == 2 and rows > 1 and lanes == 128 and deep % 32 == 0 and 4 * words < VMEM_LIMIT
        if fits:
            return tuple(all_steps(lons, levs, density, crowding))
        return general(density, crowding)

    spec = P(("trial", "lat"), "lon", "lev", None)
    return jax.shard_map(
        shards, mesh=mesh, in_specs=(spec, spec), out_specs=(spec, spec), check_vma=False
    )
```

```python
import functools

import jax
import jax.numpy as jnp
from jax import lax
from jax.experimental import pallas as pl
from jax.experimental.pallas import tpu as pltpu
from jax.sharding import PartitionSpec as P

STEPS = 4
PAD = 8
MESH = pl.DeviceIdType.MESH


def with_halo(cells, sides, width):
    for axis, dim in sides:
        count = lax.axis_size(axis)
        ends = count - 1
        head = lax.slice_in_dim(cells, 0, width, axis=dim)
        tail = lax.slice_in_dim(cells, cells.shape[dim] - width, cells.shape[dim], axis=dim)
        cells = jnp.concatenate(
            [
                lax.ppermute(tail, axis, [(i, (i + 1) % count) for i in range(ends)]),
                cells,
                lax.ppermute(head, axis, [((i + 1) % count, i) for i in range(ends)]),
            ],
            axis=dim,
        )
    return cells


def inner_cells(values, dims):
    for dim in dims:
        values = lax.slice_in_dim(values, 1, values.shape[dim] - 1, axis=dim)
    return values


def side_cells(values, dim, start, dims):
    others = [other for other in dims if other != dim]
    values = inner_cells(values, others)
    return lax.slice_in_dim(values, start, start + values.shape[dim] - 2, axis=dim)


def advance(padded, crowding):
    middle = inner_cells(padded, (0, 1, 2))
    lower = [side_cells(padded, dim, 0, (0, 1, 2)) for dim in (0, 1, 2)]
    upper = [side_cells(padded, dim, 2, (0, 1, 2)) for dim in (0, 1, 2)]
    spread = lower[0] + upper[0] + lower[1] + upper[1] + lower[2] + upper[2] - 6.0 * middle
    return middle + 0.1 * spread + 0.2 * middle * (1.0 - middle * crowding)


def general(density, crowding):
    for step in range(STEPS):
        padded = with_halo(density, (("lat", 0), ("lon", 1), ("lev", 2)), 1)
        density = advance(padded, crowding)
    count = density.shape[1] * lax.axis_size("lon")
    moved = density - 1.0
    totals, squares = lax.psum(
        (jnp.sum(moved, axis=1, keepdims=True), jnp.sum(moved * moved, axis=1, keepdims=True)),
        "lon",
    )
    line_mean = 1.0 + totals / count
    centred = density - line_mean
    line_variance = squares / count - totals / count * (totals / count)
    return (centred * lax.rsqrt(line_variance + 0.0001), density)


def tree_sum(terms):
    terms = list(terms)
    while len(terms) > 1:
        terms = [sum(terms[i : i + 2][1:], terms[i]) for i in range(0, len(terms), 2)]
    return terms[0]


def signal(sem, where):
    pl.semaphore_signal(sem, inc=1, device_id=where, device_id_type=MESH)


def split(deep):
    half, first, late = deep // 2, max(8, deep // 32 * 8), max(8, 3 * deep // 128 * 8)
    coarse = [(0, half), (half, half)]
    fine = [(0, first), (first, deep - 8 - late - first), (deep - 8 - late, late), (deep - 8, 8)]
    return coarse, fine


def place(r, rows):
    lat = lax.axis_index("lat")
    return (1 - lat) * (rows - r) + lat * (r - 1)


def tiles(first, many, act):
    def tile(i, _):
        act(pl.multiple_of(i * 8, 8))
        return 0
    lax.fori_loop(first // 8, (first + many) // 8, tile, 0)


def line_sums(values):
    cols = len(values)
    total = tree_sum(values)
    mean = total * (1.0 / cols)
    return total, tree_sum([(v - mean) * (v - mean) for v in values])


def line_scale(pair, cols):
    count = cols * len(pair)
    mean = tree_sum([p[0] for p in pair]) * (1.0 / count)
    square = tree_sum([p[1] + cols * (p[0] * (1.0 / cols) - mean) ** 2 for p in pair])
    return mean, lax.rsqrt(square * (1.0 / count) + 0.0001)


def kernel(lons, levs, dens, crowd, out_scaled, out_dens, edge, front,
           field, cap, stats, peers, load_sem, edge_sem, face_send, face_recv,
           lon_send, lon_recv, lev_send, lev_recv, stat_send, stat_recv):
    rows, cols, deep, lanes = dens.shape
    coarse, fine = split(deep)
    lat, lon, lev = lax.axis_index("lat"), lax.axis_index("lon"), lax.axis_index("lev")
    has_left, has_right = lon > 0, lon < lons - 1
    has_down, has_up = lev > 0, lev < levs - 1
    late = lax.rem(lon, 2) == 0

    first = [
        pltpu.make_async_copy(
            dens.at[place(1, rows), :, pl.ds(at, span)],
            field.at[0, 1, pl.ds(1, cols), pl.ds(PAD + at, span)],
            edge_sem.at[k])
        for k, (at, span) in enumerate(coarse)
    ]
    loads = []
    for r in range(1, rows + 1):
        if r > 1:
            loads.append(pltpu.make_async_copy(
                dens.at[place(r, rows)],
                field.at[0, r, pl.ds(1, cols), pl.ds(PAD, deep)],
                load_sem.at[0, r - 1]))
        loads.append(pltpu.make_async_copy(
            crowd.at[place(r, rows)], cap.at[r - 1], load_sem.at[1, r - 1]))

    barrier = pltpu.get_barrier_semaphore()
    signal(barrier, {"lat": 1 - lat})
    for j in range(1, lons):
        signal(barrier, {"lon": lax.rem(lon + j, lons)})
    if levs > 1:
        pl.when(has_down)(lambda: signal(barrier, {"lev": lev - 1}))
        pl.when(has_up)(lambda: signal(barrier, {"lev": lev + 1}))
    for copy in first + loads:
        copy.start()
    pl.semaphore_wait(barrier, lons + has_down.astype(jnp.int32) + has_up.astype(jnp.int32))

    def chunks(t):
        return fine if t == STEPS - 1 else coarse

    def face(t, k):
        at, span = chunks(t)[k]
        return pltpu.make_async_remote_copy(
            src_ref=field.at[t, 1, pl.ds(1, cols), pl.ds(PAD + at, span)],
            dst_ref=field.at[t, 0, pl.ds(1, cols), pl.ds(PAD + at, span)],
            send_sem=face_send.at[t, k],
            recv_sem=face_recv.at[t, k],
            device_id={"lat": 1 - lat},
            device_id_type=MESH,
        )

    bands = (pl.ds(1, 1), pl.ds(2, rows - 1))

    def lon_side(t, band, right):
        own, theirs = (cols, 0) if right else (1, cols + 1)
        span = bands[band]
        return pltpu.make_async_remote_copy(
            src_ref=field.at[t, span, own, pl.ds(PAD, deep)],
            dst_ref=field.at[t, span, theirs, pl.ds(PAD, deep)],
            send_sem=lon_send.at[t, band, int(right)],
            recv_sem=lon_recv.at[t, band, int(right)],
            device_id={"lon": lon + 1 if right else lon - 1},
            device_id_type=MESH,
        )

    def lev_side(t, band, up):
        own, theirs = (PAD + deep - 1, PAD - 1) if up else (PAD, PAD + deep)
        span = (bands[band], pl.ds(1, cols))
        return pltpu.make_async_remote_copy(
            src_ref=field.at[t, span[0], span[1], pl.ds(own, 1)],
            dst_ref=field.at[t, span[0], span[1], pl.ds(theirs, 1)],
            send_sem=lev_send.at[t, band, int(up)],
            recv_sem=lev_recv.at[t, band, int(up)],
            device_id={"lev": lev + 1 if up else lev - 1},
            device_id_type=MESH,
        )

    def sides(t, band, act):
        if lons > 1:
            pl.when(has_right)(lambda: act(lon_side(t, band, True)))
            pl.when(has_left)(lambda: act(lon_side(t, band, False)))
        if levs > 1:
            pl.when(has_up)(lambda: act(lev_side(t, band, True)))
            pl.when(has_down)(lambda: act(lev_side(t, band, False)))

    def start_sides(t, band):
        sides(t, band, lambda copy: copy.start())

    def wait_sides_sent(t, band):
        sides(t, band, lambda copy: copy.wait_send())

    def wait_sides(t, band):
        if lons > 1:
            pl.when(has_left)(lambda: lon_side(t, band, True).wait_recv())
            pl.when(has_right)(lambda: lon_side(t, band, False).wait_recv())
        if levs > 1:
            pl.when(has_down)(lambda: lev_side(t, band, True).wait_recv())
            pl.when(has_up)(lambda: lev_side(t, band, False).wait_recv())

    stat_rows = (pl.ds(0, 1), pl.ds(1, rows - 2))
    groups = range(2 if rows > 2 else 1)

    def stat(group, j):
        return pltpu.make_async_remote_copy(
            src_ref=stats.at[stat_rows[group]],
            dst_ref=peers.at[j - 1, stat_rows[group]],
            send_sem=stat_send.at[group, j - 1],
            recv_sem=stat_recv.at[group, j - 1],
            device_id={"lon": lax.rem(lon + j, lons)},
            device_id_type=MESH,
        )

    for k in range(len(coarse)):
        first[k].wait()
        face(0, k).start()

    def clear_cols(at):
        for t in range(STEPS):
            def row(i, _, t=t):
                field[t, i, at, pl.ds(PAD, deep)] = jnp.zeros((deep, lanes), jnp.float32)
                return 0
            lax.fori_loop(1, rows + 1, row, 0)

    def clear_level(at):
        for t in range(STEPS):
            def row(i, _, t=t):
                def col(c, _):
                    field[t, i, c, pl.ds(at, PAD)] = jnp.zeros((PAD, lanes), jnp.float32)
                    return 0
                return lax.fori_loop(1, cols + 1, col, 0)
            lax.fori_loop(1, rows + 1, row, 0)

    pl.when(jnp.logical_not(has_left))(lambda: clear_cols(0))
    pl.when(jnp.logical_not(has_right))(lambda: clear_cols(cols + 1))
    pl.when(jnp.logical_not(has_down))(lambda: clear_level(0))
    pl.when(jnp.logical_not(has_up))(lambda: clear_level(PAD + deep))

    for copy in loads:
        copy.wait()
    start_sides(0, 1)
    start_sides(0, 0)

    def cell(t, r, c, at, span, below, above):
        here = field[t, r, c, pl.ds(PAD + at, span)]
        near = (field[t, r, c - 1, pl.ds(PAD + at, span)] + field[t, r, c + 1, pl.ds(PAD + at, span)])
        near += (field[t, r, c, pl.ds(PAD - 1 + at, span)] + field[t, r, c, pl.ds(PAD + 1 + at, span)])
        if below:
            near += field[t, r - 1, c, pl.ds(PAD + at, span)]
        if above:
            near += field[t, r + 1, c, pl.ds(PAD + at, span)]
        limit = cap[r - 1, c - 1, pl.ds(at, span)]
        return here * (0.6 - 0.2 * (here * limit)) + 0.1 * near

    def advance_row(t, r, at, span, last):
        def col(c, _):
            value = cell(t, r, c, at, span, True, not last)
            field[t + 1, r, c, pl.ds(PAD + at, span)] = value
            if t == STEPS - 2 and isinstance(r, int) and r == 1:
                front[c - 1, pl.ds(at, span)] = value
            return 0
        lax.fori_loop(1, cols + 1, col, 0)

    def start_face(t, k):
        if t == STEPS - 1 and k == len(fine) - 1:
            return
        if t == STEPS - 1 and k > 0:
            pl.when(late)(lambda: face(t, k).start())
        else:
            face(t, k).start()

    def finish(r, at, last):
        values = [cell(STEPS - 1, r, c, at, 8, True, not last) for c in range(1, cols + 1)]
        for c in range(cols):
            out_dens[r - 2, c, pl.ds(at, 8)] = values[c]
        total, square = line_sums(values)
        stats[r - 2, 0, pl.ds(at, 8)] = total
        stats[r - 2, 1, pl.ds(at, 8)] = square

    def scale(r, at):
        pair = [(stats[r - 2, 0, pl.ds(at, 8)], stats[r - 2, 1, pl.ds(at, 8)])]
        for j in range(lons - 1):
            pair.append((peers[j, r - 2, 0, pl.ds(at, 8)], peers[j, r - 2, 1, pl.ds(at, 8)]))
        mean, gain = line_scale(pair, cols)
        for c in range(cols):
            out_scaled[r - 2, c, pl.ds(at, 8)] = (out_dens[r - 2, c, pl.ds(at, 8)] - mean) * gain

    def each_row(first, last, act):
        def row(r, _):
            tiles(0, deep, lambda at: act(r, at))
            return 0
        lax.fori_loop(first, last, row, 0)

    def send_sums(group):
        for j in range(1, lons):
            stat(group, j).start()

    def wait_sums(group):
        for j in range(1, lons):
            stat(group, j).wait_recv()

    for t in range(STEPS - 1):
        wait_sides(t, 1)

        def inner(r, _, t=t):
            advance_row(t, r, 0, deep, False)
            return 0

        lax.fori_loop(2, rows, inner, 0)
        advance_row(t, rows, 0, deep, True)
        start_sides(t + 1, 1)
        if t == STEPS - 2:
            wait_sides(t + 1, 1)
            if rows > 2:
                each_row(3, rows, lambda r, at: finish(r, at, False))
                tiles(0, deep, lambda at: finish(rows, at, True))
                send_sums(1)
                wait_sums(1)
                each_row(3, rows + 1, scale)
        wait_sides(t, 0)
        for k in range(len(coarse)):
            face(t, k).wait_recv()
            advance_row(t, 1, *coarse[k], False)
            for j, chunk in enumerate(chunks(t + 1)):
                if coarse[k][0] < sum(chunk) <= sum(coarse[k]):
                    start_face(t + 1, j)
        start_sides(t + 1, 0)

    t = STEPS - 1
    tiles(0, deep, lambda at: finish(2, at, rows == 2))
    send_sums(0)
    wait_sides(t, 0)

    def base(c, _):
        edge[c - 1] = cell(t, 1, c, 0, deep, False, True)
        return 0

    lax.fori_loop(1, cols + 1, base, 0)
    wait_sums(0)
    tiles(0, deep, lambda at: scale(2, at))

    def add_face(k):
        at, span = fine[k]
        face(t, k).wait_recv()

        def col(c, _):
            edge[c, pl.ds(at, span)] += 0.1 * field[t, 0, c + 1, pl.ds(PAD + at, span)]
            return 0
        lax.fori_loop(0, cols, col, 0)

    for s in range(STEPS - 1):
        for k in range(len(coarse)):
            face(s, k).wait_send()
    for s in range(STEPS):
        for band in range(2):
            wait_sides_sent(s, band)
    for group in groups:
        for j in range(1, lons):
            stat(group, j).wait_send()
    add_face(0)
    face(t, 0).wait_send()

    @pl.when(late)
    def _():
        for k in range(1, len(fine) - 1):
            add_face(k)
        for k in range(1, len(fine) - 1):
            face(t, k).wait_send()


def write_inner(scaled, dens, edge, out_scaled, out_dens, token, sems):
    inner, cols, _, _ = scaled.shape
    copies = []
    for i, (src, dst) in enumerate(((scaled, out_scaled), (dens, out_dens))):
        for r in range(inner):
            copies.append(pltpu.make_async_copy(
                src.at[r], dst.at[place(r + 2, inner + 1)], sems.at[i, r]))
    copies.append(pltpu.make_async_copy(edge, out_dens.at[place(1, inner + 1)], sems.at[1, inner]))
    for copy in copies:
        copy.start()
    token[...] = jnp.zeros(token.shape, jnp.float32)
    for copy in copies:
        copy.wait()


def last_row(lons, edge, front, token, out_scaled, out_dens, other, stats, peers,
             entered, face_send, face_recv, stat_send, stat_recv):
    cols, deep, lanes = edge.shape
    _, fine = split(deep)
    end = len(fine) - 1
    spans = [(0, sum(fine[1]))] + fine[2:]
    lat, lon = lax.axis_index("lat"), lax.axis_index("lon")
    early = lax.rem(lon, 2)
    late = 1 - early
    order = late * lons + lon

    barrier = pltpu.get_barrier_semaphore()
    signal(barrier, {"lat": 1 - lat})
    before = 0
    for j in range(1, lons):
        there = lax.rem(lon + j, lons)
        ahead = (1 - lax.rem(there, 2)) * lons + there < order
        before += ahead.astype(jnp.int32)
        pl.when(jnp.logical_not(ahead))(lambda: signal(barrier, {"lon": there}))
    pl.semaphore_wait(barrier, 1 + before)

    def face(k):
        at, span = fine[k]
        return pltpu.make_async_remote_copy(
            src_ref=front.at[:, pl.ds(at, span)],
            dst_ref=other.at[:, pl.ds(at, span)],
            send_sem=face_send.at[k],
            recv_sem=face_recv.at[k],
            device_id={"lat": 1 - lat},
            device_id_type=MESH,
        )

    def stat(part, j):
        pick = (slice(None), pl.ds(*spans[part]))
        return pltpu.make_async_remote_copy(
            src_ref=stats.at[pick],
            dst_ref=peers.at[(j - 1,) + pick],
            send_sem=stat_send.at[part, j - 1],
            recv_sem=stat_recv.at[part, j - 1],
            device_id={"lon": lax.rem(lon + j, lons)},
            device_id_type=MESH,
        )

    for k in range(1, end):
        pl.when(early == 1)(lambda: face(k).start())
    face(end).start()
    for j in range(1, lons):
        there = lax.rem(lon + j, lons)
        ahead = (1 - lax.rem(there, 2)) * lons + there < order
        pl.when(ahead)(lambda: signal(entered, {"lon": there}))

    def finish(at, add):
        values = [edge[c, pl.ds(at, 8)] for c in range(cols)]
        if add:
            values = [v + 0.1 * other[c, pl.ds(at, 8)] for c, v in enumerate(values)]
        for c in range(cols):
            out_dens[c, pl.ds(at, 8)] = values[c]
        total, square = line_sums(values)
        stats[0, pl.ds(at, 8)] = total
        stats[1, pl.ds(at, 8)] = square

    def scale(at):
        pair = [(stats[0, pl.ds(at, 8)], stats[1, pl.ds(at, 8)])]
        for j in range(lons - 1):
            pair.append((peers[j, 0, pl.ds(at, 8)], peers[j, 1, pl.ds(at, 8)]))
        mean, gain = line_scale(pair, cols)
        for c in range(cols):
            out_scaled[c, pl.ds(at, 8)] = (out_dens[c, pl.ds(at, 8)] - mean) * gain

    tiles(*fine[0], lambda at: finish(at, False))
    for k in range(1, end + 1):
        if k < end:
            pl.when(early == 0)(lambda: tiles(*fine[k], lambda at: finish(at, False)))

            @pl.when(early == 1)
            def _():
                face(k).wait_recv()
                tiles(*fine[k], lambda at: finish(at, True))
        else:
            face(k).wait_recv()
            tiles(*fine[k], lambda at: finish(at, True))
        if k == 1:
            pl.when(before < lons - 1)(lambda: pl.semaphore_wait(entered, lons - 1 - before))
        for j in range(1, lons):
            stat(k - 1, j).start()
        if k > 1:
            for j in range(1, lons):
                stat(k - 2, j).wait_recv()
            tiles(*spans[k - 2], scale)
    for k in range(1, end):
        pl.when(early == 1)(lambda: face(k).wait_send())
    face(end).wait_send()
    for j in range(1, lons):
        stat(end - 1, j).wait_recv()
    tiles(*spans[end - 1], scale)
    for part in range(len(spans)):
        for j in range(1, lons):
            stat(part, j).wait_send()


def write_last(scaled, dens, in_scaled, in_dens, out_scaled, out_dens, sems):
    del in_scaled, in_dens
    rows, many = out_dens.shape[0], sems.shape[1] - 1
    cols, deep, _ = dens.shape
    late = lax.rem(lax.axis_index("lon"), 2) == 0

    def copies(src, dst, i, known):
        if known:
            span = pl.ds(deep - 8, 8)
            return [pltpu.make_async_copy(
                src.at[:, span], dst.at[place(1, rows), :, span], sems.at[i, many])]
        step = cols // many
        return [
            pltpu.make_async_copy(
                src.at[pl.ds(part * step, step)],
                dst.at[place(1, rows), pl.ds(part * step, step)],
                sems.at[i, part])
            for part in range(many)
        ]

    def each(act):
        for copy in copies(scaled, out_scaled, 0, False):
            act(copy)
        for known in (False, True):
            @pl.when(late == known)
            def _():
                for copy in copies(dens, out_dens, 1, known):
                    act(copy)

    each(lambda copy: copy.start())
    each(lambda copy: copy.wait())


def in_vmem(*arrays):
    return [pltpu.with_memory_space_constraint(a, pltpu.VMEM) for a in arrays]


def all_steps(lons, levs, density, crowding):
    rows, cols, deep, lanes = density.shape
    coarse, fine = split(deep)
    sem = pltpu.SemaphoreType.DMA
    peers = max(lons - 1, 1)
    inner = pltpu.VMEM((rows - 1, cols, deep, lanes), jnp.float32)
    row = pltpu.VMEM((cols, deep, lanes), jnp.float32)
    any_space = pl.BlockSpec(memory_space=pl.ANY)
    vmem = pl.BlockSpec(memory_space=pltpu.VMEM)
    scaled, dens, edge, front = pl.pallas_call(
        functools.partial(kernel, lons, levs),
        out_shape=(inner, inner, row, row),
        in_specs=[any_space] * 2,
        out_specs=[vmem] * 4,
        scratch_shapes=[
            pltpu.VMEM((STEPS, rows + 1, cols + 2, deep + 2 * PAD, lanes), jnp.float32),
            pltpu.VMEM((rows, cols, deep, lanes), jnp.float32),
            pltpu.VMEM((rows - 1, 2, deep, lanes), jnp.float32),
            pltpu.VMEM((peers, rows - 1, 2, deep, lanes), jnp.float32),
            sem((2, rows)),
            sem((len(coarse),)),
            sem((STEPS, len(fine))),
            sem((STEPS, len(fine))),
            sem((STEPS, 2, 2)),
            sem((STEPS, 2, 2)),
            sem((STEPS, 2, 2)),
            sem((STEPS, 2, 2)),
            sem((2, peers)),
            sem((2, peers)),
        ],
        compiler_params=pltpu.CompilerParams(
            collective_id=0, has_side_effects=True, vmem_limit_bytes=VMEM_LIMIT
        ),
    )(density, crowding)

    out = jax.ShapeDtypeStruct(density.shape, density.dtype)
    out_scaled, out_dens, token = pl.pallas_call(
        write_inner,
        out_shape=(out, out, pltpu.VMEM((8, lanes), jnp.float32)),
        in_specs=[vmem] * 3,
        out_specs=[pl.BlockSpec(memory_space=pltpu.HBM)] * 2 + [vmem],
        scratch_shapes=[sem((2, rows))],
        compiler_params=pltpu.CompilerParams(vmem_limit_bytes=2**20),
    )(*in_vmem(scaled, dens, edge))

    row_scaled, row_dens = pl.pallas_call(
        functools.partial(last_row, lons),
        out_shape=(row, row),
        in_specs=[vmem] * 3,
        out_specs=[vmem] * 2,
        scratch_shapes=[
            pltpu.VMEM((cols, deep, lanes), jnp.float32),
            pltpu.VMEM((2, deep, lanes), jnp.float32),
            pltpu.VMEM((peers, 2, deep, lanes), jnp.float32),
            pltpu.SemaphoreType.REGULAR,
            sem((len(fine),)),
            sem((len(fine),)),
            sem((len(fine) - 1, peers)),
            sem((len(fine) - 1, peers)),
        ],
        compiler_params=pltpu.CompilerParams(
            collective_id=1, has_side_effects=True, vmem_limit_bytes=8 * 2**20
        ),
    )(*in_vmem(edge, front, token))

    hbm = pl.BlockSpec(memory_space=pltpu.HBM)
    return pl.pallas_call(
        write_last,
        out_shape=(out, out),
        in_specs=[vmem] * 2 + [hbm] * 2,
        out_specs=[hbm] * 2,
        input_output_aliases={2: 0, 3: 1},
        scratch_shapes=[sem((2, 5 if cols % 4 == 0 else 2))],
        compiler_params=pltpu.CompilerParams(vmem_limit_bytes=2**20),
    )(*in_vmem(row_scaled, row_dens), out_scaled, out_dens)


VMEM_LIMIT = 44 * 2**20


def solution(mesh):
    lats, lons, levs = mesh.shape["lat"], mesh.shape["lon"], mesh.shape["lev"]

    def shards(density, crowding):
        rows, cols, deep, lanes = density.shape
        words = lanes * (
            STEPS * (rows + 1) * (cols + 2) * (deep + 2 * PAD)
            + 3 * rows * cols * deep
            + 2 * lons * rows * deep
        )
        fits = lats == 2 and rows > 1 and lanes == 128 and deep % 32 == 0 and 4 * words < VMEM_LIMIT
        if fits:
            return tuple(all_steps(lons, levs, density, crowding))
        return general(density, crowding)

    spec = P(("trial", "lat"), "lon", "lev", None)
    return jax.shard_map(
        shards, mesh=mesh, in_specs=(spec, spec), out_specs=(spec, spec), check_vma=False
    )
```

```python
import functools

import jax
import jax.numpy as jnp
from jax import lax
from jax.experimental import pallas as pl
from jax.experimental.pallas import tpu as pltpu
from jax.sharding import PartitionSpec as P

STEPS = 4
PAD = 8
MESH = pl.DeviceIdType.MESH


def with_halo(cells, sides, width):
    for axis, dim in sides:
        count = lax.axis_size(axis)
        ends = count - 1
        head = lax.slice_in_dim(cells, 0, width, axis=dim)
        tail = lax.slice_in_dim(cells, cells.shape[dim] - width, cells.shape[dim], axis=dim)
        cells = jnp.concatenate(
            [
                lax.ppermute(tail, axis, [(i, (i + 1) % count) for i in range(ends)]),
                cells,
                lax.ppermute(head, axis, [((i + 1) % count, i) for i in range(ends)]),
            ],
            axis=dim,
        )
    return cells


def inner_cells(values, dims):
    for dim in dims:
        values = lax.slice_in_dim(values, 1, values.shape[dim] - 1, axis=dim)
    return values


def side_cells(values, dim, start, dims):
    others = [other for other in dims if other != dim]
    values = inner_cells(values, others)
    return lax.slice_in_dim(values, start, start + values.shape[dim] - 2, axis=dim)


def advance(padded, crowding):
    middle = inner_cells(padded, (0, 1, 2))
    lower = [side_cells(padded, dim, 0, (0, 1, 2)) for dim in (0, 1, 2)]
    upper = [side_cells(padded, dim, 2, (0, 1, 2)) for dim in (0, 1, 2)]
    spread = lower[0] + upper[0] + lower[1] + upper[1] + lower[2] + upper[2] - 6.0 * middle
    return middle + 0.1 * spread + 0.2 * middle * (1.0 - middle * crowding)


def general(density, crowding):
    for step in range(STEPS):
        padded = with_halo(density, (("lat", 0), ("lon", 1), ("lev", 2)), 1)
        density = advance(padded, crowding)
    count = density.shape[1] * lax.axis_size("lon")
    moved = density - 1.0
    totals, squares = lax.psum(
        (jnp.sum(moved, axis=1, keepdims=True), jnp.sum(moved * moved, axis=1, keepdims=True)),
        "lon",
    )
    line_mean = 1.0 + totals / count
    centred = density - line_mean
    line_variance = squares / count - totals / count * (totals / count)
    return (centred * lax.rsqrt(line_variance + 0.0001), density)


def tree_sum(terms):
    terms = list(terms)
    while len(terms) > 1:
        terms = [sum(terms[i : i + 2][1:], terms[i]) for i in range(0, len(terms), 2)]
    return terms[0]


def signal(sem, where):
    pl.semaphore_signal(sem, inc=1, device_id=where, device_id_type=MESH)


def split(deep):
    half, last = deep // 2, deep - 8
    first, late = max(8, deep // 32 * 8), max(8, deep // 64 * 8)
    opening = [(0, 8), (8, half - 8), (half, half)]
    coarse = [(0, half), (half, half)]
    fine = [(0, first), (first, last - late - first), (last - late, late), (last, 8)]
    return opening, coarse, fine


def place(r, rows):
    lat = lax.axis_index("lat")
    return (1 - lat) * (rows - r) + lat * (r - 1)


def tiles(first, many, act):
    def tile(i, _):
        act(pl.multiple_of(i * 8, 8))
        return 0
    lax.fori_loop(first // 8, (first + many) // 8, tile, 0)


def line_sums(values):
    cols = len(values)
    total = tree_sum(values)
    mean = total * (1.0 / cols)
    return total, tree_sum([(v - mean) * (v - mean) for v in values])


def line_scale(pair, cols):
    count = cols * len(pair)
    mean = tree_sum([p[0] for p in pair]) * (1.0 / count)
    square = tree_sum([p[1] + cols * (p[0] * (1.0 / cols) - mean) ** 2 for p in pair])
    return mean, lax.rsqrt(square * (1.0 / count) + 0.0001)


def kernel(lons, levs, dens, crowd, out_scaled, out_dens, edge, front,
           field, cap, stats, peers, load_sem, edge_sem, face_send, face_recv,
           lon_send, lon_recv, lev_send, lev_recv, stat_send, stat_recv):
    rows, cols, deep, lanes = dens.shape
    opening, coarse, fine = split(deep)
    lat, lon, lev = lax.axis_index("lat"), lax.axis_index("lon"), lax.axis_index("lev")
    has_left, has_right = lon > 0, lon < lons - 1
    has_down, has_up = lev > 0, lev < levs - 1
    late = lax.rem(lon, 2) == 0

    first = [
        pltpu.make_async_copy(
            dens.at[place(1, rows), :, pl.ds(at, span)],
            field.at[0, 1, pl.ds(1, cols), pl.ds(PAD + at, span)],
            edge_sem.at[k])
        for k, (at, span) in enumerate(opening)
    ]
    loads = []
    for r in range(1, rows + 1):
        if r > 1:
            loads.append(pltpu.make_async_copy(
                dens.at[place(r, rows)],
                field.at[0, r, pl.ds(1, cols), pl.ds(PAD, deep)],
                load_sem.at[0, r - 1]))
        loads.append(pltpu.make_async_copy(
            crowd.at[place(r, rows)], cap.at[r - 1], load_sem.at[1, r - 1]))

    barrier = pltpu.get_barrier_semaphore()
    signal(barrier, {"lat": 1 - lat})
    for j in range(1, lons):
        signal(barrier, {"lon": lax.rem(lon + j, lons)})
    if levs > 1:
        pl.when(has_down)(lambda: signal(barrier, {"lev": lev - 1}))
        pl.when(has_up)(lambda: signal(barrier, {"lev": lev + 1}))
    for copy in first + loads:
        copy.start()
    pl.semaphore_wait(barrier, lons + has_down.astype(jnp.int32) + has_up.astype(jnp.int32))

    def chunks(t):
        return opening if t == 0 else fine if t == STEPS - 1 else coarse

    def face(t, k):
        at, span = chunks(t)[k]
        return pltpu.make_async_remote_copy(
            src_ref=field.at[t, 1, pl.ds(1, cols), pl.ds(PAD + at, span)],
            dst_ref=field.at[t, 0, pl.ds(1, cols), pl.ds(PAD + at, span)],
            send_sem=face_send.at[t, k],
            recv_sem=face_recv.at[t, k],
            device_id={"lat": 1 - lat},
            device_id_type=MESH,
        )

    bands = (pl.ds(1, 1), pl.ds(2, rows - 1))

    def lon_side(t, band, right):
        own, theirs = (cols, 0) if right else (1, cols + 1)
        span = bands[band]
        return pltpu.make_async_remote_copy(
            src_ref=field.at[t, span, own, pl.ds(PAD, deep)],
            dst_ref=field.at[t, span, theirs, pl.ds(PAD, deep)],
            send_sem=lon_send.at[t, band, int(right)],
            recv_sem=lon_recv.at[t, band, int(right)],
            device_id={"lon": lon + 1 if right else lon - 1},
            device_id_type=MESH,
        )

    def lev_side(t, band, up):
        own, theirs = (PAD + deep - 1, PAD - 1) if up else (PAD, PAD + deep)
        span = (bands[band], pl.ds(1, cols))
        return pltpu.make_async_remote_copy(
            src_ref=field.at[t, span[0], span[1], pl.ds(own, 1)],
            dst_ref=field.at[t, span[0], span[1], pl.ds(theirs, 1)],
            send_sem=lev_send.at[t, band, int(up)],
            recv_sem=lev_recv.at[t, band, int(up)],
            device_id={"lev": lev + 1 if up else lev - 1},
            device_id_type=MESH,
        )

    def sides(t, band, act):
        if lons > 1:
            pl.when(has_right)(lambda: act(lon_side(t, band, True)))
            pl.when(has_left)(lambda: act(lon_side(t, band, False)))
        if levs > 1:
            pl.when(has_up)(lambda: act(lev_side(t, band, True)))
            pl.when(has_down)(lambda: act(lev_side(t, band, False)))

    def start_sides(t, band):
        sides(t, band, lambda copy: copy.start())

    def wait_sides_sent(t, band):
        sides(t, band, lambda copy: copy.wait_send())

    def wait_sides(t, band):
        if lons > 1:
            pl.when(has_left)(lambda: lon_side(t, band, True).wait_recv())
            pl.when(has_right)(lambda: lon_side(t, band, False).wait_recv())
        if levs > 1:
            pl.when(has_down)(lambda: lev_side(t, band, True).wait_recv())
            pl.when(has_up)(lambda: lev_side(t, band, False).wait_recv())

    stat_rows = (pl.ds(0, 1), pl.ds(1, rows - 2))
    groups = range(2 if rows > 2 else 1)

    def stat(group, j):
        return pltpu.make_async_remote_copy(
            src_ref=stats.at[stat_rows[group]],
            dst_ref=peers.at[j - 1, stat_rows[group]],
            send_sem=stat_send.at[group, j - 1],
            recv_sem=stat_recv.at[group, j - 1],
            device_id={"lon": lax.rem(lon + j, lons)},
            device_id_type=MESH,
        )

    for k in range(len(opening)):
        first[k].wait()
        face(0, k).start()

    def clear_cols(at):
        for t in range(STEPS):
            def row(i, _, t=t):
                field[t, i, at, pl.ds(PAD, deep)] = jnp.zeros((deep, lanes), jnp.float32)
                return 0
            lax.fori_loop(1, rows + 1, row, 0)

    def clear_level(at):
        for t in range(STEPS):
            def row(i, _, t=t):
                def col(c, _):
                    field[t, i, c, pl.ds(at, PAD)] = jnp.zeros((PAD, lanes), jnp.float32)
                    return 0
                return lax.fori_loop(1, cols + 1, col, 0)
            lax.fori_loop(1, rows + 1, row, 0)

    pl.when(jnp.logical_not(has_left))(lambda: clear_cols(0))
    pl.when(jnp.logical_not(has_right))(lambda: clear_cols(cols + 1))
    pl.when(jnp.logical_not(has_down))(lambda: clear_level(0))
    pl.when(jnp.logical_not(has_up))(lambda: clear_level(PAD + deep))

    for copy in loads:
        copy.wait()
    start_sides(0, 1)
    start_sides(0, 0)

    def cell(t, r, c, at, span, below, above):
        here = field[t, r, c, pl.ds(PAD + at, span)]
        near = (field[t, r, c - 1, pl.ds(PAD + at, span)] + field[t, r, c + 1, pl.ds(PAD + at, span)])
        near += (field[t, r, c, pl.ds(PAD - 1 + at, span)] + field[t, r, c, pl.ds(PAD + 1 + at, span)])
        if below:
            near += field[t, r - 1, c, pl.ds(PAD + at, span)]
        if above:
            near += field[t, r + 1, c, pl.ds(PAD + at, span)]
        limit = cap[r - 1, c - 1, pl.ds(at, span)]
        return here * (0.6 - 0.2 * (here * limit)) + 0.1 * near

    def advance_row(t, r, at, span, last):
        def col(c, _):
            value = cell(t, r, c, at, span, True, not last)
            field[t + 1, r, c, pl.ds(PAD + at, span)] = value
            if t == STEPS - 2 and isinstance(r, int) and r == 1:
                front[c - 1, pl.ds(at, span)] = value
            return 0
        lax.fori_loop(1, cols + 1, col, 0)

    def start_face(t, k):
        if t < STEPS - 1 or k == 0:
            face(t, k).start()
        elif k == 1:
            pl.when(late)(lambda: face(t, k).start())

    def finish(r, at, last):
        values = [cell(STEPS - 1, r, c, at, 8, True, not last) for c in range(1, cols + 1)]
        for c in range(cols):
            out_dens[r - 2, c, pl.ds(at, 8)] = values[c]
        total, square = line_sums(values)
        stats[r - 2, 0, pl.ds(at, 8)] = total
        stats[r - 2, 1, pl.ds(at, 8)] = square

    def scale(r, at):
        pair = [(stats[r - 2, 0, pl.ds(at, 8)], stats[r - 2, 1, pl.ds(at, 8)])]
        for j in range(lons - 1):
            pair.append((peers[j, r - 2, 0, pl.ds(at, 8)], peers[j, r - 2, 1, pl.ds(at, 8)]))
        mean, gain = line_scale(pair, cols)
        for c in range(cols):
            out_scaled[r - 2, c, pl.ds(at, 8)] = (out_dens[r - 2, c, pl.ds(at, 8)] - mean) * gain

    def each_row(first, last, act):
        def row(r, _):
            tiles(0, deep, lambda at: act(r, at))
            return 0
        lax.fori_loop(first, last, row, 0)

    def send_sums(group):
        for j in range(1, lons):
            stat(group, j).start()

    def wait_sums(group):
        for j in range(1, lons):
            stat(group, j).wait_recv()

    for t in range(STEPS - 1):
        wait_sides(t, 1)

        def inner(r, _, t=t):
            advance_row(t, r, 0, deep, False)
            return 0

        lax.fori_loop(2, rows, inner, 0)
        advance_row(t, rows, 0, deep, True)
        start_sides(t + 1, 1)
        if t == STEPS - 2:
            wait_sides(t + 1, 1)
            if rows > 2:
                each_row(3, rows, lambda r, at: finish(r, at, False))
                tiles(0, deep, lambda at: finish(rows, at, True))
                send_sums(1)
                wait_sums(1)
                each_row(3, rows + 1, scale)
        wait_sides(t, 0)
        for k, (at, span) in enumerate(chunks(t)):
            face(t, k).wait_recv()
            advance_row(t, 1, at, span, False)
            for j, chunk in enumerate(chunks(t + 1)):
                if at < sum(chunk) <= at + span:
                    start_face(t + 1, j)
        start_sides(t + 1, 0)

    t = STEPS - 1
    tiles(0, deep, lambda at: finish(2, at, rows == 2))
    send_sums(0)
    wait_sides(t, 0)

    def base(c, _):
        edge[c - 1] = cell(t, 1, c, 0, deep, False, True)
        return 0

    lax.fori_loop(1, cols + 1, base, 0)
    wait_sums(0)
    tiles(0, deep, lambda at: scale(2, at))

    def add_face(k):
        at, span = fine[k]
        face(t, k).wait_recv()

        def col(c, _):
            edge[c, pl.ds(at, span)] += 0.1 * field[t, 0, c + 1, pl.ds(PAD + at, span)]
            return 0
        lax.fori_loop(0, cols, col, 0)

    for s in range(STEPS - 1):
        for k in range(len(chunks(s))):
            face(s, k).wait_send()
    for s in range(STEPS):
        for band in range(2):
            wait_sides_sent(s, band)
    for group in groups:
        for j in range(1, lons):
            stat(group, j).wait_send()
    add_face(0)
    face(t, 0).wait_send()

    @pl.when(late)
    def _():
        add_face(1)
        face(t, 1).wait_send()


def write_inner(scaled, dens, edge, out_scaled, out_dens, token, sems):
    inner, cols, _, _ = scaled.shape
    copies = []
    for i, (src, dst) in enumerate(((scaled, out_scaled), (dens, out_dens))):
        for r in range(inner):
            copies.append(pltpu.make_async_copy(
                src.at[r], dst.at[place(r + 2, inner + 1)], sems.at[i, r]))
    copies.append(pltpu.make_async_copy(edge, out_dens.at[place(1, inner + 1)], sems.at[1, inner]))
    for copy in copies:
        copy.start()
    token[...] = jnp.zeros(token.shape, jnp.float32)
    for copy in copies:
        copy.wait()


def last_row(lons, edge, front, token, out_scaled, out_dens, other, stats, peers,
             entered, face_send, face_recv, stat_send, stat_recv):
    cols, deep, lanes = edge.shape
    _, _, fine = split(deep)
    end = len(fine) - 1
    spans = [(0, sum(fine[1]))] + fine[2:]
    lat, lon = lax.axis_index("lat"), lax.axis_index("lon")
    early = lax.rem(lon, 2)
    late = 1 - early
    order = late * lons + lon

    barrier = pltpu.get_barrier_semaphore()
    signal(barrier, {"lat": 1 - lat})
    before = 0
    for j in range(1, lons):
        there = lax.rem(lon + j, lons)
        ahead = (1 - lax.rem(there, 2)) * lons + there < order
        before += ahead.astype(jnp.int32)
        pl.when(jnp.logical_not(ahead))(lambda: signal(barrier, {"lon": there}))
    pl.semaphore_wait(barrier, 1 + before)

    def face(k):
        at, span = fine[k]
        return pltpu.make_async_remote_copy(
            src_ref=front.at[:, pl.ds(at, span)],
            dst_ref=other.at[:, pl.ds(at, span)],
            send_sem=face_send.at[k],
            recv_sem=face_recv.at[k],
            device_id={"lat": 1 - lat},
            device_id_type=MESH,
        )

    def stat(part, j):
        pick = (slice(None), pl.ds(*spans[part]))
        return pltpu.make_async_remote_copy(
            src_ref=stats.at[pick],
            dst_ref=peers.at[(j - 1,) + pick],
            send_sem=stat_send.at[part, j - 1],
            recv_sem=stat_recv.at[part, j - 1],
            device_id={"lon": lax.rem(lon + j, lons)},
            device_id_type=MESH,
        )

    pl.when(early == 1)(lambda: face(1).start())
    for k in range(2, end + 1):
        face(k).start()
    for j in range(1, lons):
        there = lax.rem(lon + j, lons)
        ahead = (1 - lax.rem(there, 2)) * lons + there < order
        pl.when(ahead)(lambda: signal(entered, {"lon": there}))

    def finish(at, add):
        values = [edge[c, pl.ds(at, 8)] for c in range(cols)]
        if add:
            values = [v + 0.1 * other[c, pl.ds(at, 8)] for c, v in enumerate(values)]
        for c in range(cols):
            out_dens[c, pl.ds(at, 8)] = values[c]
        total, square = line_sums(values)
        stats[0, pl.ds(at, 8)] = total
        stats[1, pl.ds(at, 8)] = square

    def scale(at):
        pair = [(stats[0, pl.ds(at, 8)], stats[1, pl.ds(at, 8)])]
        for j in range(lons - 1):
            pair.append((peers[j, 0, pl.ds(at, 8)], peers[j, 1, pl.ds(at, 8)]))
        mean, gain = line_scale(pair, cols)
        for c in range(cols):
            out_scaled[c, pl.ds(at, 8)] = (out_dens[c, pl.ds(at, 8)] - mean) * gain

    tiles(*fine[0], lambda at: finish(at, False))
    for k in range(1, end + 1):
        if k == 1:
            pl.when(early == 0)(lambda: tiles(*fine[k], lambda at: finish(at, False)))

            @pl.when(early == 1)
            def _():
                face(k).wait_recv()
                tiles(*fine[k], lambda at: finish(at, True))
        else:
            face(k).wait_recv()
            tiles(*fine[k], lambda at: finish(at, True))
        if k == 1:
            pl.when(before < lons - 1)(lambda: pl.semaphore_wait(entered, lons - 1 - before))
        for j in range(1, lons):
            stat(k - 1, j).start()
        if k > 1:
            for j in range(1, lons):
                stat(k - 2, j).wait_recv()
            tiles(*spans[k - 2], scale)
    pl.when(early == 1)(lambda: face(1).wait_send())
    for k in range(2, end + 1):
        face(k).wait_send()
    for j in range(1, lons):
        stat(end - 1, j).wait_recv()
    tiles(*spans[end - 1], scale)
    for part in range(len(spans)):
        for j in range(1, lons):
            stat(part, j).wait_send()


def write_last(scaled, dens, in_scaled, in_dens, out_scaled, out_dens, sems):
    del in_scaled, in_dens
    rows, many = out_dens.shape[0], sems.shape[1]
    cols, deep, _ = dens.shape
    _, _, fine = split(deep)
    late = lax.rem(lax.axis_index("lon"), 2) == 0

    def copies(src, dst, i, known):
        step = cols // many
        return [
            pltpu.make_async_copy(
                src.at[pl.ds(part * step, step), pl.ds(known, deep - known)],
                dst.at[place(1, rows), pl.ds(part * step, step), pl.ds(known, deep - known)],
                sems.at[i, part])
            for part in range(many)
        ]

    def each(act):
        for copy in copies(scaled, out_scaled, 0, 0):
            act(copy)
        for moved in range(2):
            @pl.when(late == moved)
            def _():
                for copy in copies(dens, out_dens, 1, sum(fine[moved])):
                    act(copy)

    each(lambda copy: copy.start())
    each(lambda copy: copy.wait())


def in_vmem(*arrays):
    return [pltpu.with_memory_space_constraint(a, pltpu.VMEM) for a in arrays]


def all_steps(lons, levs, density, crowding):
    rows, cols, deep, lanes = density.shape
    opening, coarse, fine = split(deep)
    sem = pltpu.SemaphoreType.DMA
    peers = max(lons - 1, 1)
    inner = pltpu.VMEM((rows - 1, cols, deep, lanes), jnp.float32)
    row = pltpu.VMEM((cols, deep, lanes), jnp.float32)
    any_space = pl.BlockSpec(memory_space=pl.ANY)
    vmem = pl.BlockSpec(memory_space=pltpu.VMEM)
    scaled, dens, edge, front = pl.pallas_call(
        functools.partial(kernel, lons, levs),
        out_shape=(inner, inner, row, row),
        in_specs=[any_space] * 2,
        out_specs=[vmem] * 4,
        scratch_shapes=[
            pltpu.VMEM((STEPS, rows + 1, cols + 2, deep + 2 * PAD, lanes), jnp.float32),
            pltpu.VMEM((rows, cols, deep, lanes), jnp.float32),
            pltpu.VMEM((rows - 1, 2, deep, lanes), jnp.float32),
            pltpu.VMEM((peers, rows - 1, 2, deep, lanes), jnp.float32),
            sem((2, rows)),
            sem((len(opening),)),
            sem((STEPS, len(fine))),
            sem((STEPS, len(fine))),
            sem((STEPS, 2, 2)),
            sem((STEPS, 2, 2)),
            sem((STEPS, 2, 2)),
            sem((STEPS, 2, 2)),
            sem((2, peers)),
            sem((2, peers)),
        ],
        compiler_params=pltpu.CompilerParams(
            collective_id=0, has_side_effects=True, vmem_limit_bytes=VMEM_LIMIT
        ),
    )(density, crowding)

    out = jax.ShapeDtypeStruct(density.shape, density.dtype)
    out_scaled, out_dens, token = pl.pallas_call(
        write_inner,
        out_shape=(out, out, pltpu.VMEM((8, lanes), jnp.float32)),
        in_specs=[vmem] * 3,
        out_specs=[pl.BlockSpec(memory_space=pltpu.HBM)] * 2 + [vmem],
        scratch_shapes=[sem((2, rows))],
        compiler_params=pltpu.CompilerParams(vmem_limit_bytes=2**20),
    )(*in_vmem(scaled, dens, edge))

    row_scaled, row_dens = pl.pallas_call(
        functools.partial(last_row, lons),
        out_shape=(row, row),
        in_specs=[vmem] * 3,
        out_specs=[vmem] * 2,
        scratch_shapes=[
            pltpu.VMEM((cols, deep, lanes), jnp.float32),
            pltpu.VMEM((2, deep, lanes), jnp.float32),
            pltpu.VMEM((peers, 2, deep, lanes), jnp.float32),
            pltpu.SemaphoreType.REGULAR,
            sem((len(fine),)),
            sem((len(fine),)),
            sem((len(fine) - 1, peers)),
            sem((len(fine) - 1, peers)),
        ],
        compiler_params=pltpu.CompilerParams(
            collective_id=1, has_side_effects=True, vmem_limit_bytes=8 * 2**20
        ),
    )(*in_vmem(edge, front, token))

    hbm = pl.BlockSpec(memory_space=pltpu.HBM)
    return pl.pallas_call(
        write_last,
        out_shape=(out, out),
        in_specs=[vmem] * 2 + [hbm] * 2,
        out_specs=[hbm] * 2,
        input_output_aliases={2: 0, 3: 1},
        scratch_shapes=[sem((2, 4 if cols % 4 == 0 else 1))],
        compiler_params=pltpu.CompilerParams(vmem_limit_bytes=2**20),
    )(*in_vmem(row_scaled, row_dens), out_scaled, out_dens)


VMEM_LIMIT = 44 * 2**20


def solution(mesh):
    lats, lons, levs = mesh.shape["lat"], mesh.shape["lon"], mesh.shape["lev"]

    def shards(density, crowding):
        rows, cols, deep, lanes = density.shape
        words = lanes * (
            STEPS * (rows + 1) * (cols + 2) * (deep + 2 * PAD)
            + 3 * rows * cols * deep
            + 2 * lons * rows * deep
        )
        fits = lats == 2 and rows > 1 and lanes == 128 and deep % 32 == 0 and 4 * words < VMEM_LIMIT
        if fits:
            return tuple(all_steps(lons, levs, density, crowding))
        return general(density, crowding)

    spec = P(("trial", "lat"), "lon", "lev", None)
    return jax.shard_map(
        shards, mesh=mesh, in_specs=(spec, spec), out_specs=(spec, spec), check_vma=False
    )
```

```python
import functools

import jax
import jax.numpy as jnp
from jax import lax
from jax.experimental import pallas as pl
from jax.experimental.pallas import tpu as pltpu
from jax.sharding import PartitionSpec as P

STEPS = 4
PAD = 8
MESH = pl.DeviceIdType.MESH


def with_halo(cells, sides, width):
    for axis, dim in sides:
        count = lax.axis_size(axis)
        ends = count - 1
        head = lax.slice_in_dim(cells, 0, width, axis=dim)
        tail = lax.slice_in_dim(cells, cells.shape[dim] - width, cells.shape[dim], axis=dim)
        cells = jnp.concatenate(
            [
                lax.ppermute(tail, axis, [(i, (i + 1) % count) for i in range(ends)]),
                cells,
                lax.ppermute(head, axis, [((i + 1) % count, i) for i in range(ends)]),
            ],
            axis=dim,
        )
    return cells


def inner_cells(values, dims):
    for dim in dims:
        values = lax.slice_in_dim(values, 1, values.shape[dim] - 1, axis=dim)
    return values


def side_cells(values, dim, start, dims):
    others = [other for other in dims if other != dim]
    values = inner_cells(values, others)
    return lax.slice_in_dim(values, start, start + values.shape[dim] - 2, axis=dim)


def advance(padded, crowding):
    middle = inner_cells(padded, (0, 1, 2))
    lower = [side_cells(padded, dim, 0, (0, 1, 2)) for dim in (0, 1, 2)]
    upper = [side_cells(padded, dim, 2, (0, 1, 2)) for dim in (0, 1, 2)]
    spread = lower[0] + upper[0] + lower[1] + upper[1] + lower[2] + upper[2] - 6.0 * middle
    return middle + 0.1 * spread + 0.2 * middle * (1.0 - middle * crowding)


def general(density, crowding):
    for step in range(STEPS):
        padded = with_halo(density, (("lat", 0), ("lon", 1), ("lev", 2)), 1)
        density = advance(padded, crowding)
    count = density.shape[1] * lax.axis_size("lon")
    moved = density - 1.0
    totals, squares = lax.psum(
        (jnp.sum(moved, axis=1, keepdims=True), jnp.sum(moved * moved, axis=1, keepdims=True)),
        "lon",
    )
    line_mean = 1.0 + totals / count
    centred = density - line_mean
    line_variance = squares / count - totals / count * (totals / count)
    return (centred * lax.rsqrt(line_variance + 0.0001), density)


def tree_sum(terms):
    terms = list(terms)
    while len(terms) > 1:
        terms = [sum(terms[i : i + 2][1:], terms[i]) for i in range(0, len(terms), 2)]
    return terms[0]


def signal(sem, where):
    pl.semaphore_signal(sem, inc=1, device_id=where, device_id_type=MESH)


def split(deep):
    half, last = deep // 2, deep - 8
    first, late = max(8, deep // 32 * 8), max(8, deep // 64 * 8)
    opening = [(0, 8), (8, half - 8), (half, half)]
    coarse = [(0, half), (half, half)]
    fine = [(0, first), (first, last - late - first), (last - late, late), (last, 8)]
    return opening, coarse, fine


def place(r, rows):
    lat = lax.axis_index("lat")
    return (1 - lat) * (rows - r) + lat * (r - 1)


def tiles(first, many, act):
    def tile(i, _):
        act(pl.multiple_of(i * 8, 8))
        return 0
    lax.fori_loop(first // 8, (first + many) // 8, tile, 0)


def line_sums(values):
    cols = len(values)
    total = tree_sum(values)
    mean = total * (1.0 / cols)
    return total, tree_sum([(v - mean) * (v - mean) for v in values])


def line_scale(pair, cols):
    count = cols * len(pair)
    mean = tree_sum([p[0] for p in pair]) * (1.0 / count)
    square = tree_sum([p[1] + cols * (p[0] * (1.0 / cols) - mean) ** 2 for p in pair])
    return mean, lax.rsqrt(square * (1.0 / count) + 0.0001)


def kernel(lons, levs, dens, crowd, out_scaled, out_dens, edge, front,
           field, cap, stats, peers, load_sem, edge_sem, face_send, face_recv,
           lon_send, lon_recv, lev_send, lev_recv, stat_send, stat_recv):
    rows, cols, deep, lanes = dens.shape
    opening, coarse, fine = split(deep)
    lat, lon, lev = lax.axis_index("lat"), lax.axis_index("lon"), lax.axis_index("lev")
    has_left, has_right = lon > 0, lon < lons - 1
    has_down, has_up = lev > 0, lev < levs - 1
    late = lax.rem(lon, 2) == 1

    first = [
        pltpu.make_async_copy(
            dens.at[place(1, rows), :, pl.ds(at, span)],
            field.at[0, 1, pl.ds(1, cols), pl.ds(PAD + at, span)],
            edge_sem.at[k])
        for k, (at, span) in enumerate(opening)
    ]
    loads = []
    for r in range(1, rows + 1):
        if r > 1:
            loads.append(pltpu.make_async_copy(
                dens.at[place(r, rows)],
                field.at[0, r, pl.ds(1, cols), pl.ds(PAD, deep)],
                load_sem.at[0, r - 1]))
        loads.append(pltpu.make_async_copy(
            crowd.at[place(r, rows)], cap.at[r - 1], load_sem.at[1, r - 1]))

    barrier = pltpu.get_barrier_semaphore()
    signal(barrier, {"lat": 1 - lat})
    for j in range(1, lons):
        signal(barrier, {"lon": lax.rem(lon + j, lons)})
    if levs > 1:
        pl.when(has_down)(lambda: signal(barrier, {"lev": lev - 1}))
        pl.when(has_up)(lambda: signal(barrier, {"lev": lev + 1}))
    for copy in first + loads:
        copy.start()
    pl.semaphore_wait(barrier, lons + has_down.astype(jnp.int32) + has_up.astype(jnp.int32))

    def chunks(t):
        return opening if t == 0 else fine if t == STEPS - 1 else coarse

    def face(t, k):
        at, span = chunks(t)[k]
        return pltpu.make_async_remote_copy(
            src_ref=field.at[t, 1, pl.ds(1, cols), pl.ds(PAD + at, span)],
            dst_ref=field.at[t, 0, pl.ds(1, cols), pl.ds(PAD + at, span)],
            send_sem=face_send.at[t, k],
            recv_sem=face_recv.at[t, k],
            device_id={"lat": 1 - lat},
            device_id_type=MESH,
        )

    bands = (pl.ds(1, 1), pl.ds(2, rows - 1))

    def lon_side(t, band, right):
        own, theirs = (cols, 0) if right else (1, cols + 1)
        span = bands[band]
        return pltpu.make_async_remote_copy(
            src_ref=field.at[t, span, own, pl.ds(PAD, deep)],
            dst_ref=field.at[t, span, theirs, pl.ds(PAD, deep)],
            send_sem=lon_send.at[t, band, int(right)],
            recv_sem=lon_recv.at[t, band, int(right)],
            device_id={"lon": lon + 1 if right else lon - 1},
            device_id_type=MESH,
        )

    def lev_side(t, band, up):
        own, theirs = (PAD + deep - 1, PAD - 1) if up else (PAD, PAD + deep)
        span = (bands[band], pl.ds(1, cols))
        return pltpu.make_async_remote_copy(
            src_ref=field.at[t, span[0], span[1], pl.ds(own, 1)],
            dst_ref=field.at[t, span[0], span[1], pl.ds(theirs, 1)],
            send_sem=lev_send.at[t, band, int(up)],
            recv_sem=lev_recv.at[t, band, int(up)],
            device_id={"lev": lev + 1 if up else lev - 1},
            device_id_type=MESH,
        )

    def sides(t, band, act):
        if lons > 1:
            pl.when(has_right)(lambda: act(lon_side(t, band, True)))
            pl.when(has_left)(lambda: act(lon_side(t, band, False)))
        if levs > 1:
            pl.when(has_up)(lambda: act(lev_side(t, band, True)))
            pl.when(has_down)(lambda: act(lev_side(t, band, False)))

    def start_sides(t, band):
        sides(t, band, lambda copy: copy.start())

    def wait_sides_sent(t, band):
        sides(t, band, lambda copy: copy.wait_send())

    def wait_sides(t, band):
        if lons > 1:
            pl.when(has_left)(lambda: lon_side(t, band, True).wait_recv())
            pl.when(has_right)(lambda: lon_side(t, band, False).wait_recv())
        if levs > 1:
            pl.when(has_down)(lambda: lev_side(t, band, True).wait_recv())
            pl.when(has_up)(lambda: lev_side(t, band, False).wait_recv())

    stat_rows = (pl.ds(0, 1), pl.ds(1, rows - 2))
    groups = range(2 if rows > 2 else 1)

    def stat(group, j):
        return pltpu.make_async_remote_copy(
            src_ref=stats.at[stat_rows[group]],
            dst_ref=peers.at[j - 1, stat_rows[group]],
            send_sem=stat_send.at[group, j - 1],
            recv_sem=stat_recv.at[group, j - 1],
            device_id={"lon": lax.rem(lon + j, lons)},
            device_id_type=MESH,
        )

    for k in range(len(opening)):
        first[k].wait()
        face(0, k).start()

    def clear_cols(at):
        for t in range(STEPS):
            def row(i, _, t=t):
                field[t, i, at, pl.ds(PAD, deep)] = jnp.zeros((deep, lanes), jnp.float32)
                return 0
            lax.fori_loop(1, rows + 1, row, 0)

    def clear_level(at):
        for t in range(STEPS):
            def row(i, _, t=t):
                def col(c, _):
                    field[t, i, c, pl.ds(at, PAD)] = jnp.zeros((PAD, lanes), jnp.float32)
                    return 0
                return lax.fori_loop(1, cols + 1, col, 0)
            lax.fori_loop(1, rows + 1, row, 0)

    pl.when(jnp.logical_not(has_left))(lambda: clear_cols(0))
    pl.when(jnp.logical_not(has_right))(lambda: clear_cols(cols + 1))
    pl.when(jnp.logical_not(has_down))(lambda: clear_level(0))
    pl.when(jnp.logical_not(has_up))(lambda: clear_level(PAD + deep))

    for copy in loads:
        copy.wait()
    start_sides(0, 1)
    start_sides(0, 0)

    def cell(t, r, c, at, span, below, above):
        here = field[t, r, c, pl.ds(PAD + at, span)]
        near = (field[t, r, c - 1, pl.ds(PAD + at, span)] + field[t, r, c + 1, pl.ds(PAD + at, span)])
        near += (field[t, r, c, pl.ds(PAD - 1 + at, span)] + field[t, r, c, pl.ds(PAD + 1 + at, span)])
        if below:
            near += field[t, r - 1, c, pl.ds(PAD + at, span)]
        if above:
            near += field[t, r + 1, c, pl.ds(PAD + at, span)]
        limit = cap[r - 1, c - 1, pl.ds(at, span)]
        return here * (0.6 - 0.2 * (here * limit)) + 0.1 * near

    def advance_row(t, r, at, span, last):
        def col(c, _):
            value = cell(t, r, c, at, span, True, not last)
            field[t + 1, r, c, pl.ds(PAD + at, span)] = value
            if t == STEPS - 2 and isinstance(r, int) and r == 1:
                front[c - 1, pl.ds(at, span)] = value
            return 0
        lax.fori_loop(1, cols + 1, col, 0)

    def start_face(t, k):
        if t < STEPS - 1 or k == 0:
            face(t, k).start()
        elif k == 1:
            pl.when(late)(lambda: face(t, k).start())

    def finish(r, at, last):
        values = [cell(STEPS - 1, r, c, at, 8, True, not last) for c in range(1, cols + 1)]
        for c in range(cols):
            out_dens[r - 2, c, pl.ds(at, 8)] = values[c]
        total, square = line_sums(values)
        stats[r - 2, 0, pl.ds(at, 8)] = total
        stats[r - 2, 1, pl.ds(at, 8)] = square

    def scale(r, at):
        pair = [(stats[r - 2, 0, pl.ds(at, 8)], stats[r - 2, 1, pl.ds(at, 8)])]
        for j in range(lons - 1):
            pair.append((peers[j, r - 2, 0, pl.ds(at, 8)], peers[j, r - 2, 1, pl.ds(at, 8)]))
        mean, gain = line_scale(pair, cols)
        for c in range(cols):
            out_scaled[r - 2, c, pl.ds(at, 8)] = (out_dens[r - 2, c, pl.ds(at, 8)] - mean) * gain

    def each_row(first, last, act):
        def row(r, _):
            tiles(0, deep, lambda at: act(r, at))
            return 0
        lax.fori_loop(first, last, row, 0)

    def send_sums(group):
        for j in range(1, lons):
            stat(group, j).start()

    def wait_sums(group):
        for j in range(1, lons):
            stat(group, j).wait_recv()

    for t in range(STEPS - 1):
        wait_sides(t, 1)

        def inner(r, _, t=t):
            advance_row(t, r, 0, deep, False)
            return 0

        lax.fori_loop(2, rows, inner, 0)
        advance_row(t, rows, 0, deep, True)
        start_sides(t + 1, 1)
        if t == STEPS - 2:
            wait_sides(t + 1, 1)
            if rows > 2:
                each_row(3, rows, lambda r, at: finish(r, at, False))
                tiles(0, deep, lambda at: finish(rows, at, True))
                send_sums(1)
                wait_sums(1)
                each_row(3, rows + 1, scale)
        wait_sides(t, 0)
        for k, (at, span) in enumerate(chunks(t)):
            face(t, k).wait_recv()
            advance_row(t, 1, at, span, False)
            for j, chunk in enumerate(chunks(t + 1)):
                if at < sum(chunk) <= at + span:
                    start_face(t + 1, j)
        start_sides(t + 1, 0)

    t = STEPS - 1
    tiles(0, deep, lambda at: finish(2, at, rows == 2))
    send_sums(0)
    wait_sides(t, 0)

    def base(c, _):
        edge[c - 1] = cell(t, 1, c, 0, deep, False, True)
        return 0

    lax.fori_loop(1, cols + 1, base, 0)
    wait_sums(0)
    tiles(0, deep, lambda at: scale(2, at))

    def add_face(k):
        at, span = fine[k]
        face(t, k).wait_recv()

        def col(c, _):
            edge[c, pl.ds(at, span)] += 0.1 * field[t, 0, c + 1, pl.ds(PAD + at, span)]
            return 0
        lax.fori_loop(0, cols, col, 0)

    for s in range(STEPS - 1):
        for k in range(len(chunks(s))):
            face(s, k).wait_send()
    for s in range(STEPS):
        for band in range(2):
            wait_sides_sent(s, band)
    for group in groups:
        for j in range(1, lons):
            stat(group, j).wait_send()
    add_face(0)
    face(t, 0).wait_send()

    @pl.when(late)
    def _():
        add_face(1)
        face(t, 1).wait_send()


def write_inner(scaled, dens, edge, out_scaled, out_dens, token, sems):
    inner, cols, _, _ = scaled.shape
    copies = []
    for i, (src, dst) in enumerate(((scaled, out_scaled), (dens, out_dens))):
        for r in range(inner):
            copies.append(pltpu.make_async_copy(
                src.at[r], dst.at[place(r + 2, inner + 1)], sems.at[i, r]))
    copies.append(pltpu.make_async_copy(edge, out_dens.at[place(1, inner + 1)], sems.at[1, inner]))
    for copy in copies:
        copy.start()
    token[...] = jnp.zeros(token.shape, jnp.float32)
    for copy in copies:
        copy.wait()


def last_row(lons, edge, front, token, out_scaled, out_dens, *refs):
    twin = lons == 2
    tile_base, tile_face, tile_sums = refs[:3] if twin else (None,) * 3
    (other, stats, peers, entered, face_send, face_recv, stat_send, stat_recv,
     tile_send, tile_recv) = refs[3:] if twin else refs
    cols, deep, lanes = edge.shape
    _, _, fine = split(deep)
    end = len(fine) - 1
    spans = [(0, sum(fine[1]))] + fine[2:]
    tail = pl.ds(*fine[end])
    lat, lon = lax.axis_index("lat"), lax.axis_index("lon")
    late = lax.rem(lon, 2) == 1
    early = jnp.logical_not(late)

    def ahead(there):
        return lax.rem(there, 2) * lons + there < lax.rem(lon, 2) * lons + lon

    barrier = pltpu.get_barrier_semaphore()
    signal(barrier, {"lat": 1 - lat})
    before = 0
    for j in range(1, lons):
        there = lax.rem(lon + j, lons)
        before += ahead(there).astype(jnp.int32)

        @pl.when(jnp.logical_not(ahead(there)))
        def _():
            signal(barrier, {"lon": there})
            if twin:
                signal(barrier, {"lat": 1 - lat, "lon": there})
    pl.semaphore_wait(barrier, 1 + before * (2 if twin else 1))

    def remote(src, dst, send, recv, where):
        return pltpu.make_async_remote_copy(
            src_ref=src, dst_ref=dst, send_sem=send, recv_sem=recv,
            device_id=where, device_id_type=MESH)

    def face(k):
        pick = (slice(None), pl.ds(*fine[k]))
        return remote(front.at[pick], other.at[pick], face_send.at[k], face_recv.at[k],
                      {"lat": 1 - lat})

    def tile_copy(i):
        src = (front, front, edge, stats)[i].at[:, tail]
        dst = (tile_face, tile_face, tile_base, tile_sums)[i]
        where = {"lat": 1 - lat} if i < 2 else {}
        if i > 0:
            where["lon"] = 1 - lon
        return remote(src, dst, tile_send.at[i], tile_recv.at[i], where)

    def stat(part, j):
        pick = (slice(None), pl.ds(*spans[part]))
        return remote(stats.at[pick], peers.at[(j - 1,) + pick],
                      stat_send.at[part, j - 1], stat_recv.at[part, j - 1],
                      {"lon": lax.rem(lon + j, lons)})

    def each_stat(part, act):
        for j in range(1, lons):
            act(stat(part, j))

    @pl.when(early)
    def _():
        for k in range(1, end + 1):
            face(k).start()

    @pl.when(late)
    def _():
        for k in range(2, end if twin else end + 1):
            face(k).start()
        if twin:
            for i in (1, 0, 2):
                tile_copy(i).start()

    for j in range(1, lons):
        there = lax.rem(lon + j, lons)
        pl.when(ahead(there))(lambda: signal(entered, {"lon": there}))

    def finish(at, add):
        values = [edge[c, pl.ds(at, 8)] for c in range(cols)]
        if add:
            values = [v + 0.1 * other[c, pl.ds(at, 8)] for c, v in enumerate(values)]
        for c in range(cols):
            out_dens[c, pl.ds(at, 8)] = values[c]
        total, square = line_sums(values)
        stats[0, pl.ds(at, 8)] = total
        stats[1, pl.ds(at, 8)] = square

    def scale(at):
        pair = [(stats[0, pl.ds(at, 8)], stats[1, pl.ds(at, 8)])]
        for j in range(lons - 1):
            pair.append((peers[j, 0, pl.ds(at, 8)], peers[j, 1, pl.ds(at, 8)]))
        mean, gain = line_scale(pair, cols)
        for c in range(cols):
            out_scaled[c, pl.ds(at, 8)] = (out_dens[c, pl.ds(at, 8)] - mean) * gain

    def land(k):
        face(k).wait_recv()
        tiles(*fine[k], lambda at: finish(at, True))

    tiles(*fine[0], lambda at: finish(at, False))
    pl.when(late)(lambda: tiles(*fine[1], lambda at: finish(at, False)))
    pl.when(early)(lambda: land(1))
    pl.when(before < lons - 1)(lambda: pl.semaphore_wait(entered, lons - 1 - before))
    each_stat(0, lambda copy: copy.start())
    land(2)
    each_stat(1, lambda copy: copy.start())
    each_stat(0, lambda copy: copy.wait_recv())
    tiles(*spans[0], scale)
    if twin:
        @pl.when(early)
        def _():
            land(end)
            tile_copy(3).start()
            tile_sums[...] = stats[:, tail]
    else:
        land(end)
        each_stat(2, lambda copy: copy.start())
    each_stat(1, lambda copy: copy.wait_recv())
    tiles(*spans[1], scale)

    face(2).wait_send()
    for part in range(2):
        each_stat(part, lambda copy: copy.wait_send())
    if twin:
        @pl.when(early)
        def _():
            face(1).wait_send()
            face(end).wait_send()
            tile_copy(3).wait_send()
            tile_copy(2).wait_recv()
            tile_copy(1).wait_recv()

        @pl.when(late)
        def _():
            tile_base[...] = edge[:, tail]
            for i in range(3):
                tile_copy(i).wait_send()
            tile_copy(3).wait_recv()
            tile_copy(0).wait_recv()
    else:
        pl.when(early)(lambda: face(1).wait_send())
        face(end).wait_send()
        each_stat(2, lambda copy: copy.wait_recv())
        tiles(*spans[2], scale)
        each_stat(2, lambda copy: copy.wait_send())


def write_last(lons, scaled, dens, *refs):
    twin = lons == 2
    if twin:
        tile_base, tile_face, tile_sums, _, _, out_scaled, out_dens, sems = refs[:8]
        own_scaled, own_dens, tile_sem = refs[8:]
    else:
        _, _, out_scaled, out_dens, sems = refs
    rows, many = out_dens.shape[0], sems.shape[1]
    cols, deep, _ = dens.shape
    _, _, fine = split(deep)
    last = fine[-1][0]
    late = lax.rem(lax.axis_index("lon"), 2)

    def copies(src, dst, i, begin, end):
        step, span = cols // many, pl.ds(begin, end - begin)
        return [
            pltpu.make_async_copy(
                src.at[pl.ds(part * step, step), span],
                dst.at[place(1, rows), pl.ds(part * step, step), span],
                sems.at[i, part])
            for part in range(many)
        ]

    def each(act):
        for copy in copies(scaled, out_scaled, 0, 0, last if twin else deep):
            act(copy)
        for moved in range(2):
            @pl.when(late == moved)
            def _():
                stop = last if twin and moved else deep
                for copy in copies(dens, out_dens, 1, sum(fine[moved]), stop):
                    act(copy)

    def tile_out(i):
        src, dst = ((own_scaled, out_scaled), (own_dens, out_dens))[i]
        return pltpu.make_async_copy(
            src, dst.at[place(1, rows), :, pl.ds(last, 8)], tile_sem.at[i])

    each(lambda copy: copy.start())
    if twin:
        values = [tile_base[c] + 0.1 * tile_face[c] for c in range(cols)]
        mean, gain = line_scale([line_sums(values), (tile_sums[0], tile_sums[1])], cols)

        @pl.when(late == 1)
        def _():
            for c in range(cols):
                own_dens[c] = values[c]
                own_scaled[c] = (values[c] - mean) * gain
            tile_out(1).start()

        @pl.when(late == 0)
        def _():
            for c in range(cols):
                own_scaled[c] = (dens[c, pl.ds(last, 8)] - mean) * gain

        tile_out(0).start()
        pl.when(late == 1)(lambda: tile_out(1).wait())
        tile_out(0).wait()
    each(lambda copy: copy.wait())


def in_vmem(*arrays):
    return [pltpu.with_memory_space_constraint(a, pltpu.VMEM) for a in arrays]


def all_steps(lons, levs, density, crowding):
    rows, cols, deep, lanes = density.shape
    opening, coarse, fine = split(deep)
    sem = pltpu.SemaphoreType.DMA
    peers = max(lons - 1, 1)
    inner = pltpu.VMEM((rows - 1, cols, deep, lanes), jnp.float32)
    row = pltpu.VMEM((cols, deep, lanes), jnp.float32)
    any_space = pl.BlockSpec(memory_space=pl.ANY)
    vmem = pl.BlockSpec(memory_space=pltpu.VMEM)
    scaled, dens, edge, front = pl.pallas_call(
        functools.partial(kernel, lons, levs),
        out_shape=(inner, inner, row, row),
        in_specs=[any_space] * 2,
        out_specs=[vmem] * 4,
        scratch_shapes=[
            pltpu.VMEM((STEPS, rows + 1, cols + 2, deep + 2 * PAD, lanes), jnp.float32),
            pltpu.VMEM((rows, cols, deep, lanes), jnp.float32),
            pltpu.VMEM((rows - 1, 2, deep, lanes), jnp.float32),
            pltpu.VMEM((peers, rows - 1, 2, deep, lanes), jnp.float32),
            sem((2, rows)),
            sem((len(opening),)),
            sem((STEPS, len(fine))),
            sem((STEPS, len(fine))),
            sem((STEPS, 2, 2)),
            sem((STEPS, 2, 2)),
            sem((STEPS, 2, 2)),
            sem((STEPS, 2, 2)),
            sem((2, peers)),
            sem((2, peers)),
        ],
        compiler_params=pltpu.CompilerParams(
            collective_id=0, has_side_effects=True, vmem_limit_bytes=VMEM_LIMIT
        ),
    )(density, crowding)

    out = jax.ShapeDtypeStruct(density.shape, density.dtype)
    out_scaled, out_dens, token = pl.pallas_call(
        write_inner,
        out_shape=(out, out, pltpu.VMEM((8, lanes), jnp.float32)),
        in_specs=[vmem] * 3,
        out_specs=[pl.BlockSpec(memory_space=pltpu.HBM)] * 2 + [vmem],
        scratch_shapes=[sem((2, rows))],
        compiler_params=pltpu.CompilerParams(vmem_limit_bytes=2**20),
    )(*in_vmem(scaled, dens, edge))

    twin = lons == 2
    tile = pltpu.VMEM((cols, 8, lanes), jnp.float32)
    extra = (tile, tile, pltpu.VMEM((2, 8, lanes), jnp.float32)) if twin else ()
    row_parts = pl.pallas_call(
        functools.partial(last_row, lons),
        out_shape=(row, row) + extra,
        in_specs=[vmem] * 3,
        out_specs=[vmem] * (2 + len(extra)),
        scratch_shapes=[
            pltpu.VMEM((cols, deep, lanes), jnp.float32),
            pltpu.VMEM((2, deep, lanes), jnp.float32),
            pltpu.VMEM((peers, 2, deep, lanes), jnp.float32),
            pltpu.SemaphoreType.REGULAR,
            sem((len(fine),)),
            sem((len(fine),)),
            sem((len(fine) - 1, peers)),
            sem((len(fine) - 1, peers)),
            sem((4,)),
            sem((4,)),
        ],
        compiler_params=pltpu.CompilerParams(
            collective_id=1, has_side_effects=True, vmem_limit_bytes=8 * 2**20
        ),
    )(*in_vmem(edge, front, token))

    hbm = pl.BlockSpec(memory_space=pltpu.HBM)
    known = len(row_parts)
    return pl.pallas_call(
        functools.partial(write_last, lons),
        out_shape=(out, out),
        in_specs=[vmem] * known + [hbm] * 2,
        out_specs=[hbm] * 2,
        input_output_aliases={known: 0, known + 1: 1},
        scratch_shapes=[sem((2, 4 if cols % 4 == 0 else 1))] + ([tile, tile, sem((2,))] if twin else []),
        compiler_params=pltpu.CompilerParams(vmem_limit_bytes=2**20),
    )(*in_vmem(*row_parts), out_scaled, out_dens)


VMEM_LIMIT = 44 * 2**20


def solution(mesh):
    lats, lons, levs = mesh.shape["lat"], mesh.shape["lon"], mesh.shape["lev"]

    def shards(density, crowding):
        rows, cols, deep, lanes = density.shape
        words = lanes * (
            STEPS * (rows + 1) * (cols + 2) * (deep + 2 * PAD)
            + 3 * rows * cols * deep
            + 2 * lons * rows * deep
        )
        fits = lats == 2 and rows > 1 and lanes == 128 and deep % 32 == 0 and 4 * words < VMEM_LIMIT
        if fits:
            return tuple(all_steps(lons, levs, density, crowding))
        return general(density, crowding)

    spec = P(("trial", "lat"), "lon", "lev", None)
    return jax.shard_map(
        shards, mesh=mesh, in_specs=(spec, spec), out_specs=(spec, spec), check_vma=False
    )
```

```python
import functools

import jax
import jax.numpy as jnp
from jax import lax
from jax.experimental import pallas as pl
from jax.experimental.pallas import tpu as pltpu
from jax.sharding import PartitionSpec as P

STEPS = 4
PAD = 8
MESH = pl.DeviceIdType.MESH


def with_halo(cells, sides, width):
    for axis, dim in sides:
        count = lax.axis_size(axis)
        ends = count - 1
        head = lax.slice_in_dim(cells, 0, width, axis=dim)
        tail = lax.slice_in_dim(cells, cells.shape[dim] - width, cells.shape[dim], axis=dim)
        cells = jnp.concatenate(
            [
                lax.ppermute(tail, axis, [(i, (i + 1) % count) for i in range(ends)]),
                cells,
                lax.ppermute(head, axis, [((i + 1) % count, i) for i in range(ends)]),
            ],
            axis=dim,
        )
    return cells


def inner_cells(values, dims):
    for dim in dims:
        values = lax.slice_in_dim(values, 1, values.shape[dim] - 1, axis=dim)
    return values


def side_cells(values, dim, start, dims):
    others = [other for other in dims if other != dim]
    values = inner_cells(values, others)
    return lax.slice_in_dim(values, start, start + values.shape[dim] - 2, axis=dim)


def advance(padded, crowding):
    middle = inner_cells(padded, (0, 1, 2))
    lower = [side_cells(padded, dim, 0, (0, 1, 2)) for dim in (0, 1, 2)]
    upper = [side_cells(padded, dim, 2, (0, 1, 2)) for dim in (0, 1, 2)]
    spread = lower[0] + upper[0] + lower[1] + upper[1] + lower[2] + upper[2] - 6.0 * middle
    return middle + 0.1 * spread + 0.2 * middle * (1.0 - middle * crowding)


def general(density, crowding):
    for step in range(STEPS):
        padded = with_halo(density, (("lat", 0), ("lon", 1), ("lev", 2)), 1)
        density = advance(padded, crowding)
    count = density.shape[1] * lax.axis_size("lon")
    moved = density - 1.0
    totals, squares = lax.psum(
        (jnp.sum(moved, axis=1, keepdims=True), jnp.sum(moved * moved, axis=1, keepdims=True)),
        "lon",
    )
    line_mean = 1.0 + totals / count
    centred = density - line_mean
    line_variance = squares / count - totals / count * (totals / count)
    return (centred * lax.rsqrt(line_variance + 0.0001), density)


def tree_sum(terms):
    terms = list(terms)
    while len(terms) > 1:
        terms = [sum(terms[i : i + 2][1:], terms[i]) for i in range(0, len(terms), 2)]
    return terms[0]


def signal(sem, where):
    pl.semaphore_signal(sem, inc=1, device_id=where, device_id_type=MESH)


def split(deep):
    half, last = deep // 2, deep - 8
    first, late = max(8, deep // 32 * 8), max(8, deep // 64 * 8)
    opening = [(0, 8), (8, half - 8), (half, half)]
    coarse = [(0, half), (half, half)]
    fine = [(0, first), (first, last - late - first), (last - late, late), (last, 8)]
    return opening, coarse, fine


def place(r, rows):
    lat = lax.axis_index("lat")
    return (1 - lat) * (rows - r) + lat * (r - 1)


def tiles(first, many, act):
    def tile(i, _):
        act(pl.multiple_of(i * 8, 8))
        return 0
    lax.fori_loop(first // 8, (first + many) // 8, tile, 0)


def line_sums(values):
    cols = len(values)
    total = tree_sum(values)
    mean = total * (1.0 / cols)
    return total, tree_sum([(v - mean) * (v - mean) for v in values])


def line_scale(pair, cols):
    count = cols * len(pair)
    mean = tree_sum([p[0] for p in pair]) * (1.0 / count)
    square = tree_sum([p[1] + cols * (p[0] * (1.0 / cols) - mean) ** 2 for p in pair])
    return mean, lax.rsqrt(square * (1.0 / count) + 0.0001)


def kernel(lons, levs, dens, crowd, out_scaled, out_dens, edge, front,
           field, cap, stats, peers, load_sem, edge_sem, face_send, face_recv,
           lon_send, lon_recv, lev_send, lev_recv, stat_send, stat_recv):
    rows, cols, deep, lanes = dens.shape
    opening, coarse, fine = split(deep)
    lat, lon, lev = lax.axis_index("lat"), lax.axis_index("lon"), lax.axis_index("lev")
    has_left, has_right = lon > 0, lon < lons - 1
    has_down, has_up = lev > 0, lev < levs - 1
    late = lax.rem(lon, 2) == 0

    first = [
        pltpu.make_async_copy(
            dens.at[place(1, rows), :, pl.ds(at, span)],
            field.at[0, 1, pl.ds(1, cols), pl.ds(PAD + at, span)],
            edge_sem.at[k])
        for k, (at, span) in enumerate(opening)
    ]
    loads = []
    for r in range(1, rows + 1):
        if r > 1:
            loads.append(pltpu.make_async_copy(
                dens.at[place(r, rows)],
                field.at[0, r, pl.ds(1, cols), pl.ds(PAD, deep)],
                load_sem.at[0, r - 1]))
        loads.append(pltpu.make_async_copy(
            crowd.at[place(r, rows)], cap.at[r - 1], load_sem.at[1, r - 1]))

    barrier = pltpu.get_barrier_semaphore()
    signal(barrier, {"lat": 1 - lat})
    for j in range(1, lons):
        signal(barrier, {"lon": lax.rem(lon + j, lons)})
    if levs > 1:
        pl.when(has_down)(lambda: signal(barrier, {"lev": lev - 1}))
        pl.when(has_up)(lambda: signal(barrier, {"lev": lev + 1}))
    for copy in first + loads:
        copy.start()
    pl.semaphore_wait(barrier, lons + has_down.astype(jnp.int32) + has_up.astype(jnp.int32))

    def chunks(t):
        return opening if t == 0 else fine if t == STEPS - 1 else coarse

    def face(t, k):
        at, span = chunks(t)[k]
        return pltpu.make_async_remote_copy(
            src_ref=field.at[t, 1, pl.ds(1, cols), pl.ds(PAD + at, span)],
            dst_ref=field.at[t, 0, pl.ds(1, cols), pl.ds(PAD + at, span)],
            send_sem=face_send.at[t, k],
            recv_sem=face_recv.at[t, k],
            device_id={"lat": 1 - lat},
            device_id_type=MESH,
        )

    bands = (pl.ds(1, 1), pl.ds(2, rows - 1))

    def lon_side(t, band, right):
        own, theirs = (cols, 0) if right else (1, cols + 1)
        span = bands[band]
        return pltpu.make_async_remote_copy(
            src_ref=field.at[t, span, own, pl.ds(PAD, deep)],
            dst_ref=field.at[t, span, theirs, pl.ds(PAD, deep)],
            send_sem=lon_send.at[t, band, int(right)],
            recv_sem=lon_recv.at[t, band, int(right)],
            device_id={"lon": lon + 1 if right else lon - 1},
            device_id_type=MESH,
        )

    def lev_side(t, band, up):
        own, theirs = (PAD + deep - 1, PAD - 1) if up else (PAD, PAD + deep)
        span = (bands[band], pl.ds(1, cols))
        return pltpu.make_async_remote_copy(
            src_ref=field.at[t, span[0], span[1], pl.ds(own, 1)],
            dst_ref=field.at[t, span[0], span[1], pl.ds(theirs, 1)],
            send_sem=lev_send.at[t, band, int(up)],
            recv_sem=lev_recv.at[t, band, int(up)],
            device_id={"lev": lev + 1 if up else lev - 1},
            device_id_type=MESH,
        )

    def sides(t, band, act):
        if lons > 1:
            pl.when(has_right)(lambda: act(lon_side(t, band, True)))
            pl.when(has_left)(lambda: act(lon_side(t, band, False)))
        if levs > 1:
            pl.when(has_up)(lambda: act(lev_side(t, band, True)))
            pl.when(has_down)(lambda: act(lev_side(t, band, False)))

    def start_sides(t, band):
        sides(t, band, lambda copy: copy.start())

    def wait_sides_sent(t, band):
        sides(t, band, lambda copy: copy.wait_send())

    def wait_sides(t, band):
        if lons > 1:
            pl.when(has_left)(lambda: lon_side(t, band, True).wait_recv())
            pl.when(has_right)(lambda: lon_side(t, band, False).wait_recv())
        if levs > 1:
            pl.when(has_down)(lambda: lev_side(t, band, True).wait_recv())
            pl.when(has_up)(lambda: lev_side(t, band, False).wait_recv())

    stat_rows = (pl.ds(0, 1), pl.ds(1, rows - 2))
    groups = range(2 if rows > 2 else 1)

    def stat(group, j):
        return pltpu.make_async_remote_copy(
            src_ref=stats.at[stat_rows[group]],
            dst_ref=peers.at[j - 1, stat_rows[group]],
            send_sem=stat_send.at[group, j - 1],
            recv_sem=stat_recv.at[group, j - 1],
            device_id={"lon": lax.rem(lon + j, lons)},
            device_id_type=MESH,
        )

    for k in range(len(opening)):
        first[k].wait()
        face(0, k).start()

    def clear_cols(at):
        for t in range(STEPS):
            def row(i, _, t=t):
                field[t, i, at, pl.ds(PAD, deep)] = jnp.zeros((deep, lanes), jnp.float32)
                return 0
            lax.fori_loop(1, rows + 1, row, 0)

    def clear_level(at):
        for t in range(STEPS):
            def row(i, _, t=t):
                def col(c, _):
                    field[t, i, c, pl.ds(at, PAD)] = jnp.zeros((PAD, lanes), jnp.float32)
                    return 0
                return lax.fori_loop(1, cols + 1, col, 0)
            lax.fori_loop(1, rows + 1, row, 0)

    pl.when(jnp.logical_not(has_left))(lambda: clear_cols(0))
    pl.when(jnp.logical_not(has_right))(lambda: clear_cols(cols + 1))
    pl.when(jnp.logical_not(has_down))(lambda: clear_level(0))
    pl.when(jnp.logical_not(has_up))(lambda: clear_level(PAD + deep))

    for copy in loads:
        copy.wait()
    start_sides(0, 1)
    start_sides(0, 0)

    def cell(t, r, c, at, span, below, above):
        here = field[t, r, c, pl.ds(PAD + at, span)]
        near = (field[t, r, c - 1, pl.ds(PAD + at, span)] + field[t, r, c + 1, pl.ds(PAD + at, span)])
        near += (field[t, r, c, pl.ds(PAD - 1 + at, span)] + field[t, r, c, pl.ds(PAD + 1 + at, span)])
        if below:
            near += field[t, r - 1, c, pl.ds(PAD + at, span)]
        if above:
            near += field[t, r + 1, c, pl.ds(PAD + at, span)]
        limit = cap[r - 1, c - 1, pl.ds(at, span)]
        return here * (0.6 - 0.2 * (here * limit)) + 0.1 * near

    def advance_row(t, r, at, span, last):
        def col(c, _):
            value = cell(t, r, c, at, span, True, not last)
            field[t + 1, r, c, pl.ds(PAD + at, span)] = value
            if t == STEPS - 2 and isinstance(r, int) and r == 1:
                front[c - 1, pl.ds(at, span)] = value
            return 0
        lax.fori_loop(1, cols + 1, col, 0)

    def start_face(t, k):
        if t < STEPS - 1 or k == 0:
            face(t, k).start()
        elif k == 1:
            pl.when(late)(lambda: face(t, k).start())

    def finish(r, at, last):
        values = [cell(STEPS - 1, r, c, at, 8, True, not last) for c in range(1, cols + 1)]
        for c in range(cols):
            out_dens[r - 2, c, pl.ds(at, 8)] = values[c]
        total, square = line_sums(values)
        stats[r - 2, 0, pl.ds(at, 8)] = total
        stats[r - 2, 1, pl.ds(at, 8)] = square

    def scale(r, at):
        pair = [(stats[r - 2, 0, pl.ds(at, 8)], stats[r - 2, 1, pl.ds(at, 8)])]
        for j in range(lons - 1):
            pair.append((peers[j, r - 2, 0, pl.ds(at, 8)], peers[j, r - 2, 1, pl.ds(at, 8)]))
        mean, gain = line_scale(pair, cols)
        for c in range(cols):
            out_scaled[r - 2, c, pl.ds(at, 8)] = (out_dens[r - 2, c, pl.ds(at, 8)] - mean) * gain

    def each_row(first, last, act):
        def row(r, _):
            tiles(0, deep, lambda at: act(r, at))
            return 0
        lax.fori_loop(first, last, row, 0)

    def send_sums(group):
        for j in range(1, lons):
            stat(group, j).start()

    def wait_sums(group):
        for j in range(1, lons):
            stat(group, j).wait_recv()

    for t in range(STEPS - 1):
        wait_sides(t, 1)

        def inner(r, _, t=t):
            advance_row(t, r, 0, deep, False)
            return 0

        lax.fori_loop(2, rows, inner, 0)
        advance_row(t, rows, 0, deep, True)
        start_sides(t + 1, 1)
        if t == STEPS - 2:
            wait_sides(t + 1, 1)
            if rows > 2:
                each_row(3, rows, lambda r, at: finish(r, at, False))
                tiles(0, deep, lambda at: finish(rows, at, True))
                send_sums(1)
                wait_sums(1)
                each_row(3, rows + 1, scale)
        wait_sides(t, 0)
        for k, (at, span) in enumerate(chunks(t)):
            face(t, k).wait_recv()
            advance_row(t, 1, at, span, False)
            for j, chunk in enumerate(chunks(t + 1)):
                if at < sum(chunk) <= at + span:
                    start_face(t + 1, j)
        start_sides(t + 1, 0)

    t = STEPS - 1
    tiles(0, deep, lambda at: finish(2, at, rows == 2))
    send_sums(0)
    wait_sides(t, 0)

    def base(c, _):
        edge[c - 1] = cell(t, 1, c, 0, deep, False, True)
        return 0

    lax.fori_loop(1, cols + 1, base, 0)
    wait_sums(0)
    tiles(0, deep, lambda at: scale(2, at))

    def add_face(k):
        at, span = fine[k]
        face(t, k).wait_recv()

        def col(c, _):
            edge[c, pl.ds(at, span)] += 0.1 * field[t, 0, c + 1, pl.ds(PAD + at, span)]
            return 0
        lax.fori_loop(0, cols, col, 0)

    for s in range(STEPS - 1):
        for k in range(len(chunks(s))):
            face(s, k).wait_send()
    for s in range(STEPS):
        for band in range(2):
            wait_sides_sent(s, band)
    for group in groups:
        for j in range(1, lons):
            stat(group, j).wait_send()
    add_face(0)
    face(t, 0).wait_send()

    @pl.when(late)
    def _():
        add_face(1)
        face(t, 1).wait_send()


def write_inner(scaled, dens, edge, out_scaled, out_dens, token, sems):
    inner, cols, _, _ = scaled.shape
    copies = []
    for i, (src, dst) in enumerate(((scaled, out_scaled), (dens, out_dens))):
        for r in range(inner):
            copies.append(pltpu.make_async_copy(
                src.at[r], dst.at[place(r + 2, inner + 1)], sems.at[i, r]))
    copies.append(pltpu.make_async_copy(edge, out_dens.at[place(1, inner + 1)], sems.at[1, inner]))
    for copy in copies:
        copy.start()
    token[...] = jnp.zeros(token.shape, jnp.float32)
    for copy in copies:
        copy.wait()


def last_row(lons, edge, front, token, out_scaled, out_dens, *refs):
    twin = lons == 2
    tile_base, tile_face, tile_sums = refs[:3] if twin else (None,) * 3
    (other, stats, peers, entered, face_send, face_recv, stat_send, stat_recv,
     tile_send, tile_recv) = refs[3:] if twin else refs
    cols, deep, lanes = edge.shape
    _, _, fine = split(deep)
    end = len(fine) - 1
    spans = [(0, sum(fine[1]))] + fine[2:]
    tail = pl.ds(*fine[end])
    lat, lon = lax.axis_index("lat"), lax.axis_index("lon")
    late = lax.rem(lon, 2) == 0
    early = jnp.logical_not(late)

    def ahead(there):
        return there - lax.rem(there, 2) * lons < lon - lax.rem(lon, 2) * lons

    barrier = pltpu.get_barrier_semaphore()
    signal(barrier, {"lat": 1 - lat})
    before = 0
    for j in range(1, lons):
        there = lax.rem(lon + j, lons)
        before += ahead(there).astype(jnp.int32)

        @pl.when(jnp.logical_not(ahead(there)))
        def _():
            signal(barrier, {"lon": there})
            if twin:
                signal(barrier, {"lat": 1 - lat, "lon": there})
    pl.semaphore_wait(barrier, 1 + before * (2 if twin else 1))

    def remote(src, dst, send, recv, where):
        return pltpu.make_async_remote_copy(
            src_ref=src, dst_ref=dst, send_sem=send, recv_sem=recv,
            device_id=where, device_id_type=MESH)

    def face(k):
        pick = (slice(None), pl.ds(*fine[k]))
        return remote(front.at[pick], other.at[pick], face_send.at[k], face_recv.at[k],
                      {"lat": 1 - lat})

    def tile_copy(i):
        src = (front, front, edge, stats)[i].at[:, tail]
        dst = (tile_face, tile_face, tile_base, tile_sums)[i]
        where = {"lat": 1 - lat} if i < 2 else {}
        if i > 0:
            where["lon"] = 1 - lon
        return remote(src, dst, tile_send.at[i], tile_recv.at[i], where)

    def stat(part, j):
        pick = (slice(None), pl.ds(*spans[part]))
        return remote(stats.at[pick], peers.at[(j - 1,) + pick],
                      stat_send.at[part, j - 1], stat_recv.at[part, j - 1],
                      {"lon": lax.rem(lon + j, lons)})

    def each_stat(part, act):
        for j in range(1, lons):
            act(stat(part, j))

    @pl.when(early)
    def _():
        for k in range(1, end + 1):
            face(k).start()

    @pl.when(late)
    def _():
        for k in range(2, end if twin else end + 1):
            face(k).start()
        if twin:
            for i in (1, 0, 2):
                tile_copy(i).start()

    for j in range(1, lons):
        there = lax.rem(lon + j, lons)
        pl.when(ahead(there))(lambda: signal(entered, {"lon": there}))

    def finish(at, add):
        values = [edge[c, pl.ds(at, 8)] for c in range(cols)]
        if add:
            values = [v + 0.1 * other[c, pl.ds(at, 8)] for c, v in enumerate(values)]
        for c in range(cols):
            out_dens[c, pl.ds(at, 8)] = values[c]
        total, square = line_sums(values)
        stats[0, pl.ds(at, 8)] = total
        stats[1, pl.ds(at, 8)] = square

    def scale(at):
        pair = [(stats[0, pl.ds(at, 8)], stats[1, pl.ds(at, 8)])]
        for j in range(lons - 1):
            pair.append((peers[j, 0, pl.ds(at, 8)], peers[j, 1, pl.ds(at, 8)]))
        mean, gain = line_scale(pair, cols)
        for c in range(cols):
            out_scaled[c, pl.ds(at, 8)] = (out_dens[c, pl.ds(at, 8)] - mean) * gain

    def land(k):
        face(k).wait_recv()
        tiles(*fine[k], lambda at: finish(at, True))

    tiles(*fine[0], lambda at: finish(at, False))
    pl.when(late)(lambda: tiles(*fine[1], lambda at: finish(at, False)))
    pl.when(early)(lambda: land(1))
    pl.when(before < lons - 1)(lambda: pl.semaphore_wait(entered, lons - 1 - before))
    each_stat(0, lambda copy: copy.start())
    land(2)
    each_stat(1, lambda copy: copy.start())
    each_stat(0, lambda copy: copy.wait_recv())
    tiles(*spans[0], scale)
    if twin:
        @pl.when(early)
        def _():
            land(end)
            tile_copy(3).start()
            tile_sums[...] = stats[:, tail]
    else:
        land(end)
        each_stat(2, lambda copy: copy.start())
    each_stat(1, lambda copy: copy.wait_recv())
    tiles(*spans[1], scale)

    face(2).wait_send()
    for part in range(2):
        each_stat(part, lambda copy: copy.wait_send())
    if twin:
        @pl.when(early)
        def _():
            face(1).wait_send()
            face(end).wait_send()
            tile_copy(3).wait_send()
            tile_copy(2).wait_recv()
            tile_copy(1).wait_recv()

        @pl.when(late)
        def _():
            tile_base[...] = edge[:, tail]
            for i in range(3):
                tile_copy(i).wait_send()
            tile_copy(3).wait_recv()
            tile_copy(0).wait_recv()
    else:
        pl.when(early)(lambda: face(1).wait_send())
        face(end).wait_send()
        each_stat(2, lambda copy: copy.wait_recv())
        tiles(*spans[2], scale)
        each_stat(2, lambda copy: copy.wait_send())


def write_last(lons, scaled, dens, *refs):
    twin = lons == 2
    if twin:
        tile_base, tile_face, tile_sums, _, _, out_scaled, out_dens, sems = refs[:8]
        own_scaled, own_dens, tile_sem = refs[8:]
    else:
        _, _, out_scaled, out_dens, sems = refs
    rows, many = out_dens.shape[0], sems.shape[1]
    cols, deep, _ = dens.shape
    _, _, fine = split(deep)
    last = fine[-1][0]
    late = 1 - lax.rem(lax.axis_index("lon"), 2)

    def copies(src, dst, i, begin, end):
        step, span = cols // many, pl.ds(begin, end - begin)
        return [
            pltpu.make_async_copy(
                src.at[pl.ds(part * step, step), span],
                dst.at[place(1, rows), pl.ds(part * step, step), span],
                sems.at[i, part])
            for part in range(many)
        ]

    def each(act):
        for copy in copies(scaled, out_scaled, 0, 0, last if twin else deep):
            act(copy)
        for moved in range(2):
            @pl.when(late == moved)
            def _():
                stop = last if twin and moved else deep
                for copy in copies(dens, out_dens, 1, sum(fine[moved]), stop):
                    act(copy)

    def tile_out(i):
        src, dst = ((own_scaled, out_scaled), (own_dens, out_dens))[i]
        return pltpu.make_async_copy(
            src, dst.at[place(1, rows), :, pl.ds(last, 8)], tile_sem.at[i])

    each(lambda copy: copy.start())
    if twin:
        values = [tile_base[c] + 0.1 * tile_face[c] for c in range(cols)]
        mean, gain = line_scale([line_sums(values), (tile_sums[0], tile_sums[1])], cols)

        @pl.when(late == 1)
        def _():
            for c in range(cols):
                own_dens[c] = values[c]
                own_scaled[c] = (values[c] - mean) * gain
            tile_out(1).start()

        @pl.when(late == 0)
        def _():
            for c in range(cols):
                own_scaled[c] = (dens[c, pl.ds(last, 8)] - mean) * gain

        tile_out(0).start()
        pl.when(late == 1)(lambda: tile_out(1).wait())
        tile_out(0).wait()
    each(lambda copy: copy.wait())


def in_vmem(*arrays):
    return [pltpu.with_memory_space_constraint(a, pltpu.VMEM) for a in arrays]


def all_steps(lons, levs, density, crowding):
    rows, cols, deep, lanes = density.shape
    opening, coarse, fine = split(deep)
    sem = pltpu.SemaphoreType.DMA
    peers = max(lons - 1, 1)
    inner = pltpu.VMEM((rows - 1, cols, deep, lanes), jnp.float32)
    row = pltpu.VMEM((cols, deep, lanes), jnp.float32)
    any_space = pl.BlockSpec(memory_space=pl.ANY)
    vmem = pl.BlockSpec(memory_space=pltpu.VMEM)
    scaled, dens, edge, front = pl.pallas_call(
        functools.partial(kernel, lons, levs),
        out_shape=(inner, inner, row, row),
        in_specs=[any_space] * 2,
        out_specs=[vmem] * 4,
        scratch_shapes=[
            pltpu.VMEM((STEPS, rows + 1, cols + 2, deep + 2 * PAD, lanes), jnp.float32),
            pltpu.VMEM((rows, cols, deep, lanes), jnp.float32),
            pltpu.VMEM((rows - 1, 2, deep, lanes), jnp.float32),
            pltpu.VMEM((peers, rows - 1, 2, deep, lanes), jnp.float32),
            sem((2, rows)),
            sem((len(opening),)),
            sem((STEPS, len(fine))),
            sem((STEPS, len(fine))),
            sem((STEPS, 2, 2)),
            sem((STEPS, 2, 2)),
            sem((STEPS, 2, 2)),
            sem((STEPS, 2, 2)),
            sem((2, peers)),
            sem((2, peers)),
        ],
        compiler_params=pltpu.CompilerParams(
            collective_id=0, has_side_effects=True, vmem_limit_bytes=VMEM_LIMIT
        ),
    )(density, crowding)

    out = jax.ShapeDtypeStruct(density.shape, density.dtype)
    out_scaled, out_dens, token = pl.pallas_call(
        write_inner,
        out_shape=(out, out, pltpu.VMEM((8, lanes), jnp.float32)),
        in_specs=[vmem] * 3,
        out_specs=[pl.BlockSpec(memory_space=pltpu.HBM)] * 2 + [vmem],
        scratch_shapes=[sem((2, rows))],
        compiler_params=pltpu.CompilerParams(vmem_limit_bytes=2**20),
    )(*in_vmem(scaled, dens, edge))

    twin = lons == 2
    tile = pltpu.VMEM((cols, 8, lanes), jnp.float32)
    extra = (tile, tile, pltpu.VMEM((2, 8, lanes), jnp.float32)) if twin else ()
    row_parts = pl.pallas_call(
        functools.partial(last_row, lons),
        out_shape=(row, row) + extra,
        in_specs=[vmem] * 3,
        out_specs=[vmem] * (2 + len(extra)),
        scratch_shapes=[
            pltpu.VMEM((cols, deep, lanes), jnp.float32),
            pltpu.VMEM((2, deep, lanes), jnp.float32),
            pltpu.VMEM((peers, 2, deep, lanes), jnp.float32),
            pltpu.SemaphoreType.REGULAR,
            sem((len(fine),)),
            sem((len(fine),)),
            sem((len(fine) - 1, peers)),
            sem((len(fine) - 1, peers)),
            sem((4,)),
            sem((4,)),
        ],
        compiler_params=pltpu.CompilerParams(
            collective_id=1, has_side_effects=True, vmem_limit_bytes=8 * 2**20
        ),
    )(*in_vmem(edge, front, token))

    hbm = pl.BlockSpec(memory_space=pltpu.HBM)
    known = len(row_parts)
    return pl.pallas_call(
        functools.partial(write_last, lons),
        out_shape=(out, out),
        in_specs=[vmem] * known + [hbm] * 2,
        out_specs=[hbm] * 2,
        input_output_aliases={known: 0, known + 1: 1},
        scratch_shapes=[sem((2, 4 if cols % 4 == 0 else 1))] + ([tile, tile, sem((2,))] if twin else []),
        compiler_params=pltpu.CompilerParams(vmem_limit_bytes=2**20),
    )(*in_vmem(*row_parts), out_scaled, out_dens)


VMEM_LIMIT = 44 * 2**20


def solution(mesh):
    lats, lons, levs = mesh.shape["lat"], mesh.shape["lon"], mesh.shape["lev"]

    def shards(density, crowding):
        rows, cols, deep, lanes = density.shape
        words = lanes * (
            STEPS * (rows + 1) * (cols + 2) * (deep + 2 * PAD)
            + 3 * rows * cols * deep
            + 2 * lons * rows * deep
        )
        fits = lats == 2 and rows > 1 and lanes == 128 and deep % 32 == 0 and 4 * words < VMEM_LIMIT
        if fits:
            return tuple(all_steps(lons, levs, density, crowding))
        return general(density, crowding)

    spec = P(("trial", "lat"), "lon", "lev", None)
    return jax.shard_map(
        shards, mesh=mesh, in_specs=(spec, spec), out_specs=(spec, spec), check_vma=False
    )
```

```python
import functools

import jax
import jax.numpy as jnp
from jax import lax
from jax.experimental import pallas as pl
from jax.experimental.pallas import tpu as pltpu
from jax.sharding import PartitionSpec as P

STEPS = 4
PAD = 8
MESH = pl.DeviceIdType.MESH


def with_halo(cells, sides, width):
    for axis, dim in sides:
        count = lax.axis_size(axis)
        ends = count - 1
        head = lax.slice_in_dim(cells, 0, width, axis=dim)
        tail = lax.slice_in_dim(cells, cells.shape[dim] - width, cells.shape[dim], axis=dim)
        cells = jnp.concatenate(
            [
                lax.ppermute(tail, axis, [(i, (i + 1) % count) for i in range(ends)]),
                cells,
                lax.ppermute(head, axis, [((i + 1) % count, i) for i in range(ends)]),
            ],
            axis=dim,
        )
    return cells


def inner_cells(values, dims):
    for dim in dims:
        values = lax.slice_in_dim(values, 1, values.shape[dim] - 1, axis=dim)
    return values


def side_cells(values, dim, start, dims):
    others = [other for other in dims if other != dim]
    values = inner_cells(values, others)
    return lax.slice_in_dim(values, start, start + values.shape[dim] - 2, axis=dim)


def advance(padded, crowding):
    middle = inner_cells(padded, (0, 1, 2))
    lower = [side_cells(padded, dim, 0, (0, 1, 2)) for dim in (0, 1, 2)]
    upper = [side_cells(padded, dim, 2, (0, 1, 2)) for dim in (0, 1, 2)]
    spread = lower[0] + upper[0] + lower[1] + upper[1] + lower[2] + upper[2] - 6.0 * middle
    return middle + 0.1 * spread + 0.2 * middle * (1.0 - middle * crowding)


def general(density, crowding):
    for step in range(STEPS):
        padded = with_halo(density, (("lat", 0), ("lon", 1), ("lev", 2)), 1)
        density = advance(padded, crowding)
    count = density.shape[1] * lax.axis_size("lon")
    moved = density - 1.0
    totals, squares = lax.psum(
        (jnp.sum(moved, axis=1, keepdims=True), jnp.sum(moved * moved, axis=1, keepdims=True)),
        "lon",
    )
    line_mean = 1.0 + totals / count
    centred = density - line_mean
    line_variance = squares / count - totals / count * (totals / count)
    return (centred * lax.rsqrt(line_variance + 0.0001), density)


def tree_sum(terms):
    terms = list(terms)
    while len(terms) > 1:
        terms = [sum(terms[i : i + 2][1:], terms[i]) for i in range(0, len(terms), 2)]
    return terms[0]


def signal(sem, where):
    pl.semaphore_signal(sem, inc=1, device_id=where, device_id_type=MESH)


def split(deep):
    half, last = deep // 2, deep - 8
    first, late = max(8, deep // 32 * 8), max(8, deep // 64 * 8)
    opening = [(0, 8), (8, half - 8), (half, half)]
    coarse = [(0, half), (half, half)]
    fine = [(0, first), (first, last - late - first), (last - late, late), (last, 8)]
    return opening, coarse, fine


def place(r, rows):
    lat = lax.axis_index("lat")
    return (1 - lat) * (rows - r) + lat * (r - 1)


def tiles(first, many, act):
    def tile(i, _):
        act(pl.multiple_of(i * 8, 8))
        return 0
    lax.fori_loop(first // 8, (first + many) // 8, tile, 0)


def ahead(there, lon, lons):
    return there - lax.rem(there, 2) * lons < lon - lax.rem(lon, 2) * lons


def line_sums(values):
    cols = len(values)
    total = tree_sum(values)
    mean = total * (1.0 / cols)
    return total, tree_sum([(v - mean) * (v - mean) for v in values])


def line_scale(pair, cols):
    count = cols * len(pair)
    mean = tree_sum([p[0] for p in pair]) * (1.0 / count)
    square = tree_sum([p[1] + cols * (p[0] * (1.0 / cols) - mean) ** 2 for p in pair])
    return mean, lax.rsqrt(square * (1.0 / count) + 0.0001)


def kernel(lons, levs, dens, crowd, out_scaled, out_dens, edge, front,
           field, cap, stats, peers, entered, load_sem, edge_sem, face_send, face_recv,
           lon_send, lon_recv, lev_send, lev_recv, stat_send, stat_recv):
    rows, cols, deep, lanes = dens.shape
    opening, coarse, fine = split(deep)
    lat, lon, lev = lax.axis_index("lat"), lax.axis_index("lon"), lax.axis_index("lev")
    has_left, has_right = lon > 0, lon < lons - 1
    has_down, has_up = lev > 0, lev < levs - 1
    late = lax.rem(lon, 2) == 0

    first = [
        pltpu.make_async_copy(
            dens.at[place(1, rows), :, pl.ds(at, span)],
            field.at[0, 1, pl.ds(1, cols), pl.ds(PAD + at, span)],
            edge_sem.at[k])
        for k, (at, span) in enumerate(opening)
    ]
    loads = []
    for r in range(1, rows + 1):
        if r > 1:
            loads.append(pltpu.make_async_copy(
                dens.at[place(r, rows)],
                field.at[0, r, pl.ds(1, cols), pl.ds(PAD, deep)],
                load_sem.at[0, r - 1]))
        loads.append(pltpu.make_async_copy(
            crowd.at[place(r, rows)], cap.at[r - 1], load_sem.at[1, r - 1]))

    barrier = pltpu.get_barrier_semaphore()
    signal(barrier, {"lat": 1 - lat})
    before = 0
    for j in range(1, lons):
        there = lax.rem(lon + j, lons)
        before += ahead(there, lon, lons).astype(jnp.int32)
        pl.when(jnp.logical_not(ahead(there, lon, lons)))(lambda: signal(barrier, {"lon": there}))
    if levs > 1:
        pl.when(has_up)(lambda: signal(barrier, {"lev": lev + 1}))
    for copy in first + loads:
        copy.start()
    pl.semaphore_wait(barrier, 1 + before + has_down.astype(jnp.int32))

    def greet():
        for j in range(1, lons):
            there = lax.rem(lon + j, lons)
            pl.when(ahead(there, lon, lons))(lambda: signal(entered.at[0], {"lon": there}))
        if levs > 1:
            pl.when(has_down)(lambda: signal(entered.at[1], {"lev": lev - 1}))

    def wait_greeted():
        pl.when(before < lons - 1)(lambda: pl.semaphore_wait(entered.at[0], lons - 1 - before))
        if levs > 1:
            pl.when(has_up)(lambda: pl.semaphore_wait(entered.at[1], 1))

    def chunks(t):
        return opening if t == 0 else fine if t == STEPS - 1 else coarse

    def face(t, k):
        at, span = chunks(t)[k]
        return pltpu.make_async_remote_copy(
            src_ref=field.at[t, 1, pl.ds(1, cols), pl.ds(PAD + at, span)],
            dst_ref=field.at[t, 0, pl.ds(1, cols), pl.ds(PAD + at, span)],
            send_sem=face_send.at[t, k],
            recv_sem=face_recv.at[t, k],
            device_id={"lat": 1 - lat},
            device_id_type=MESH,
        )

    bands = (pl.ds(1, 1), pl.ds(2, rows - 1))

    def lon_side(t, band, right):
        own, theirs = (cols, 0) if right else (1, cols + 1)
        span = bands[band]
        return pltpu.make_async_remote_copy(
            src_ref=field.at[t, span, own, pl.ds(PAD, deep)],
            dst_ref=field.at[t, span, theirs, pl.ds(PAD, deep)],
            send_sem=lon_send.at[t, band, int(right)],
            recv_sem=lon_recv.at[t, band, int(right)],
            device_id={"lon": lon + 1 if right else lon - 1},
            device_id_type=MESH,
        )

    def lev_side(t, band, up):
        own, theirs = (PAD + deep - 1, PAD - 1) if up else (PAD, PAD + deep)
        span = (bands[band], pl.ds(1, cols))
        return pltpu.make_async_remote_copy(
            src_ref=field.at[t, span[0], span[1], pl.ds(own, 1)],
            dst_ref=field.at[t, span[0], span[1], pl.ds(theirs, 1)],
            send_sem=lev_send.at[t, band, int(up)],
            recv_sem=lev_recv.at[t, band, int(up)],
            device_id={"lev": lev + 1 if up else lev - 1},
            device_id_type=MESH,
        )

    def sides(t, band, act):
        if lons > 1:
            pl.when(has_right)(lambda: act(lon_side(t, band, True)))
            pl.when(has_left)(lambda: act(lon_side(t, band, False)))
        if levs > 1:
            pl.when(has_up)(lambda: act(lev_side(t, band, True)))
            pl.when(has_down)(lambda: act(lev_side(t, band, False)))

    def start_sides(t, band):
        sides(t, band, lambda copy: copy.start())

    def wait_sides_sent(t, band):
        sides(t, band, lambda copy: copy.wait_send())

    def wait_sides(t, band):
        if lons > 1:
            pl.when(has_left)(lambda: lon_side(t, band, True).wait_recv())
            pl.when(has_right)(lambda: lon_side(t, band, False).wait_recv())
        if levs > 1:
            pl.when(has_down)(lambda: lev_side(t, band, True).wait_recv())
            pl.when(has_up)(lambda: lev_side(t, band, False).wait_recv())

    stat_rows = (pl.ds(0, 1), pl.ds(1, rows - 2))
    groups = range(2 if rows > 2 else 1)

    def stat(group, j):
        return pltpu.make_async_remote_copy(
            src_ref=stats.at[stat_rows[group]],
            dst_ref=peers.at[j - 1, stat_rows[group]],
            send_sem=stat_send.at[group, j - 1],
            recv_sem=stat_recv.at[group, j - 1],
            device_id={"lon": lax.rem(lon + j, lons)},
            device_id_type=MESH,
        )

    for k in range(len(opening)):
        first[k].wait()
        face(0, k).start()
        if k == 0:
            greet()

    def clear_cols(at):
        for t in range(STEPS):
            def row(i, _, t=t):
                field[t, i, at, pl.ds(PAD, deep)] = jnp.zeros((deep, lanes), jnp.float32)
                return 0
            lax.fori_loop(1, rows + 1, row, 0)

    def clear_level(at):
        for t in range(STEPS):
            def row(i, _, t=t):
                def col(c, _):
                    field[t, i, c, pl.ds(at, PAD)] = jnp.zeros((PAD, lanes), jnp.float32)
                    return 0
                return lax.fori_loop(1, cols + 1, col, 0)
            lax.fori_loop(1, rows + 1, row, 0)

    pl.when(jnp.logical_not(has_left))(lambda: clear_cols(0))
    pl.when(jnp.logical_not(has_right))(lambda: clear_cols(cols + 1))
    pl.when(jnp.logical_not(has_down))(lambda: clear_level(0))
    pl.when(jnp.logical_not(has_up))(lambda: clear_level(PAD + deep))

    for copy in loads:
        copy.wait()
    wait_greeted()
    start_sides(0, 1)
    start_sides(0, 0)

    def cell(t, r, c, at, span, below, above):
        here = field[t, r, c, pl.ds(PAD + at, span)]
        near = (field[t, r, c - 1, pl.ds(PAD + at, span)] + field[t, r, c + 1, pl.ds(PAD + at, span)])
        near += (field[t, r, c, pl.ds(PAD - 1 + at, span)] + field[t, r, c, pl.ds(PAD + 1 + at, span)])
        if below:
            near += field[t, r - 1, c, pl.ds(PAD + at, span)]
        if above:
            near += field[t, r + 1, c, pl.ds(PAD + at, span)]
        limit = cap[r - 1, c - 1, pl.ds(at, span)]
        return here * (0.6 - 0.2 * (here * limit)) + 0.1 * near

    def advance_row(t, r, at, span, last):
        def col(c, _):
            value = cell(t, r, c, at, span, True, not last)
            field[t + 1, r, c, pl.ds(PAD + at, span)] = value
            if t == STEPS - 2 and isinstance(r, int) and r == 1:
                front[c - 1, pl.ds(at, span)] = value
            return 0
        lax.fori_loop(1, cols + 1, col, 0)

    def start_face(t, k):
        if t < STEPS - 1 or k == 0:
            face(t, k).start()
        elif k == 1:
            pl.when(late)(lambda: face(t, k).start())

    def finish(r, at, last):
        values = [cell(STEPS - 1, r, c, at, 8, True, not last) for c in range(1, cols + 1)]
        for c in range(cols):
            out_dens[r - 2, c, pl.ds(at, 8)] = values[c]
        total, square = line_sums(values)
        stats[r - 2, 0, pl.ds(at, 8)] = total
        stats[r - 2, 1, pl.ds(at, 8)] = square

    def scale(r, at):
        pair = [(stats[r - 2, 0, pl.ds(at, 8)], stats[r - 2, 1, pl.ds(at, 8)])]
        for j in range(lons - 1):
            pair.append((peers[j, r - 2, 0, pl.ds(at, 8)], peers[j, r - 2, 1, pl.ds(at, 8)]))
        mean, gain = line_scale(pair, cols)
        for c in range(cols):
            out_scaled[r - 2, c, pl.ds(at, 8)] = (out_dens[r - 2, c, pl.ds(at, 8)] - mean) * gain

    def each_row(first, last, act):
        def row(r, _):
            tiles(0, deep, lambda at: act(r, at))
            return 0
        lax.fori_loop(first, last, row, 0)

    def send_sums(group):
        for j in range(1, lons):
            stat(group, j).start()

    def wait_sums(group):
        for j in range(1, lons):
            stat(group, j).wait_recv()

    for t in range(STEPS - 1):
        wait_sides(t, 1)

        def inner(r, _, t=t):
            advance_row(t, r, 0, deep, False)
            return 0

        lax.fori_loop(2, rows, inner, 0)
        advance_row(t, rows, 0, deep, True)
        start_sides(t + 1, 1)
        if t == STEPS - 2:
            wait_sides(t + 1, 1)
            if rows > 2:
                each_row(3, rows, lambda r, at: finish(r, at, False))
                tiles(0, deep, lambda at: finish(rows, at, True))
                send_sums(1)
                wait_sums(1)
                each_row(3, rows + 1, scale)
        wait_sides(t, 0)
        for k, (at, span) in enumerate(chunks(t)):
            face(t, k).wait_recv()
            advance_row(t, 1, at, span, False)
            for j, chunk in enumerate(chunks(t + 1)):
                if at < sum(chunk) <= at + span:
                    start_face(t + 1, j)
        start_sides(t + 1, 0)

    t = STEPS - 1
    tiles(0, deep, lambda at: finish(2, at, rows == 2))
    send_sums(0)
    wait_sides(t, 0)

    def base(c, _):
        edge[c - 1] = cell(t, 1, c, 0, deep, False, True)
        return 0

    lax.fori_loop(1, cols + 1, base, 0)
    wait_sums(0)
    tiles(0, deep, lambda at: scale(2, at))

    def add_face(k):
        at, span = fine[k]
        face(t, k).wait_recv()

        def col(c, _):
            edge[c, pl.ds(at, span)] += 0.1 * field[t, 0, c + 1, pl.ds(PAD + at, span)]
            return 0
        lax.fori_loop(0, cols, col, 0)

    for s in range(STEPS - 1):
        for k in range(len(chunks(s))):
            face(s, k).wait_send()
    for s in range(STEPS):
        for band in range(2):
            wait_sides_sent(s, band)
    for group in groups:
        for j in range(1, lons):
            stat(group, j).wait_send()
    add_face(0)
    face(t, 0).wait_send()

    @pl.when(late)
    def _():
        add_face(1)
        face(t, 1).wait_send()


def write_inner(scaled, dens, edge, out_scaled, out_dens, token, sems):
    inner, cols, _, _ = scaled.shape
    copies = []
    for i, (src, dst) in enumerate(((scaled, out_scaled), (dens, out_dens))):
        for r in range(inner):
            copies.append(pltpu.make_async_copy(
                src.at[r], dst.at[place(r + 2, inner + 1)], sems.at[i, r]))
    copies.append(pltpu.make_async_copy(edge, out_dens.at[place(1, inner + 1)], sems.at[1, inner]))
    for copy in copies:
        copy.start()
    token[...] = jnp.zeros(token.shape, jnp.float32)
    for copy in copies:
        copy.wait()


def last_row(lons, edge, front, token, out_scaled, out_dens, *refs):
    twin = lons == 2
    tile_base, tile_face, tile_sums = refs[:3] if twin else (None,) * 3
    (other, stats, peers, entered, face_send, face_recv, stat_send, stat_recv,
     tile_send, tile_recv) = refs[3:] if twin else refs
    cols, deep, lanes = edge.shape
    _, _, fine = split(deep)
    end = len(fine) - 1
    spans = [(0, sum(fine[1]))] + fine[2:]
    tail = pl.ds(*fine[end])
    lat, lon = lax.axis_index("lat"), lax.axis_index("lon")
    late = lax.rem(lon, 2) == 0
    early = jnp.logical_not(late)

    barrier = pltpu.get_barrier_semaphore()
    signal(barrier, {"lat": 1 - lat})
    before = 0
    for j in range(1, lons):
        there = lax.rem(lon + j, lons)
        before += ahead(there, lon, lons).astype(jnp.int32)

        @pl.when(jnp.logical_not(ahead(there, lon, lons)))
        def _():
            signal(barrier, {"lon": there})
            if twin:
                signal(barrier, {"lat": 1 - lat, "lon": there})
    pl.semaphore_wait(barrier, 1 + before * (2 if twin else 1))

    def remote(src, dst, send, recv, where):
        return pltpu.make_async_remote_copy(
            src_ref=src, dst_ref=dst, send_sem=send, recv_sem=recv,
            device_id=where, device_id_type=MESH)

    def face(k):
        pick = (slice(None), pl.ds(*fine[k]))
        return remote(front.at[pick], other.at[pick], face_send.at[k], face_recv.at[k],
                      {"lat": 1 - lat})

    def tile_copy(i):
        src = (front, front, edge, stats)[i].at[:, tail]
        dst = (tile_face, tile_face, tile_base, tile_sums)[i]
        where = {"lat": 1 - lat} if i < 2 else {}
        if i > 0:
            where["lon"] = 1 - lon
        return remote(src, dst, tile_send.at[i], tile_recv.at[i], where)

    def stat(part, j):
        pick = (slice(None), pl.ds(*spans[part]))
        return remote(stats.at[pick], peers.at[(j - 1,) + pick],
                      stat_send.at[part, j - 1], stat_recv.at[part, j - 1],
                      {"lon": lax.rem(lon + j, lons)})

    def each_stat(part, act):
        for j in range(1, lons):
            act(stat(part, j))

    @pl.when(early)
    def _():
        for k in range(1, end + 1):
            face(k).start()

    @pl.when(late)
    def _():
        for k in range(2, end if twin else end + 1):
            face(k).start()
        if twin:
            for i in (1, 0, 2):
                tile_copy(i).start()

    for j in range(1, lons):
        there = lax.rem(lon + j, lons)
        pl.when(ahead(there, lon, lons))(lambda: signal(entered, {"lon": there}))

    def finish(at, add):
        values = [edge[c, pl.ds(at, 8)] for c in range(cols)]
        if add:
            values = [v + 0.1 * other[c, pl.ds(at, 8)] for c, v in enumerate(values)]
        for c in range(cols):
            out_dens[c, pl.ds(at, 8)] = values[c]
        total, square = line_sums(values)
        stats[0, pl.ds(at, 8)] = total
        stats[1, pl.ds(at, 8)] = square

    def scale(at):
        pair = [(stats[0, pl.ds(at, 8)], stats[1, pl.ds(at, 8)])]
        for j in range(lons - 1):
            pair.append((peers[j, 0, pl.ds(at, 8)], peers[j, 1, pl.ds(at, 8)]))
        mean, gain = line_scale(pair, cols)
        for c in range(cols):
            out_scaled[c, pl.ds(at, 8)] = (out_dens[c, pl.ds(at, 8)] - mean) * gain

    def land(k):
        face(k).wait_recv()
        tiles(*fine[k], lambda at: finish(at, True))

    tiles(*fine[0], lambda at: finish(at, False))
    pl.when(late)(lambda: tiles(*fine[1], lambda at: finish(at, False)))
    pl.when(early)(lambda: land(1))
    pl.when(before < lons - 1)(lambda: pl.semaphore_wait(entered, lons - 1 - before))
    each_stat(0, lambda copy: copy.start())
    land(2)
    each_stat(1, lambda copy: copy.start())
    each_stat(0, lambda copy: copy.wait_recv())
    tiles(*spans[0], scale)
    if twin:
        @pl.when(early)
        def _():
            land(end)
            tile_copy(3).start()
            tile_sums[...] = stats[:, tail]
    else:
        land(end)
        each_stat(2, lambda copy: copy.start())
    each_stat(1, lambda copy: copy.wait_recv())
    tiles(*spans[1], scale)

    face(2).wait_send()
    for part in range(2):
        each_stat(part, lambda copy: copy.wait_send())
    if twin:
        @pl.when(early)
        def _():
            face(1).wait_send()
            face(end).wait_send()
            tile_copy(3).wait_send()
            tile_copy(2).wait_recv()
            tile_copy(1).wait_recv()

        @pl.when(late)
        def _():
            tile_base[...] = edge[:, tail]
            for i in range(3):
                tile_copy(i).wait_send()
            tile_copy(3).wait_recv()
            tile_copy(0).wait_recv()
    else:
        pl.when(early)(lambda: face(1).wait_send())
        face(end).wait_send()
        each_stat(2, lambda copy: copy.wait_recv())
        tiles(*spans[2], scale)
        each_stat(2, lambda copy: copy.wait_send())


def write_last(lons, scaled, dens, *refs):
    twin = lons == 2
    if twin:
        tile_base, tile_face, tile_sums, _, _, out_scaled, out_dens, sems = refs[:8]
        own_scaled, own_dens, tile_sem = refs[8:]
    else:
        _, _, out_scaled, out_dens, sems = refs
    rows, many = out_dens.shape[0], sems.shape[1]
    cols, deep, _ = dens.shape
    _, _, fine = split(deep)
    last = fine[-1][0]
    late = 1 - lax.rem(lax.axis_index("lon"), 2)

    def copies(src, dst, i, begin, end):
        step, span = cols // many, pl.ds(begin, end - begin)
        return [
            pltpu.make_async_copy(
                src.at[pl.ds(part * step, step), span],
                dst.at[place(1, rows), pl.ds(part * step, step), span],
                sems.at[i, part])
            for part in range(many)
        ]

    def each(act):
        for copy in copies(scaled, out_scaled, 0, 0, last if twin else deep):
            act(copy)
        for moved in range(2):
            @pl.when(late == moved)
            def _():
                stop = last if twin and moved else deep
                for copy in copies(dens, out_dens, 1, sum(fine[moved]), stop):
                    act(copy)

    def tile_out(i):
        src, dst = ((own_scaled, out_scaled), (own_dens, out_dens))[i]
        return pltpu.make_async_copy(
            src, dst.at[place(1, rows), :, pl.ds(last, 8)], tile_sem.at[i])

    each(lambda copy: copy.start())
    if twin:
        values = [tile_base[c] + 0.1 * tile_face[c] for c in range(cols)]
        mean, gain = line_scale([line_sums(values), (tile_sums[0], tile_sums[1])], cols)

        @pl.when(late == 1)
        def _():
            for c in range(cols):
                own_dens[c] = values[c]
                own_scaled[c] = (values[c] - mean) * gain
            tile_out(1).start()

        @pl.when(late == 0)
        def _():
            for c in range(cols):
                own_scaled[c] = (dens[c, pl.ds(last, 8)] - mean) * gain

        tile_out(0).start()
        pl.when(late == 1)(lambda: tile_out(1).wait())
        tile_out(0).wait()
    each(lambda copy: copy.wait())


def in_vmem(*arrays):
    return [pltpu.with_memory_space_constraint(a, pltpu.VMEM) for a in arrays]


def all_steps(lons, levs, density, crowding):
    rows, cols, deep, lanes = density.shape
    opening, coarse, fine = split(deep)
    sem = pltpu.SemaphoreType.DMA
    peers = max(lons - 1, 1)
    inner = pltpu.VMEM((rows - 1, cols, deep, lanes), jnp.float32)
    row = pltpu.VMEM((cols, deep, lanes), jnp.float32)
    any_space = pl.BlockSpec(memory_space=pl.ANY)
    vmem = pl.BlockSpec(memory_space=pltpu.VMEM)
    scaled, dens, edge, front = pl.pallas_call(
        functools.partial(kernel, lons, levs),
        out_shape=(inner, inner, row, row),
        in_specs=[any_space] * 2,
        out_specs=[vmem] * 4,
        scratch_shapes=[
            pltpu.VMEM((STEPS, rows + 1, cols + 2, deep + 2 * PAD, lanes), jnp.float32),
            pltpu.VMEM((rows, cols, deep, lanes), jnp.float32),
            pltpu.VMEM((rows - 1, 2, deep, lanes), jnp.float32),
            pltpu.VMEM((peers, rows - 1, 2, deep, lanes), jnp.float32),
            pltpu.SemaphoreType.REGULAR((2,)),
            sem((2, rows)),
            sem((len(opening),)),
            sem((STEPS, len(fine))),
            sem((STEPS, len(fine))),
            sem((STEPS, 2, 2)),
            sem((STEPS, 2, 2)),
            sem((STEPS, 2, 2)),
            sem((STEPS, 2, 2)),
            sem((2, peers)),
            sem((2, peers)),
        ],
        compiler_params=pltpu.CompilerParams(
            collective_id=0, has_side_effects=True, vmem_limit_bytes=VMEM_LIMIT
        ),
    )(density, crowding)

    out = jax.ShapeDtypeStruct(density.shape, density.dtype)
    out_scaled, out_dens, token = pl.pallas_call(
        write_inner,
        out_shape=(out, out, pltpu.VMEM((8, lanes), jnp.float32)),
        in_specs=[vmem] * 3,
        out_specs=[pl.BlockSpec(memory_space=pltpu.HBM)] * 2 + [vmem],
        scratch_shapes=[sem((2, rows))],
        compiler_params=pltpu.CompilerParams(vmem_limit_bytes=2**20),
    )(*in_vmem(scaled, dens, edge))

    twin = lons == 2
    tile = pltpu.VMEM((cols, 8, lanes), jnp.float32)
    extra = (tile, tile, pltpu.VMEM((2, 8, lanes), jnp.float32)) if twin else ()
    row_parts = pl.pallas_call(
        functools.partial(last_row, lons),
        out_shape=(row, row) + extra,
        in_specs=[vmem] * 3,
        out_specs=[vmem] * (2 + len(extra)),
        scratch_shapes=[
            pltpu.VMEM((cols, deep, lanes), jnp.float32),
            pltpu.VMEM((2, deep, lanes), jnp.float32),
            pltpu.VMEM((peers, 2, deep, lanes), jnp.float32),
            pltpu.SemaphoreType.REGULAR,
            sem((len(fine),)),
            sem((len(fine),)),
            sem((len(fine) - 1, peers)),
            sem((len(fine) - 1, peers)),
            sem((4,)),
            sem((4,)),
        ],
        compiler_params=pltpu.CompilerParams(
            collective_id=1, has_side_effects=True, vmem_limit_bytes=8 * 2**20
        ),
    )(*in_vmem(edge, front, token))

    hbm = pl.BlockSpec(memory_space=pltpu.HBM)
    known = len(row_parts)
    return pl.pallas_call(
        functools.partial(write_last, lons),
        out_shape=(out, out),
        in_specs=[vmem] * known + [hbm] * 2,
        out_specs=[hbm] * 2,
        input_output_aliases={known: 0, known + 1: 1},
        scratch_shapes=[sem((2, 4 if cols % 4 == 0 else 1))] + ([tile, tile, sem((2,))] if twin else []),
        compiler_params=pltpu.CompilerParams(vmem_limit_bytes=2**20),
    )(*in_vmem(*row_parts), out_scaled, out_dens)


VMEM_LIMIT = 44 * 2**20


def solution(mesh):
    lats, lons, levs = mesh.shape["lat"], mesh.shape["lon"], mesh.shape["lev"]

    def shards(density, crowding):
        rows, cols, deep, lanes = density.shape
        words = lanes * (
            STEPS * (rows + 1) * (cols + 2) * (deep + 2 * PAD)
            + 3 * rows * cols * deep
            + 2 * lons * rows * deep
        )
        fits = lats == 2 and rows > 1 and lanes == 128 and deep % 32 == 0 and 4 * words < VMEM_LIMIT
        if fits:
            return tuple(all_steps(lons, levs, density, crowding))
        return general(density, crowding)

    spec = P(("trial", "lat"), "lon", "lev", None)
    return jax.shard_map(
        shards, mesh=mesh, in_specs=(spec, spec), out_specs=(spec, spec), check_vma=False
    )
```

```python
import functools

import jax
import jax.numpy as jnp
from jax import lax
from jax.experimental import pallas as pl
from jax.experimental.pallas import tpu as pltpu
from jax.sharding import PartitionSpec as P

STEPS = 4
PAD = 8
MESH = pl.DeviceIdType.MESH


def with_halo(cells, sides, width):
    for axis, dim in sides:
        count = lax.axis_size(axis)
        ends = count - 1
        head = lax.slice_in_dim(cells, 0, width, axis=dim)
        tail = lax.slice_in_dim(cells, cells.shape[dim] - width, cells.shape[dim], axis=dim)
        cells = jnp.concatenate(
            [
                lax.ppermute(tail, axis, [(i, (i + 1) % count) for i in range(ends)]),
                cells,
                lax.ppermute(head, axis, [((i + 1) % count, i) for i in range(ends)]),
            ],
            axis=dim,
        )
    return cells


def inner_cells(values, dims):
    for dim in dims:
        values = lax.slice_in_dim(values, 1, values.shape[dim] - 1, axis=dim)
    return values


def side_cells(values, dim, start, dims):
    others = [other for other in dims if other != dim]
    values = inner_cells(values, others)
    return lax.slice_in_dim(values, start, start + values.shape[dim] - 2, axis=dim)


def advance(padded, crowding):
    middle = inner_cells(padded, (0, 1, 2))
    lower = [side_cells(padded, dim, 0, (0, 1, 2)) for dim in (0, 1, 2)]
    upper = [side_cells(padded, dim, 2, (0, 1, 2)) for dim in (0, 1, 2)]
    spread = lower[0] + upper[0] + lower[1] + upper[1] + lower[2] + upper[2] - 6.0 * middle
    return middle + 0.1 * spread + 0.2 * middle * (1.0 - middle * crowding)


def general(density, crowding):
    for step in range(STEPS):
        padded = with_halo(density, (("lat", 0), ("lon", 1), ("lev", 2)), 1)
        density = advance(padded, crowding)
    count = density.shape[1] * lax.axis_size("lon")
    moved = density - 1.0
    totals, squares = lax.psum(
        (jnp.sum(moved, axis=1, keepdims=True), jnp.sum(moved * moved, axis=1, keepdims=True)),
        "lon",
    )
    line_mean = 1.0 + totals / count
    centred = density - line_mean
    line_variance = squares / count - totals / count * (totals / count)
    return (centred * lax.rsqrt(line_variance + 0.0001), density)


def tree_sum(terms):
    terms = list(terms)
    while len(terms) > 1:
        terms = [sum(terms[i : i + 2][1:], terms[i]) for i in range(0, len(terms), 2)]
    return terms[0]


def signal(sem, where):
    pl.semaphore_signal(sem, inc=1, device_id=where, device_id_type=MESH)


def split(deep):
    half, last = deep // 2, deep - 8
    first, late = max(8, deep // 32 * 8), max(8, deep // 64 * 8)
    opening = [(0, 8), (8, half - 8), (half, half)]
    coarse = [(0, half), (half, half)]
    fine = [(0, first), (first, last - late - first), (last - late, late), (last, 8)]
    return opening, coarse, fine


def place(r, rows):
    lat = lax.axis_index("lat")
    return (1 - lat) * (rows - r) + lat * (r - 1)


def tiles(first, many, act):
    def tile(i, _):
        act(pl.multiple_of(i * 8, 8))
        return 0
    lax.fori_loop(first // 8, (first + many) // 8, tile, 0)


def ahead(there, lon, lons):
    return there - lax.rem(there, 2) * lons < lon - lax.rem(lon, 2) * lons


def line_sums(values):
    cols = len(values)
    total = tree_sum(values)
    mean = total * (1.0 / cols)
    return total, tree_sum([(v - mean) * (v - mean) for v in values])


def line_scale(pair, cols):
    count = cols * len(pair)
    mean = tree_sum([p[0] for p in pair]) * (1.0 / count)
    square = tree_sum([p[1] + cols * (p[0] * (1.0 / cols) - mean) ** 2 for p in pair])
    return mean, lax.rsqrt(square * (1.0 / count) + 0.0001)


def kernel(lons, levs, dens, crowd, out_scaled, out_dens, edge, front,
           field, cap, stats, peers, entered, load_sem, edge_sem, face_send, face_recv,
           lon_send, lon_recv, lev_send, lev_recv, stat_send, stat_recv):
    rows, cols, deep, lanes = dens.shape
    opening, coarse, fine = split(deep)
    lat, lon, lev = lax.axis_index("lat"), lax.axis_index("lon"), lax.axis_index("lev")
    has_left, has_right = lon > 0, lon < lons - 1
    has_down, has_up = lev > 0, lev < levs - 1
    late = lax.rem(lon, 2) == 0

    first = [
        pltpu.make_async_copy(
            dens.at[place(1, rows), :, pl.ds(at, span)],
            field.at[0, 1, pl.ds(1, cols), pl.ds(PAD + at, span)],
            edge_sem.at[k])
        for k, (at, span) in enumerate(opening)
    ]
    loads = []
    for r in range(1, rows + 1):
        if r > 1:
            loads.append(pltpu.make_async_copy(
                dens.at[place(r, rows)],
                field.at[0, r, pl.ds(1, cols), pl.ds(PAD, deep)],
                load_sem.at[0, r - 1]))
        loads.append(pltpu.make_async_copy(
            crowd.at[place(r, rows)], cap.at[r - 1], load_sem.at[1, r - 1]))

    barrier = pltpu.get_barrier_semaphore()
    signal(barrier, {"lat": 1 - lat})
    before = 0
    for j in range(1, lons):
        there = lax.rem(lon + j, lons)
        before += ahead(there, lon, lons).astype(jnp.int32)
        pl.when(jnp.logical_not(ahead(there, lon, lons)))(lambda: signal(barrier, {"lon": there}))
    if levs > 1:
        pl.when(has_up)(lambda: signal(barrier, {"lev": lev + 1}))
    for copy in first + loads:
        copy.start()
    pl.semaphore_wait(barrier, 1 + before + has_down.astype(jnp.int32))

    def greet():
        for j in range(1, lons):
            there = lax.rem(lon + j, lons)
            pl.when(ahead(there, lon, lons))(lambda: signal(entered.at[0], {"lon": there}))
        if levs > 1:
            pl.when(has_down)(lambda: signal(entered.at[1], {"lev": lev - 1}))

    def wait_greeted():
        pl.when(before < lons - 1)(lambda: pl.semaphore_wait(entered.at[0], lons - 1 - before))
        if levs > 1:
            pl.when(has_up)(lambda: pl.semaphore_wait(entered.at[1], 1))

    def chunks(t):
        return opening if t == 0 else fine if t == STEPS - 1 else coarse

    def face(t, k):
        at, span = chunks(t)[k]
        return pltpu.make_async_remote_copy(
            src_ref=field.at[t, 1, pl.ds(1, cols), pl.ds(PAD + at, span)],
            dst_ref=field.at[t, 0, pl.ds(1, cols), pl.ds(PAD + at, span)],
            send_sem=face_send.at[t, k],
            recv_sem=face_recv.at[t, k],
            device_id={"lat": 1 - lat},
            device_id_type=MESH,
        )

    bands = (pl.ds(1, 1), pl.ds(2, rows - 1))

    def lon_side(t, band, right):
        own, theirs = (cols, 0) if right else (1, cols + 1)
        span = bands[band]
        return pltpu.make_async_remote_copy(
            src_ref=field.at[t, span, own, pl.ds(PAD, deep)],
            dst_ref=field.at[t, span, theirs, pl.ds(PAD, deep)],
            send_sem=lon_send.at[t, band, int(right)],
            recv_sem=lon_recv.at[t, band, int(right)],
            device_id={"lon": lon + 1 if right else lon - 1},
            device_id_type=MESH,
        )

    def lev_side(t, band, up):
        own, theirs = (PAD + deep - 1, PAD - 1) if up else (PAD, PAD + deep)
        span = (bands[band], pl.ds(1, cols))
        return pltpu.make_async_remote_copy(
            src_ref=field.at[t, span[0], span[1], pl.ds(own, 1)],
            dst_ref=field.at[t, span[0], span[1], pl.ds(theirs, 1)],
            send_sem=lev_send.at[t, band, int(up)],
            recv_sem=lev_recv.at[t, band, int(up)],
            device_id={"lev": lev + 1 if up else lev - 1},
            device_id_type=MESH,
        )

    def sides(t, band, act):
        if lons > 1:
            pl.when(has_right)(lambda: act(lon_side(t, band, True)))
            pl.when(has_left)(lambda: act(lon_side(t, band, False)))
        if levs > 1:
            pl.when(has_up)(lambda: act(lev_side(t, band, True)))
            pl.when(has_down)(lambda: act(lev_side(t, band, False)))

    def start_sides(t, band):
        sides(t, band, lambda copy: copy.start())

    def wait_sides_sent(t, band):
        sides(t, band, lambda copy: copy.wait_send())

    def wait_sides(t, band):
        if lons > 1:
            pl.when(has_left)(lambda: lon_side(t, band, True).wait_recv())
            pl.when(has_right)(lambda: lon_side(t, band, False).wait_recv())
        if levs > 1:
            pl.when(has_down)(lambda: lev_side(t, band, True).wait_recv())
            pl.when(has_up)(lambda: lev_side(t, band, False).wait_recv())

    stat_rows = (pl.ds(0, 1), pl.ds(1, rows - 2))
    groups = range(2 if rows > 2 else 1)

    def stat(group, j):
        return pltpu.make_async_remote_copy(
            src_ref=stats.at[stat_rows[group]],
            dst_ref=peers.at[j - 1, stat_rows[group]],
            send_sem=stat_send.at[group, j - 1],
            recv_sem=stat_recv.at[group, j - 1],
            device_id={"lon": lax.rem(lon + j, lons)},
            device_id_type=MESH,
        )

    for k in range(len(opening)):
        first[k].wait()
        face(0, k).start()
        if k == 0:
            greet()

    def clear_cols(at):
        for t in range(STEPS):
            def row(i, _, t=t):
                field[t, i, at, pl.ds(PAD, deep)] = jnp.zeros((deep, lanes), jnp.float32)
                return 0
            lax.fori_loop(1, rows + 1, row, 0)

    def clear_level(at):
        for t in range(STEPS):
            def row(i, _, t=t):
                def col(c, _):
                    field[t, i, c, pl.ds(at, PAD)] = jnp.zeros((PAD, lanes), jnp.float32)
                    return 0
                return lax.fori_loop(1, cols + 1, col, 0)
            lax.fori_loop(1, rows + 1, row, 0)

    pl.when(jnp.logical_not(has_left))(lambda: clear_cols(0))
    pl.when(jnp.logical_not(has_right))(lambda: clear_cols(cols + 1))
    pl.when(jnp.logical_not(has_down))(lambda: clear_level(0))
    pl.when(jnp.logical_not(has_up))(lambda: clear_level(PAD + deep))

    for copy in loads:
        copy.wait()
    wait_greeted()
    start_sides(0, 1)
    start_sides(0, 0)

    def cell(t, r, c, at, span, below, above):
        here = field[t, r, c, pl.ds(PAD + at, span)]
        near = (field[t, r, c - 1, pl.ds(PAD + at, span)] + field[t, r, c + 1, pl.ds(PAD + at, span)])
        near += (field[t, r, c, pl.ds(PAD - 1 + at, span)] + field[t, r, c, pl.ds(PAD + 1 + at, span)])
        if below:
            near += field[t, r - 1, c, pl.ds(PAD + at, span)]
        if above:
            near += field[t, r + 1, c, pl.ds(PAD + at, span)]
        limit = cap[r - 1, c - 1, pl.ds(at, span)]
        return here * (0.6 - 0.2 * (here * limit)) + 0.1 * near

    def advance_row(t, r, at, span, last):
        def col(c, _):
            value = cell(t, r, c, at, span, True, not last)
            field[t + 1, r, c, pl.ds(PAD + at, span)] = value
            if t == STEPS - 2 and isinstance(r, int) and r == 1:
                front[c - 1, pl.ds(at, span)] = value
            return 0
        lax.fori_loop(1, cols + 1, col, 0)

    def start_face(t, k):
        if t < STEPS - 1 or k == 0:
            face(t, k).start()
        elif k == 1:
            pl.when(late)(lambda: face(t, k).start())

    def finish(r, at, last):
        values = [cell(STEPS - 1, r, c, at, 8, True, not last) for c in range(1, cols + 1)]
        for c in range(cols):
            out_dens[r - 2, c, pl.ds(at, 8)] = values[c]
        total, square = line_sums(values)
        stats[r - 2, 0, pl.ds(at, 8)] = total
        stats[r - 2, 1, pl.ds(at, 8)] = square

    def scale(r, at):
        pair = [(stats[r - 2, 0, pl.ds(at, 8)], stats[r - 2, 1, pl.ds(at, 8)])]
        for j in range(lons - 1):
            pair.append((peers[j, r - 2, 0, pl.ds(at, 8)], peers[j, r - 2, 1, pl.ds(at, 8)]))
        mean, gain = line_scale(pair, cols)
        for c in range(cols):
            out_scaled[r - 2, c, pl.ds(at, 8)] = (out_dens[r - 2, c, pl.ds(at, 8)] - mean) * gain

    def each_row(first, last, act):
        def row(r, _):
            tiles(0, deep, lambda at: act(r, at))
            return 0
        lax.fori_loop(first, last, row, 0)

    def send_sums(group):
        for j in range(1, lons):
            stat(group, j).start()

    def wait_sums(group):
        for j in range(1, lons):
            stat(group, j).wait_recv()

    for t in range(STEPS - 1):
        wait_sides(t, 1)

        def inner(r, _, t=t):
            advance_row(t, r, 0, deep, False)
            return 0

        lax.fori_loop(2, rows, inner, 0)
        advance_row(t, rows, 0, deep, True)
        start_sides(t + 1, 1)
        if t == STEPS - 2:
            wait_sides(t + 1, 1)
            if rows > 2:
                each_row(3, rows, lambda r, at: finish(r, at, False))
                tiles(0, deep, lambda at: finish(rows, at, True))
                send_sums(1)
                wait_sums(1)
                each_row(3, rows + 1, scale)
        wait_sides(t, 0)
        for k, (at, span) in enumerate(chunks(t)):
            face(t, k).wait_recv()
            advance_row(t, 1, at, span, False)
            for j, chunk in enumerate(chunks(t + 1)):
                if at < sum(chunk) <= at + span:
                    start_face(t + 1, j)
        start_sides(t + 1, 0)

    t = STEPS - 1
    tiles(0, deep, lambda at: finish(2, at, rows == 2))
    send_sums(0)
    wait_sides(t, 0)

    def base(c, _):
        edge[c - 1] = cell(t, 1, c, 0, deep, False, True)
        return 0

    lax.fori_loop(1, cols + 1, base, 0)
    wait_sums(0)
    tiles(0, deep, lambda at: scale(2, at))

    def add_face(k):
        at, span = fine[k]
        face(t, k).wait_recv()

        def col(c, _):
            edge[c, pl.ds(at, span)] += 0.1 * field[t, 0, c + 1, pl.ds(PAD + at, span)]
            return 0
        lax.fori_loop(0, cols, col, 0)

    for s in range(STEPS - 1):
        for k in range(len(chunks(s))):
            face(s, k).wait_send()
    for s in range(STEPS):
        for band in range(2):
            wait_sides_sent(s, band)
    for group in groups:
        for j in range(1, lons):
            stat(group, j).wait_send()
    add_face(0)
    face(t, 0).wait_send()

    @pl.when(late)
    def _():
        add_face(1)
        face(t, 1).wait_send()


def write_inner(scaled, dens, edge, out_scaled, out_dens, token, sems):
    inner, cols, _, _ = scaled.shape
    copies = []
    for i, (src, dst) in enumerate(((scaled, out_scaled), (dens, out_dens))):
        for r in range(inner):
            copies.append(pltpu.make_async_copy(
                src.at[r], dst.at[place(r + 2, inner + 1)], sems.at[i, r]))
    copies.append(pltpu.make_async_copy(edge, out_dens.at[place(1, inner + 1)], sems.at[1, inner]))
    for copy in copies:
        copy.start()
    token[...] = jnp.zeros(token.shape, jnp.float32)
    for copy in copies:
        copy.wait()


def last_row(lons, edge, front, token, out_scaled, out_dens, *refs):
    twin = lons == 2
    tile_base, tile_face, tile_sums = refs[:3] if twin else (None,) * 3
    (other, stats, peers, entered, face_send, face_recv, stat_send, stat_recv,
     tile_send, tile_recv) = refs[3:] if twin else refs
    cols, deep, lanes = edge.shape
    _, _, fine = split(deep)
    end = len(fine) - 1
    spans = [(0, sum(fine[1]))] + fine[2:]
    tail = pl.ds(*fine[end])
    lat, lon = lax.axis_index("lat"), lax.axis_index("lon")
    late = lax.rem(lon, 2) == 0
    early = jnp.logical_not(late)

    barrier = pltpu.get_barrier_semaphore()
    signal(barrier, {"lat": 1 - lat})
    before = 0
    for j in range(1, lons):
        there = lax.rem(lon + j, lons)
        before += ahead(there, lon, lons).astype(jnp.int32)

        @pl.when(jnp.logical_not(ahead(there, lon, lons)))
        def _():
            signal(barrier, {"lon": there})
            if twin:
                signal(barrier, {"lat": 1 - lat, "lon": there})
    pl.semaphore_wait(barrier, 1 + before * (2 if twin else 1))

    def remote(src, dst, send, recv, where):
        return pltpu.make_async_remote_copy(
            src_ref=src, dst_ref=dst, send_sem=send, recv_sem=recv,
            device_id=where, device_id_type=MESH)

    def face(k):
        pick = (slice(None), pl.ds(*fine[k]))
        return remote(front.at[pick], other.at[pick], face_send.at[k], face_recv.at[k],
                      {"lat": 1 - lat})

    def tile_copy(i):
        src = (front, front, edge, stats)[i].at[:, tail]
        dst = (tile_face, tile_face, tile_base, tile_sums)[i]
        where = {"lat": 1 - lat} if i < 2 else {}
        if i > 0:
            where["lon"] = 1 - lon
        return remote(src, dst, tile_send.at[i], tile_recv.at[i], where)

    def stat(part, j):
        pick = (slice(None), pl.ds(*spans[part]))
        return remote(stats.at[pick], peers.at[(j - 1,) + pick],
                      stat_send.at[part, j - 1], stat_recv.at[part, j - 1],
                      {"lon": lax.rem(lon + j, lons)})

    def each_stat(part, act):
        for j in range(1, lons):
            act(stat(part, j))

    @pl.when(early)
    def _():
        for k in range(1, end + 1):
            face(k).start()

    @pl.when(late)
    def _():
        for k in range(2, end if twin else end + 1):
            face(k).start()
        if twin:
            for i in (2, 0, 1):
                tile_copy(i).start()

    for j in range(1, lons):
        there = lax.rem(lon + j, lons)
        pl.when(ahead(there, lon, lons))(lambda: signal(entered, {"lon": there}))

    def finish(at, add):
        values = [edge[c, pl.ds(at, 8)] for c in range(cols)]
        if add:
            values = [v + 0.1 * other[c, pl.ds(at, 8)] for c, v in enumerate(values)]
        for c in range(cols):
            out_dens[c, pl.ds(at, 8)] = values[c]
        total, square = line_sums(values)
        stats[0, pl.ds(at, 8)] = total
        stats[1, pl.ds(at, 8)] = square

    def scale(at):
        pair = [(stats[0, pl.ds(at, 8)], stats[1, pl.ds(at, 8)])]
        for j in range(lons - 1):
            pair.append((peers[j, 0, pl.ds(at, 8)], peers[j, 1, pl.ds(at, 8)]))
        mean, gain = line_scale(pair, cols)
        for c in range(cols):
            out_scaled[c, pl.ds(at, 8)] = (out_dens[c, pl.ds(at, 8)] - mean) * gain

    def land(k):
        face(k).wait_recv()
        tiles(*fine[k], lambda at: finish(at, True))

    tiles(*fine[0], lambda at: finish(at, False))
    pl.when(late)(lambda: tiles(*fine[1], lambda at: finish(at, False)))
    pl.when(early)(lambda: land(1))
    pl.when(before < lons - 1)(lambda: pl.semaphore_wait(entered, lons - 1 - before))
    each_stat(0, lambda copy: copy.start())
    land(2)
    each_stat(1, lambda copy: copy.start())
    each_stat(0, lambda copy: copy.wait_recv())
    tiles(*spans[0], scale)
    if twin:
        @pl.when(early)
        def _():
            land(end)
            tile_copy(3).start()
            tile_sums[...] = stats[:, tail]
    else:
        land(end)
        each_stat(2, lambda copy: copy.start())
    each_stat(1, lambda copy: copy.wait_recv())
    tiles(*spans[1], scale)

    face(2).wait_send()
    for part in range(2):
        each_stat(part, lambda copy: copy.wait_send())
    if twin:
        @pl.when(early)
        def _():
            face(1).wait_send()
            face(end).wait_send()
            tile_copy(3).wait_send()
            tile_copy(2).wait_recv()
            tile_copy(1).wait_recv()

        @pl.when(late)
        def _():
            tile_base[...] = edge[:, tail]
            for i in range(3):
                tile_copy(i).wait_send()
            tile_copy(3).wait_recv()
            tile_copy(0).wait_recv()
    else:
        pl.when(early)(lambda: face(1).wait_send())
        face(end).wait_send()
        each_stat(2, lambda copy: copy.wait_recv())
        tiles(*spans[2], scale)
        each_stat(2, lambda copy: copy.wait_send())


def write_last(lons, scaled, dens, *refs):
    twin = lons == 2
    if twin:
        tile_base, tile_face, tile_sums, _, _, out_scaled, out_dens, sems = refs[:8]
        own_scaled, own_dens, tile_sem = refs[8:]
    else:
        _, _, out_scaled, out_dens, sems = refs
    rows, many = out_dens.shape[0], sems.shape[1]
    cols, deep, _ = dens.shape
    _, _, fine = split(deep)
    last = fine[-1][0]
    late = 1 - lax.rem(lax.axis_index("lon"), 2)

    def copies(src, dst, i, begin, end):
        step, span = cols // many, pl.ds(begin, end - begin)
        return [
            pltpu.make_async_copy(
                src.at[pl.ds(part * step, step), span],
                dst.at[place(1, rows), pl.ds(part * step, step), span],
                sems.at[i, part])
            for part in range(many)
        ]

    def each(act):
        for copy in copies(scaled, out_scaled, 0, 0, last if twin else deep):
            act(copy)
        for moved in range(2):
            @pl.when(late == moved)
            def _():
                stop = last if twin and moved else deep
                for copy in copies(dens, out_dens, 1, sum(fine[moved]), stop):
                    act(copy)

    def tile_out(i):
        src, dst = ((own_scaled, out_scaled), (own_dens, out_dens))[i]
        return pltpu.make_async_copy(
            src, dst.at[place(1, rows), :, pl.ds(last, 8)], tile_sem.at[i])

    each(lambda copy: copy.start())
    if twin:
        values = [tile_base[c] + 0.1 * tile_face[c] for c in range(cols)]
        mean, gain = line_scale([line_sums(values), (tile_sums[0], tile_sums[1])], cols)

        @pl.when(late == 1)
        def _():
            for c in range(cols):
                own_dens[c] = values[c]
                own_scaled[c] = (values[c] - mean) * gain
            tile_out(1).start()

        @pl.when(late == 0)
        def _():
            for c in range(cols):
                own_scaled[c] = (dens[c, pl.ds(last, 8)] - mean) * gain

        tile_out(0).start()
        pl.when(late == 1)(lambda: tile_out(1).wait())
        tile_out(0).wait()
    each(lambda copy: copy.wait())


def in_vmem(*arrays):
    return [pltpu.with_memory_space_constraint(a, pltpu.VMEM) for a in arrays]


def all_steps(lons, levs, density, crowding):
    rows, cols, deep, lanes = density.shape
    opening, coarse, fine = split(deep)
    sem = pltpu.SemaphoreType.DMA
    peers = max(lons - 1, 1)
    inner = pltpu.VMEM((rows - 1, cols, deep, lanes), jnp.float32)
    row = pltpu.VMEM((cols, deep, lanes), jnp.float32)
    any_space = pl.BlockSpec(memory_space=pl.ANY)
    vmem = pl.BlockSpec(memory_space=pltpu.VMEM)
    scaled, dens, edge, front = pl.pallas_call(
        functools.partial(kernel, lons, levs),
        out_shape=(inner, inner, row, row),
        in_specs=[any_space] * 2,
        out_specs=[vmem] * 4,
        scratch_shapes=[
            pltpu.VMEM((STEPS, rows + 1, cols + 2, deep + 2 * PAD, lanes), jnp.float32),
            pltpu.VMEM((rows, cols, deep, lanes), jnp.float32),
            pltpu.VMEM((rows - 1, 2, deep, lanes), jnp.float32),
            pltpu.VMEM((peers, rows - 1, 2, deep, lanes), jnp.float32),
            pltpu.SemaphoreType.REGULAR((2,)),
            sem((2, rows)),
            sem((len(opening),)),
            sem((STEPS, len(fine))),
            sem((STEPS, len(fine))),
            sem((STEPS, 2, 2)),
            sem((STEPS, 2, 2)),
            sem((STEPS, 2, 2)),
            sem((STEPS, 2, 2)),
            sem((2, peers)),
            sem((2, peers)),
        ],
        compiler_params=pltpu.CompilerParams(
            collective_id=0, has_side_effects=True, vmem_limit_bytes=VMEM_LIMIT
        ),
    )(density, crowding)

    out = jax.ShapeDtypeStruct(density.shape, density.dtype)
    out_scaled, out_dens, token = pl.pallas_call(
        write_inner,
        out_shape=(out, out, pltpu.VMEM((8, lanes), jnp.float32)),
        in_specs=[vmem] * 3,
        out_specs=[pl.BlockSpec(memory_space=pltpu.HBM)] * 2 + [vmem],
        scratch_shapes=[sem((2, rows))],
        compiler_params=pltpu.CompilerParams(vmem_limit_bytes=2**20),
    )(*in_vmem(scaled, dens, edge))

    twin = lons == 2
    tile = pltpu.VMEM((cols, 8, lanes), jnp.float32)
    extra = (tile, tile, pltpu.VMEM((2, 8, lanes), jnp.float32)) if twin else ()
    row_parts = pl.pallas_call(
        functools.partial(last_row, lons),
        out_shape=(row, row) + extra,
        in_specs=[vmem] * 3,
        out_specs=[vmem] * (2 + len(extra)),
        scratch_shapes=[
            pltpu.VMEM((cols, deep, lanes), jnp.float32),
            pltpu.VMEM((2, deep, lanes), jnp.float32),
            pltpu.VMEM((peers, 2, deep, lanes), jnp.float32),
            pltpu.SemaphoreType.REGULAR,
            sem((len(fine),)),
            sem((len(fine),)),
            sem((len(fine) - 1, peers)),
            sem((len(fine) - 1, peers)),
            sem((4,)),
            sem((4,)),
        ],
        compiler_params=pltpu.CompilerParams(
            collective_id=1, has_side_effects=True, vmem_limit_bytes=8 * 2**20
        ),
    )(*in_vmem(edge, front, token))

    hbm = pl.BlockSpec(memory_space=pltpu.HBM)
    known = len(row_parts)
    return pl.pallas_call(
        functools.partial(write_last, lons),
        out_shape=(out, out),
        in_specs=[vmem] * known + [hbm] * 2,
        out_specs=[hbm] * 2,
        input_output_aliases={known: 0, known + 1: 1},
        scratch_shapes=[sem((2, 4 if cols % 4 == 0 else 1))] + ([tile, tile, sem((2,))] if twin else []),
        compiler_params=pltpu.CompilerParams(vmem_limit_bytes=2**20),
    )(*in_vmem(*row_parts), out_scaled, out_dens)


VMEM_LIMIT = 44 * 2**20


def solution(mesh):
    lats, lons, levs = mesh.shape["lat"], mesh.shape["lon"], mesh.shape["lev"]

    def shards(density, crowding):
        rows, cols, deep, lanes = density.shape
        words = lanes * (
            STEPS * (rows + 1) * (cols + 2) * (deep + 2 * PAD)
            + 3 * rows * cols * deep
            + 2 * lons * rows * deep
        )
        fits = lats == 2 and rows > 1 and lanes == 128 and deep % 32 == 0 and 4 * words < VMEM_LIMIT
        if fits:
            return tuple(all_steps(lons, levs, density, crowding))
        return general(density, crowding)

    spec = P(("trial", "lat"), "lon", "lev", None)
    return jax.shard_map(
        shards, mesh=mesh, in_specs=(spec, spec), out_specs=(spec, spec), check_vma=False
    )
```

```python
import functools

import jax
import jax.numpy as jnp
from jax import lax
from jax.experimental import pallas as pl
from jax.experimental.pallas import tpu as pltpu
from jax.sharding import PartitionSpec as P

STEPS = 4
PAD = 8
MESH = pl.DeviceIdType.MESH


def with_halo(cells, sides, width):
    for axis, dim in sides:
        count = lax.axis_size(axis)
        ends = count - 1
        head = lax.slice_in_dim(cells, 0, width, axis=dim)
        tail = lax.slice_in_dim(cells, cells.shape[dim] - width, cells.shape[dim], axis=dim)
        cells = jnp.concatenate(
            [
                lax.ppermute(tail, axis, [(i, (i + 1) % count) for i in range(ends)]),
                cells,
                lax.ppermute(head, axis, [((i + 1) % count, i) for i in range(ends)]),
            ],
            axis=dim,
        )
    return cells


def inner_cells(values, dims):
    for dim in dims:
        values = lax.slice_in_dim(values, 1, values.shape[dim] - 1, axis=dim)
    return values


def side_cells(values, dim, start, dims):
    others = [other for other in dims if other != dim]
    values = inner_cells(values, others)
    return lax.slice_in_dim(values, start, start + values.shape[dim] - 2, axis=dim)


def advance(padded, crowding):
    middle = inner_cells(padded, (0, 1, 2))
    lower = [side_cells(padded, dim, 0, (0, 1, 2)) for dim in (0, 1, 2)]
    upper = [side_cells(padded, dim, 2, (0, 1, 2)) for dim in (0, 1, 2)]
    spread = lower[0] + upper[0] + lower[1] + upper[1] + lower[2] + upper[2] - 6.0 * middle
    return middle + 0.1 * spread + 0.2 * middle * (1.0 - middle * crowding)


def general(density, crowding):
    for step in range(STEPS):
        padded = with_halo(density, (("lat", 0), ("lon", 1), ("lev", 2)), 1)
        density = advance(padded, crowding)
    count = density.shape[1] * lax.axis_size("lon")
    moved = density - 1.0
    totals, squares = lax.psum(
        (jnp.sum(moved, axis=1, keepdims=True), jnp.sum(moved * moved, axis=1, keepdims=True)),
        "lon",
    )
    line_mean = 1.0 + totals / count
    centred = density - line_mean
    line_variance = squares / count - totals / count * (totals / count)
    return (centred * lax.rsqrt(line_variance + 0.0001), density)


def tree_sum(terms):
    terms = list(terms)
    while len(terms) > 1:
        terms = [sum(terms[i : i + 2][1:], terms[i]) for i in range(0, len(terms), 2)]
    return terms[0]


def signal(sem, where):
    pl.semaphore_signal(sem, inc=1, device_id=where, device_id_type=MESH)


def split(deep):
    half, last = deep // 2, deep - 8
    first, late = max(8, deep // 32 * 8), max(8, deep // 64 * 8)
    opening = [(0, 8), (8, half - 8), (half, half)]
    coarse = [(0, half), (half, half)]
    fine = [(0, first), (first, last - late - first), (last - late, late), (last, 8)]
    return opening, coarse, fine


def place(r, rows):
    lat = lax.axis_index("lat")
    return (1 - lat) * (rows - r) + lat * (r - 1)


def tiles(first, many, act):
    def tile(i, _):
        act(pl.multiple_of(i * 8, 8))
        return 0
    lax.fori_loop(first // 8, (first + many) // 8, tile, 0)


def ahead(there, lon, lons):
    return there - lax.rem(there, 2) * lons < lon - lax.rem(lon, 2) * lons


def line_sums(values):
    cols = len(values)
    total = tree_sum(values)
    mean = total * (1.0 / cols)
    return total, tree_sum([(v - mean) * (v - mean) for v in values])


def line_scale(pair, cols):
    count = cols * len(pair)
    mean = tree_sum([p[0] for p in pair]) * (1.0 / count)
    square = tree_sum([p[1] + cols * (p[0] * (1.0 / cols) - mean) ** 2 for p in pair])
    return mean, lax.rsqrt(square * (1.0 / count) + 0.0001)


def kernel(lons, levs, dens, crowd, out_scaled, out_dens, edge, front,
           field, cap, stats, peers, entered, load_sem, edge_sem, face_send, face_recv,
           lon_send, lon_recv, lev_send, lev_recv, stat_send, stat_recv):
    rows, cols, deep, lanes = dens.shape
    opening, coarse, fine = split(deep)
    lat, lon, lev = lax.axis_index("lat"), lax.axis_index("lon"), lax.axis_index("lev")
    has_left, has_right = lon > 0, lon < lons - 1
    has_down, has_up = lev > 0, lev < levs - 1
    late = lax.rem(lon, 2) == 0

    first = [
        pltpu.make_async_copy(
            dens.at[place(1, rows), :, pl.ds(at, span)],
            field.at[0, 1, pl.ds(1, cols), pl.ds(PAD + at, span)],
            edge_sem.at[k])
        for k, (at, span) in enumerate(opening)
    ]
    loads = [pltpu.make_async_copy(crowd, cap, load_sem.at[0])] + [
        pltpu.make_async_copy(
            dens.at[place(r, rows)],
            field.at[0, r, pl.ds(1, cols), pl.ds(PAD, deep)],
            load_sem.at[1])
        for r in range(2, rows + 1)
    ]
    all_rows = pltpu.make_async_copy(
        dens.at[pl.ds(0, rows - 1)],
        field.at[0, pl.ds(2, rows - 1), pl.ds(1, cols), pl.ds(PAD, deep)],
        load_sem.at[1])

    barrier = pltpu.get_barrier_semaphore()
    signal(barrier, {"lat": 1 - lat})
    before = 0
    for j in range(1, lons):
        there = lax.rem(lon + j, lons)
        before += ahead(there, lon, lons).astype(jnp.int32)
        pl.when(jnp.logical_not(ahead(there, lon, lons)))(lambda: signal(barrier, {"lon": there}))
    if levs > 1:
        pl.when(has_up)(lambda: signal(barrier, {"lev": lev + 1}))
    for copy in first + loads:
        copy.start()
    pl.semaphore_wait(barrier, 1 + before + has_down.astype(jnp.int32))

    def greet():
        for j in range(1, lons):
            there = lax.rem(lon + j, lons)
            pl.when(ahead(there, lon, lons))(lambda: signal(entered.at[0], {"lon": there}))
        if levs > 1:
            pl.when(has_down)(lambda: signal(entered.at[1], {"lev": lev - 1}))

    def wait_greeted():
        pl.when(before < lons - 1)(lambda: pl.semaphore_wait(entered.at[0], lons - 1 - before))
        if levs > 1:
            pl.when(has_up)(lambda: pl.semaphore_wait(entered.at[1], 1))

    def chunks(t):
        return opening if t == 0 else fine if t == STEPS - 1 else coarse

    def face(t, k):
        at, span = chunks(t)[k]
        return pltpu.make_async_remote_copy(
            src_ref=field.at[t, 1, pl.ds(1, cols), pl.ds(PAD + at, span)],
            dst_ref=field.at[t, 0, pl.ds(1, cols), pl.ds(PAD + at, span)],
            send_sem=face_send.at[k],
            recv_sem=face_recv.at[t % 2, k],
            device_id={"lat": 1 - lat},
            device_id_type=MESH,
        )

    bands = (pl.ds(1, 1), pl.ds(2, rows - 1))
    sent = []

    def way(count, forward):
        return int(forward) if count > 2 else 0

    def lon_side(t, band, right):
        own, theirs = (cols, 0) if right else (1, cols + 1)
        span = bands[band]
        return pltpu.make_async_remote_copy(
            src_ref=field.at[t, span, own, pl.ds(PAD, deep)],
            dst_ref=field.at[t, span, theirs, pl.ds(PAD, deep)],
            send_sem=lon_send.at[way(lons, right)],
            recv_sem=lon_recv.at[t % 2, band, way(lons, right)],
            device_id={"lon": lon + 1 if right else lon - 1},
            device_id_type=MESH,
        )

    def lev_side(t, band, up):
        own, theirs = (PAD + deep - 1, PAD - 1) if up else (PAD, PAD + deep)
        span = (bands[band], pl.ds(1, cols))
        return pltpu.make_async_remote_copy(
            src_ref=field.at[t, span[0], span[1], pl.ds(own, 1)],
            dst_ref=field.at[t, span[0], span[1], pl.ds(theirs, 1)],
            send_sem=lev_send.at[way(levs, up)],
            recv_sem=lev_recv.at[t % 2, band, way(levs, up)],
            device_id={"lev": lev + 1 if up else lev - 1},
            device_id_type=MESH,
        )

    def sides(t, band, act):
        if lons > 1:
            pl.when(has_right)(lambda: act(lon_side(t, band, True)))
            pl.when(has_left)(lambda: act(lon_side(t, band, False)))
        if levs > 1:
            pl.when(has_up)(lambda: act(lev_side(t, band, True)))
            pl.when(has_down)(lambda: act(lev_side(t, band, False)))

    def wait_sides_sent():
        if sent:
            sides(*sent.pop(), lambda copy: copy.wait_send())

    def start_sides(t, band):
        wait_sides_sent()
        sides(t, band, lambda copy: copy.start())
        sent.append((t, band))

    def wait_sides(t, band):
        if lons > 1:
            pl.when(has_left)(lambda: lon_side(t, band, True).wait_recv())
            pl.when(has_right)(lambda: lon_side(t, band, False).wait_recv())
        if levs > 1:
            pl.when(has_down)(lambda: lev_side(t, band, True).wait_recv())
            pl.when(has_up)(lambda: lev_side(t, band, False).wait_recv())

    stat_rows = (pl.ds(0, 1), pl.ds(1, rows - 2))

    def stat(group, j):
        return pltpu.make_async_remote_copy(
            src_ref=stats.at[stat_rows[group]],
            dst_ref=peers.at[j - 1, stat_rows[group]],
            send_sem=stat_send.at[j - 1],
            recv_sem=stat_recv.at[group, j - 1],
            device_id={"lon": lax.rem(lon + j, lons)},
            device_id_type=MESH,
        )

    for k in range(len(opening)):
        first[k].wait()
        face(0, k).start()
        if k == 0:
            greet()

    def clear_cols(at):
        for t in range(STEPS):
            def row(i, _, t=t):
                field[t, i, at, pl.ds(PAD, deep)] = jnp.zeros((deep, lanes), jnp.float32)
                return 0
            lax.fori_loop(1, rows + 1, row, 0)

    def clear_level(at):
        for t in range(STEPS):
            def row(i, _, t=t):
                def col(c, _):
                    field[t, i, c, pl.ds(at, PAD)] = jnp.zeros((PAD, lanes), jnp.float32)
                    return 0
                return lax.fori_loop(1, cols + 1, col, 0)
            lax.fori_loop(1, rows + 1, row, 0)

    pl.when(jnp.logical_not(has_left))(lambda: clear_cols(0))
    pl.when(jnp.logical_not(has_right))(lambda: clear_cols(cols + 1))
    pl.when(jnp.logical_not(has_down))(lambda: clear_level(0))
    pl.when(jnp.logical_not(has_up))(lambda: clear_level(PAD + deep))

    loads[0].wait()
    all_rows.wait()
    wait_greeted()
    start_sides(0, 1)
    start_sides(0, 0)

    def cell(t, r, c, at, span, below, above):
        here = field[t, r, c, pl.ds(PAD + at, span)]
        near = (field[t, r, c - 1, pl.ds(PAD + at, span)] + field[t, r, c + 1, pl.ds(PAD + at, span)])
        near += (field[t, r, c, pl.ds(PAD - 1 + at, span)] + field[t, r, c, pl.ds(PAD + 1 + at, span)])
        if below:
            near += field[t, r - 1, c, pl.ds(PAD + at, span)]
        if above:
            near += field[t, r + 1, c, pl.ds(PAD + at, span)]
        limit = cap[place(r, rows), c - 1, pl.ds(at, span)]
        return here * (0.6 - 0.2 * (here * limit)) + 0.1 * near

    def advance_row(t, r, at, span, last):
        def col(c, _):
            value = cell(t, r, c, at, span, True, not last)
            field[t + 1, r, c, pl.ds(PAD + at, span)] = value
            if t == STEPS - 2 and isinstance(r, int) and r == 1:
                front[c - 1, pl.ds(at, span)] = value
            return 0
        lax.fori_loop(1, cols + 1, col, 0)

    def start_face(t, k):
        def go():
            face(t - 1, k).wait_send()
            face(t, k).start()

        if t < STEPS - 1 or k == 0:
            go()
        elif k == 1:
            pl.when(late)(go)

    def finish(r, at, last):
        values = [cell(STEPS - 1, r, c, at, 8, True, not last) for c in range(1, cols + 1)]
        for c in range(cols):
            out_dens[r - 2, c, pl.ds(at, 8)] = values[c]
        total, square = line_sums(values)
        stats[r - 2, 0, pl.ds(at, 8)] = total
        stats[r - 2, 1, pl.ds(at, 8)] = square

    def scale(r, at):
        pair = [(stats[r - 2, 0, pl.ds(at, 8)], stats[r - 2, 1, pl.ds(at, 8)])]
        for j in range(lons - 1):
            pair.append((peers[j, r - 2, 0, pl.ds(at, 8)], peers[j, r - 2, 1, pl.ds(at, 8)]))
        mean, gain = line_scale(pair, cols)
        for c in range(cols):
            out_scaled[r - 2, c, pl.ds(at, 8)] = (out_dens[r - 2, c, pl.ds(at, 8)] - mean) * gain

    def each_row(first, last, act):
        def row(r, _):
            tiles(0, deep, lambda at: act(r, at))
            return 0
        lax.fori_loop(first, last, row, 0)

    def send_sums(group):
        for j in range(1, lons):
            if group == 0 and rows > 2:
                stat(1, j).wait_send()
            stat(group, j).start()

    def wait_sums(group):
        for j in range(1, lons):
            stat(group, j).wait_recv()

    for t in range(STEPS - 1):
        wait_sides(t, 1)

        def inner(r, _, t=t):
            advance_row(t, r, 0, deep, False)
            return 0

        lax.fori_loop(2, rows, inner, 0)
        advance_row(t, rows, 0, deep, True)
        start_sides(t + 1, 1)
        if t == STEPS - 2:
            wait_sides(t + 1, 1)
            if rows > 2:
                each_row(3, rows, lambda r, at: finish(r, at, False))
                tiles(0, deep, lambda at: finish(rows, at, True))
                send_sums(1)
                wait_sums(1)
                each_row(3, rows + 1, scale)
        wait_sides(t, 0)
        for k, (at, span) in enumerate(chunks(t)):
            face(t, k).wait_recv()
            advance_row(t, 1, at, span, False)
            for j, chunk in enumerate(chunks(t + 1)):
                if at < sum(chunk) <= at + span:
                    start_face(t + 1, j)
        start_sides(t + 1, 0)

    t = STEPS - 1
    tiles(0, deep, lambda at: finish(2, at, rows == 2))
    send_sums(0)
    wait_sides(t, 0)

    def base(c, _):
        edge[c - 1] = cell(t, 1, c, 0, deep, False, True)
        return 0

    lax.fori_loop(1, cols + 1, base, 0)
    wait_sums(0)
    tiles(0, deep, lambda at: scale(2, at))

    def add_face(k):
        at, span = fine[k]
        face(t, k).wait_recv()

        def col(c, _):
            edge[c, pl.ds(at, span)] += 0.1 * field[t, 0, c + 1, pl.ds(PAD + at, span)]
            return 0
        lax.fori_loop(0, cols, col, 0)

    for k in range(2, len(opening)):
        face(0, k).wait_send()
    wait_sides_sent()
    for j in range(1, lons):
        stat(0, j).wait_send()
    pl.when(jnp.logical_not(late))(lambda: face(t - 1, 1).wait_send())
    add_face(0)
    face(t, 0).wait_send()

    @pl.when(late)
    def _():
        add_face(1)
        face(t, 1).wait_send()


def write_inner(scaled, dens, edge, out_scaled, out_dens, token, sems):
    inner, cols, _, _ = scaled.shape
    waits = [pltpu.make_async_copy(edge, out_dens.at[place(1, inner + 1)], sems.at[2])]
    waits[0].start()
    for i, (src, dst) in enumerate(((scaled, out_scaled), (dens, out_dens))):
        for r in range(inner):
            pltpu.make_async_copy(src.at[r], dst.at[place(r + 2, inner + 1)], sems.at[i]).start()
        waits.append(pltpu.make_async_copy(src, dst.at[pl.ds(0, inner)], sems.at[i]))
    token[...] = jnp.zeros(token.shape, jnp.float32)
    for copy in waits:
        copy.wait()


def last_row(lons, edge, front, token, out_scaled, out_dens, *refs):
    twin = lons == 2
    tile_base, tile_face, tile_sums = refs[:3] if twin else (None,) * 3
    (other, stats, peers, entered, face_send, face_recv, stat_send, stat_recv,
     tile_send, tile_recv) = refs[3:] if twin else refs
    cols, deep, lanes = edge.shape
    _, _, fine = split(deep)
    end = len(fine) - 1
    spans = [(0, sum(fine[1]))] + fine[2:]
    tail = pl.ds(*fine[end])
    lat, lon = lax.axis_index("lat"), lax.axis_index("lon")
    late = lax.rem(lon, 2) == 0
    early = jnp.logical_not(late)

    barrier = pltpu.get_barrier_semaphore()
    signal(barrier, {"lat": 1 - lat})
    before = 0
    for j in range(1, lons):
        there = lax.rem(lon + j, lons)
        before += ahead(there, lon, lons).astype(jnp.int32)

        @pl.when(jnp.logical_not(ahead(there, lon, lons)))
        def _():
            signal(barrier, {"lon": there})
            if twin:
                signal(barrier, {"lat": 1 - lat, "lon": there})
    pl.semaphore_wait(barrier, 1 + before * (2 if twin else 1))

    def remote(src, dst, send, recv, where):
        return pltpu.make_async_remote_copy(
            src_ref=src, dst_ref=dst, send_sem=send, recv_sem=recv,
            device_id=where, device_id_type=MESH)

    def face(k):
        pick = (slice(None), pl.ds(*fine[k]))
        return remote(front.at[pick], other.at[pick], face_send.at[0], face_recv.at[k - 1],
                      {"lat": 1 - lat})

    def wait_faces_sent(k, stop):
        at = fine[k][0]
        pick = (slice(None), pl.ds(at, sum(fine[stop]) - at))
        remote(front.at[pick], other.at[pick], face_send.at[0], face_recv.at[k - 1],
               {"lat": 1 - lat}).wait_send()

    def tile_copy(i):
        src = (front, front, edge, stats)[i].at[:, tail]
        dst = (tile_face, tile_face, tile_base, tile_sums)[i]
        where = {"lat": 1 - lat} if i < 2 else {}
        if i > 0:
            where["lon"] = 1 - lon
        return remote(src, dst, tile_send.at[i % 3], tile_recv.at[i // 2], where)

    def stat(part, j):
        pick = (slice(None), pl.ds(*spans[part]))
        return remote(stats.at[pick], peers.at[(j - 1,) + pick],
                      stat_send.at[j - 1], stat_recv.at[part, j - 1],
                      {"lon": lax.rem(lon + j, lons)})

    def each_stat(part, act):
        for j in range(1, lons):
            act(stat(part, j))

    @pl.when(early)
    def _():
        for k in range(1, end + 1):
            face(k).start()

    @pl.when(late)
    def _():
        for k in range(2, end if twin else end + 1):
            face(k).start()
        if twin:
            for i in (2, 0, 1):
                tile_copy(i).start()

    for j in range(1, lons):
        there = lax.rem(lon + j, lons)
        pl.when(ahead(there, lon, lons))(lambda: signal(entered, {"lon": there}))

    def finish(at, add):
        values = [edge[c, pl.ds(at, 8)] for c in range(cols)]
        if add:
            values = [v + 0.1 * other[c, pl.ds(at, 8)] for c, v in enumerate(values)]
        for c in range(cols):
            out_dens[c, pl.ds(at, 8)] = values[c]
        total, square = line_sums(values)
        stats[0, pl.ds(at, 8)] = total
        stats[1, pl.ds(at, 8)] = square

    def scale(at):
        pair = [(stats[0, pl.ds(at, 8)], stats[1, pl.ds(at, 8)])]
        for j in range(lons - 1):
            pair.append((peers[j, 0, pl.ds(at, 8)], peers[j, 1, pl.ds(at, 8)]))
        mean, gain = line_scale(pair, cols)
        for c in range(cols):
            out_scaled[c, pl.ds(at, 8)] = (out_dens[c, pl.ds(at, 8)] - mean) * gain

    def land(k):
        face(k).wait_recv()
        tiles(*fine[k], lambda at: finish(at, True))

    tiles(*fine[0], lambda at: finish(at, False))
    pl.when(late)(lambda: tiles(*fine[1], lambda at: finish(at, False)))
    pl.when(early)(lambda: land(1))
    pl.when(before < lons - 1)(lambda: pl.semaphore_wait(entered, lons - 1 - before))
    each_stat(0, lambda copy: copy.start())
    land(2)
    each_stat(0, lambda copy: copy.wait_send())
    each_stat(1, lambda copy: copy.start())
    each_stat(0, lambda copy: copy.wait_recv())
    tiles(*spans[0], scale)
    if twin:
        @pl.when(early)
        def _():
            land(end)
            tile_copy(3).start()
            tile_sums[...] = stats[:, tail]
    else:
        land(end)
        each_stat(1, lambda copy: copy.wait_send())
        each_stat(2, lambda copy: copy.start())
    each_stat(1, lambda copy: copy.wait_recv())
    tiles(*spans[1], scale)

    pl.when(early)(lambda: wait_faces_sent(1, end))
    pl.when(late)(lambda: wait_faces_sent(2, end - 1 if twin else end))
    if twin:
        each_stat(1, lambda copy: copy.wait_send())

        @pl.when(early)
        def _():
            tile_copy(3).wait_send()
            tile_copy(2).wait_recv()
            tile_copy(1).wait_recv()

        @pl.when(late)
        def _():
            tile_base[...] = edge[:, tail]
            for i in range(3):
                tile_copy(i).wait_send()
            tile_copy(3).wait_recv()
            tile_copy(0).wait_recv()
    else:
        each_stat(2, lambda copy: copy.wait_recv())
        tiles(*spans[2], scale)
        each_stat(2, lambda copy: copy.wait_send())


def write_last(lons, scaled, dens, *refs):
    twin = lons == 2
    if twin:
        tile_base, tile_face, tile_sums, _, _, out_scaled, out_dens, sems = refs[:8]
        own_scaled, own_dens, tile_sem = refs[8:]
    else:
        _, _, out_scaled, out_dens, sems = refs
    rows = out_dens.shape[0]
    cols, deep, _ = dens.shape
    _, _, fine = split(deep)
    last = fine[-1][0]
    late = 1 - lax.rem(lax.axis_index("lon"), 2)

    def copy(src, dst, i, begin, end):
        span = pl.ds(begin, end - begin)
        return pltpu.make_async_copy(
            src.at[:, span], dst.at[place(1, rows), :, span], sems.at[i])

    def each(act):
        act(copy(scaled, out_scaled, 0, 0, last if twin else deep))
        for moved in range(2):
            @pl.when(late == moved)
            def _():
                stop = last if twin and moved else deep
                act(copy(dens, out_dens, 1, sum(fine[moved]), stop))

    def tile_out(i):
        src, dst = ((own_scaled, out_scaled), (own_dens, out_dens))[i]
        return pltpu.make_async_copy(
            src, dst.at[place(1, rows), :, pl.ds(last, 8)], tile_sem.at[i])

    each(lambda copy: copy.start())
    if twin:
        values = [tile_base[c] + 0.1 * tile_face[c] for c in range(cols)]
        mean, gain = line_scale([line_sums(values), (tile_sums[0], tile_sums[1])], cols)

        @pl.when(late == 1)
        def _():
            for c in range(cols):
                own_dens[c] = values[c]
                own_scaled[c] = (values[c] - mean) * gain
            tile_out(1).start()

        @pl.when(late == 0)
        def _():
            for c in range(cols):
                own_scaled[c] = (dens[c, pl.ds(last, 8)] - mean) * gain

        tile_out(0).start()
        pl.when(late == 1)(lambda: tile_out(1).wait())
        tile_out(0).wait()
    each(lambda copy: copy.wait())


def in_vmem(*arrays):
    return [pltpu.with_memory_space_constraint(a, pltpu.VMEM) for a in arrays]


def all_steps(lons, levs, density, crowding):
    rows, cols, deep, lanes = density.shape
    opening, coarse, fine = split(deep)
    sem = pltpu.SemaphoreType.DMA
    peers = max(lons - 1, 1)
    inner = pltpu.VMEM((rows - 1, cols, deep, lanes), jnp.float32)
    row = pltpu.VMEM((cols, deep, lanes), jnp.float32)
    any_space = pl.BlockSpec(memory_space=pl.ANY)
    vmem = pl.BlockSpec(memory_space=pltpu.VMEM)
    scaled, dens, edge, front = pl.pallas_call(
        functools.partial(kernel, lons, levs),
        out_shape=(inner, inner, row, row),
        in_specs=[any_space] * 2,
        out_specs=[vmem] * 4,
        scratch_shapes=[
            pltpu.VMEM((STEPS, rows + 1, cols + 2, deep + 2 * PAD, lanes), jnp.float32),
            pltpu.VMEM((rows, cols, deep, lanes), jnp.float32),
            pltpu.VMEM((rows - 1, 2, deep, lanes), jnp.float32),
            pltpu.VMEM((peers, rows - 1, 2, deep, lanes), jnp.float32),
            pltpu.SemaphoreType.REGULAR((2,)),
            sem((2,)),
            sem((len(opening),)),
            sem((len(opening),)),
            sem((2, len(opening))),
            sem((2 if lons > 2 else 1,)),
            sem((2, 2, 2 if lons > 2 else 1)),
            sem((2 if levs > 2 else 1,)),
            sem((2, 2, 2 if levs > 2 else 1)),
            sem((peers,)),
            sem((2, peers)),
        ],
        compiler_params=pltpu.CompilerParams(
            collective_id=0, has_side_effects=True, vmem_limit_bytes=VMEM_LIMIT
        ),
    )(density, crowding)

    out = jax.ShapeDtypeStruct(density.shape, density.dtype)
    out_scaled, out_dens, token = pl.pallas_call(
        write_inner,
        out_shape=(out, out, pltpu.VMEM((8, lanes), jnp.float32)),
        in_specs=[vmem] * 3,
        out_specs=[pl.BlockSpec(memory_space=pltpu.HBM)] * 2 + [vmem],
        scratch_shapes=[sem((3,))],
        compiler_params=pltpu.CompilerParams(vmem_limit_bytes=2**20),
    )(*in_vmem(scaled, dens, edge))

    twin = lons == 2
    tile = pltpu.VMEM((cols, 8, lanes), jnp.float32)
    extra = (tile, tile, pltpu.VMEM((2, 8, lanes), jnp.float32)) if twin else ()
    row_parts = pl.pallas_call(
        functools.partial(last_row, lons),
        out_shape=(row, row) + extra,
        in_specs=[vmem] * 3,
        out_specs=[vmem] * (2 + len(extra)),
        scratch_shapes=[
            pltpu.VMEM((cols, deep, lanes), jnp.float32),
            pltpu.VMEM((2, deep, lanes), jnp.float32),
            pltpu.VMEM((peers, 2, deep, lanes), jnp.float32),
            pltpu.SemaphoreType.REGULAR,
            sem((1,)),
            sem((len(fine) - 1,)),
            sem((peers,)),
            sem((2 if twin else 3, peers)),
            sem((3,)),
            sem((2,)),
        ],
        compiler_params=pltpu.CompilerParams(
            collective_id=1, has_side_effects=True, vmem_limit_bytes=8 * 2**20
        ),
    )(*in_vmem(edge, front, token))

    hbm = pl.BlockSpec(memory_space=pltpu.HBM)
    known = len(row_parts)
    return pl.pallas_call(
        functools.partial(write_last, lons),
        out_shape=(out, out),
        in_specs=[vmem] * known + [hbm] * 2,
        out_specs=[hbm] * 2,
        input_output_aliases={known: 0, known + 1: 1},
        scratch_shapes=[sem((2,))] + ([tile, tile, sem((2,))] if twin else []),
        compiler_params=pltpu.CompilerParams(vmem_limit_bytes=2**20),
    )(*in_vmem(*row_parts), out_scaled, out_dens)


VMEM_LIMIT = 44 * 2**20


def solution(mesh):
    lats, lons, levs = mesh.shape["lat"], mesh.shape["lon"], mesh.shape["lev"]

    def shards(density, crowding):
        rows, cols, deep, lanes = density.shape
        words = lanes * (
            STEPS * (rows + 1) * (cols + 2) * (deep + 2 * PAD)
            + 3 * rows * cols * deep
            + 2 * lons * rows * deep
        )
        fits = lats == 2 and rows > 1 and lanes == 128 and deep % 32 == 0 and 4 * words < VMEM_LIMIT
        if fits:
            return tuple(all_steps(lons, levs, density, crowding))
        return general(density, crowding)

    spec = P(("trial", "lat"), "lon", "lev", None)
    return jax.shard_map(
        shards, mesh=mesh, in_specs=(spec, spec), out_specs=(spec, spec), check_vma=False
    )
```

```python
import functools

import jax
import jax.numpy as jnp
from jax import lax
from jax.experimental import pallas as pl
from jax.experimental.pallas import tpu as pltpu
from jax.sharding import PartitionSpec as P

STEPS = 4
PAD = 8
MESH = pl.DeviceIdType.MESH


def with_halo(cells, sides, width):
    for axis, dim in sides:
        count = lax.axis_size(axis)
        ends = count - 1
        head = lax.slice_in_dim(cells, 0, width, axis=dim)
        tail = lax.slice_in_dim(cells, cells.shape[dim] - width, cells.shape[dim], axis=dim)
        cells = jnp.concatenate(
            [
                lax.ppermute(tail, axis, [(i, (i + 1) % count) for i in range(ends)]),
                cells,
                lax.ppermute(head, axis, [((i + 1) % count, i) for i in range(ends)]),
            ],
            axis=dim,
        )
    return cells


def inner_cells(values, dims):
    for dim in dims:
        values = lax.slice_in_dim(values, 1, values.shape[dim] - 1, axis=dim)
    return values


def side_cells(values, dim, start, dims):
    others = [other for other in dims if other != dim]
    values = inner_cells(values, others)
    return lax.slice_in_dim(values, start, start + values.shape[dim] - 2, axis=dim)


def advance(padded, crowding):
    middle = inner_cells(padded, (0, 1, 2))
    lower = [side_cells(padded, dim, 0, (0, 1, 2)) for dim in (0, 1, 2)]
    upper = [side_cells(padded, dim, 2, (0, 1, 2)) for dim in (0, 1, 2)]
    spread = lower[0] + upper[0] + lower[1] + upper[1] + lower[2] + upper[2] - 6.0 * middle
    return middle + 0.1 * spread + 0.2 * middle * (1.0 - middle * crowding)


def general(density, crowding):
    for step in range(STEPS):
        padded = with_halo(density, (("lat", 0), ("lon", 1), ("lev", 2)), 1)
        density = advance(padded, crowding)
    count = density.shape[1] * lax.axis_size("lon")
    moved = density - 1.0
    totals, squares = lax.psum(
        (jnp.sum(moved, axis=1, keepdims=True), jnp.sum(moved * moved, axis=1, keepdims=True)),
        "lon",
    )
    line_mean = 1.0 + totals / count
    centred = density - line_mean
    line_variance = squares / count - totals / count * (totals / count)
    return (centred * lax.rsqrt(line_variance + 0.0001), density)


def tree_sum(terms):
    terms = list(terms)
    while len(terms) > 1:
        terms = [sum(terms[i : i + 2][1:], terms[i]) for i in range(0, len(terms), 2)]
    return terms[0]


def signal(sem, where):
    pl.semaphore_signal(sem, inc=1, device_id=where, device_id_type=MESH)


def split(deep):
    half, last = deep // 2, deep - 8
    first, late = max(8, deep // 32 * 8), max(8, deep // 64 * 8)
    coarse = [(0, half), (half, half)]
    fine = [(0, first), (first, last - late - first), (last - late, late), (last, 8)]
    return coarse, fine


def place(r, rows):
    lat = lax.axis_index("lat")
    return (1 - lat) * (rows - r) + lat * (r - 1)


def tiles(first, many, act):
    def tile(i, _):
        act(pl.multiple_of(i * 8, 8))
        return 0
    lax.fori_loop(first // 8, (first + many) // 8, tile, 0)


def ahead(there, lon, lons):
    return there - lax.rem(there, 2) * lons < lon - lax.rem(lon, 2) * lons


def line_sums(values):
    cols = len(values)
    total = tree_sum(values)
    mean = total * (1.0 / cols)
    return total, tree_sum([(v - mean) * (v - mean) for v in values])


def line_scale(pair, cols):
    count = cols * len(pair)
    mean = tree_sum([p[0] for p in pair]) * (1.0 / count)
    square = tree_sum([p[1] + cols * (p[0] * (1.0 / cols) - mean) ** 2 for p in pair])
    return mean, lax.rsqrt(square * (1.0 / count) + 0.0001)


def kernel(lons, levs, dens, crowd, out_scaled, out_dens, edge, front,
           field, cap, stats, peers, entered, load_sem, face_send, face_recv,
           lon_send, lon_recv, lev_send, lev_recv, stat_send, stat_recv):
    rows, cols, deep, lanes = dens.shape
    coarse, fine = split(deep)
    lat, lon, lev = lax.axis_index("lat"), lax.axis_index("lon"), lax.axis_index("lev")
    has_left, has_right = lon > 0, lon < lons - 1
    has_down, has_up = lev > 0, lev < levs - 1
    late = lax.rem(lon, 2) == 0

    loads = [pltpu.make_async_copy(crowd, cap, load_sem.at[0])] + [
        pltpu.make_async_copy(
            dens.at[place(r, rows)],
            field.at[0, r, pl.ds(1, cols), pl.ds(PAD, deep)],
            load_sem.at[1])
        for r in range(1, rows + 1)
    ]
    all_rows = pltpu.make_async_copy(
        dens, field.at[0, pl.ds(1, rows), pl.ds(1, cols), pl.ds(PAD, deep)], load_sem.at[1])

    barrier = pltpu.get_barrier_semaphore()
    signal(barrier, {"lat": 1 - lat})
    before = 0
    for j in range(1, lons):
        there = lax.rem(lon + j, lons)
        before += ahead(there, lon, lons).astype(jnp.int32)
        pl.when(jnp.logical_not(ahead(there, lon, lons)))(lambda: signal(barrier, {"lon": there}))
    if levs > 1:
        pl.when(has_up)(lambda: signal(barrier, {"lev": lev + 1}))
    for copy in loads:
        copy.start()
    pl.semaphore_wait(barrier, 1 + before + has_down.astype(jnp.int32))

    def greet():
        for j in range(1, lons):
            there = lax.rem(lon + j, lons)
            pl.when(ahead(there, lon, lons))(lambda: signal(entered.at[0], {"lon": there}))
        if levs > 1:
            pl.when(has_down)(lambda: signal(entered.at[1], {"lev": lev - 1}))

    def wait_greeted():
        pl.when(before < lons - 1)(lambda: pl.semaphore_wait(entered.at[0], lons - 1 - before))
        if levs > 1:
            pl.when(has_up)(lambda: pl.semaphore_wait(entered.at[1], 1))

    def chunks(t):
        return fine if t == STEPS - 1 else coarse

    def face(t, k):
        at, span = chunks(t)[k]
        src = field.at[t, 1, pl.ds(1, cols), pl.ds(PAD + at, span)]
        if t == 0:
            src = dens.at[place(1, rows), :, pl.ds(at, span)]
        return pltpu.make_async_remote_copy(
            src_ref=src,
            dst_ref=field.at[t, 0, pl.ds(1, cols), pl.ds(PAD + at, span)],
            send_sem=face_send.at[k],
            recv_sem=face_recv.at[t % 2, k],
            device_id={"lat": 1 - lat},
            device_id_type=MESH,
        )

    bands = (pl.ds(1, 1), pl.ds(2, rows - 1))
    sent = []

    def way(count, forward):
        return int(forward) if count > 2 else 0

    def lon_side(t, band, right):
        own, theirs = (cols, 0) if right else (1, cols + 1)
        span = bands[band]
        return pltpu.make_async_remote_copy(
            src_ref=field.at[t, span, own, pl.ds(PAD, deep)],
            dst_ref=field.at[t, span, theirs, pl.ds(PAD, deep)],
            send_sem=lon_send.at[way(lons, right)],
            recv_sem=lon_recv.at[t % 2, band, way(lons, right)],
            device_id={"lon": lon + 1 if right else lon - 1},
            device_id_type=MESH,
        )

    def lev_side(t, band, up):
        own, theirs = (PAD + deep - 1, PAD - 1) if up else (PAD, PAD + deep)
        span = (bands[band], pl.ds(1, cols))
        return pltpu.make_async_remote_copy(
            src_ref=field.at[t, span[0], span[1], pl.ds(own, 1)],
            dst_ref=field.at[t, span[0], span[1], pl.ds(theirs, 1)],
            send_sem=lev_send.at[way(levs, up)],
            recv_sem=lev_recv.at[t % 2, band, way(levs, up)],
            device_id={"lev": lev + 1 if up else lev - 1},
            device_id_type=MESH,
        )

    def sides(t, band, act):
        if lons > 1:
            pl.when(has_right)(lambda: act(lon_side(t, band, True)))
            pl.when(has_left)(lambda: act(lon_side(t, band, False)))
        if levs > 1:
            pl.when(has_up)(lambda: act(lev_side(t, band, True)))
            pl.when(has_down)(lambda: act(lev_side(t, band, False)))

    def wait_sides_sent():
        if sent:
            sides(*sent.pop(), lambda copy: copy.wait_send())

    def start_sides(t, band):
        wait_sides_sent()
        sides(t, band, lambda copy: copy.start())
        sent.append((t, band))

    def wait_sides(t, band):
        if lons > 1:
            pl.when(has_left)(lambda: lon_side(t, band, True).wait_recv())
            pl.when(has_right)(lambda: lon_side(t, band, False).wait_recv())
        if levs > 1:
            pl.when(has_down)(lambda: lev_side(t, band, True).wait_recv())
            pl.when(has_up)(lambda: lev_side(t, band, False).wait_recv())

    stat_rows = (pl.ds(0, 1), pl.ds(1, rows - 2))

    def stat(group, j):
        return pltpu.make_async_remote_copy(
            src_ref=stats.at[stat_rows[group]],
            dst_ref=peers.at[j - 1, stat_rows[group]],
            send_sem=stat_send.at[j - 1],
            recv_sem=stat_recv.at[group, j - 1],
            device_id={"lon": lax.rem(lon + j, lons)},
            device_id_type=MESH,
        )

    for k in range(len(coarse)):
        face(0, k).start()
    greet()

    def clear_cols(at):
        for t in range(STEPS):
            def row(i, _, t=t):
                field[t, i, at, pl.ds(PAD, deep)] = jnp.zeros((deep, lanes), jnp.float32)
                return 0
            lax.fori_loop(1, rows + 1, row, 0)

    def clear_level(at):
        for t in range(STEPS):
            def row(i, _, t=t):
                def col(c, _):
                    field[t, i, c, pl.ds(at, PAD)] = jnp.zeros((PAD, lanes), jnp.float32)
                    return 0
                return lax.fori_loop(1, cols + 1, col, 0)
            lax.fori_loop(1, rows + 1, row, 0)

    pl.when(jnp.logical_not(has_left))(lambda: clear_cols(0))
    pl.when(jnp.logical_not(has_right))(lambda: clear_cols(cols + 1))
    pl.when(jnp.logical_not(has_down))(lambda: clear_level(0))
    pl.when(jnp.logical_not(has_up))(lambda: clear_level(PAD + deep))

    loads[0].wait()
    all_rows.wait()
    wait_greeted()
    start_sides(0, 1)
    start_sides(0, 0)

    def cell(t, r, c, at, span, below, above):
        here = field[t, r, c, pl.ds(PAD + at, span)]
        near = (field[t, r, c - 1, pl.ds(PAD + at, span)] + field[t, r, c + 1, pl.ds(PAD + at, span)])
        near += (field[t, r, c, pl.ds(PAD - 1 + at, span)] + field[t, r, c, pl.ds(PAD + 1 + at, span)])
        if below:
            near += field[t, r - 1, c, pl.ds(PAD + at, span)]
        if above:
            near += field[t, r + 1, c, pl.ds(PAD + at, span)]
        limit = cap[place(r, rows), c - 1, pl.ds(at, span)]
        return here * (0.6 - 0.2 * (here * limit)) + 0.1 * near

    def advance_row(t, r, at, span, last):
        def col(c, _):
            value = cell(t, r, c, at, span, True, not last)
            field[t + 1, r, c, pl.ds(PAD + at, span)] = value
            if t == STEPS - 2 and isinstance(r, int) and r == 1:
                front[c - 1, pl.ds(at, span)] = value
            return 0
        lax.fori_loop(1, cols + 1, col, 0)

    def start_face(t, k):
        def go():
            face(t - 1, k).wait_send()
            face(t, k).start()

        if t < STEPS - 1 or k == 0:
            go()
        elif k == 1:
            pl.when(late)(go)

    def finish(r, at, last):
        values = [cell(STEPS - 1, r, c, at, 8, True, not last) for c in range(1, cols + 1)]
        for c in range(cols):
            out_dens[r - 2, c, pl.ds(at, 8)] = values[c]
        total, square = line_sums(values)
        stats[r - 2, 0, pl.ds(at, 8)] = total
        stats[r - 2, 1, pl.ds(at, 8)] = square

    def scale(r, at):
        pair = [(stats[r - 2, 0, pl.ds(at, 8)], stats[r - 2, 1, pl.ds(at, 8)])]
        for j in range(lons - 1):
            pair.append((peers[j, r - 2, 0, pl.ds(at, 8)], peers[j, r - 2, 1, pl.ds(at, 8)]))
        mean, gain = line_scale(pair, cols)
        for c in range(cols):
            out_scaled[r - 2, c, pl.ds(at, 8)] = (out_dens[r - 2, c, pl.ds(at, 8)] - mean) * gain

    def each_row(first, last, act):
        def row(r, _):
            tiles(0, deep, lambda at: act(r, at))
            return 0
        lax.fori_loop(first, last, row, 0)

    def send_sums(group):
        for j in range(1, lons):
            if group == 0 and rows > 2:
                stat(1, j).wait_send()
            stat(group, j).start()

    def wait_sums(group):
        for j in range(1, lons):
            stat(group, j).wait_recv()

    for t in range(STEPS - 1):
        wait_sides(t, 1)

        def inner(r, _, t=t):
            advance_row(t, r, 0, deep, False)
            return 0

        lax.fori_loop(2, rows, inner, 0)
        advance_row(t, rows, 0, deep, True)
        start_sides(t + 1, 1)
        if t == STEPS - 2:
            wait_sides(t + 1, 1)
            if rows > 2:
                each_row(3, rows, lambda r, at: finish(r, at, False))
                tiles(0, deep, lambda at: finish(rows, at, True))
                send_sums(1)
                wait_sums(1)
                each_row(3, rows + 1, scale)
        wait_sides(t, 0)
        for k, (at, span) in enumerate(chunks(t)):
            face(t, k).wait_recv()
            advance_row(t, 1, at, span, False)
            for j, chunk in enumerate(chunks(t + 1)):
                if at < sum(chunk) <= at + span:
                    start_face(t + 1, j)
        start_sides(t + 1, 0)

    t = STEPS - 1
    tiles(0, deep, lambda at: finish(2, at, rows == 2))
    send_sums(0)
    wait_sides(t, 0)

    def base(c, _):
        edge[c - 1] = cell(t, 1, c, 0, deep, False, True)
        return 0

    lax.fori_loop(1, cols + 1, base, 0)
    wait_sums(0)
    tiles(0, deep, lambda at: scale(2, at))

    def add_face(k):
        at, span = fine[k]
        face(t, k).wait_recv()

        def col(c, _):
            edge[c, pl.ds(at, span)] += 0.1 * field[t, 0, c + 1, pl.ds(PAD + at, span)]
            return 0
        lax.fori_loop(0, cols, col, 0)

    wait_sides_sent()
    for j in range(1, lons):
        stat(0, j).wait_send()
    pl.when(jnp.logical_not(late))(lambda: face(t - 1, 1).wait_send())
    add_face(0)
    face(t, 0).wait_send()

    @pl.when(late)
    def _():
        add_face(1)
        face(t, 1).wait_send()


def write_inner(scaled, dens, edge, out_scaled, out_dens, token, sems):
    inner, cols, _, _ = scaled.shape
    waits = [pltpu.make_async_copy(edge, out_dens.at[place(1, inner + 1)], sems.at[2])]
    waits[0].start()
    for i, (src, dst) in enumerate(((scaled, out_scaled), (dens, out_dens))):
        for r in range(inner):
            pltpu.make_async_copy(src.at[r], dst.at[place(r + 2, inner + 1)], sems.at[i]).start()
        waits.append(pltpu.make_async_copy(src, dst.at[pl.ds(0, inner)], sems.at[i]))
    token[...] = jnp.zeros(token.shape, jnp.float32)
    for copy in waits:
        copy.wait()


def last_row(lons, edge, front, token, out_scaled, out_dens, *refs):
    twin = lons == 2
    tile_base, tile_face, tile_sums = refs[:3] if twin else (None,) * 3
    (other, stats, peers, entered, face_send, face_recv, stat_send, stat_recv,
     tile_send, tile_recv) = refs[3:] if twin else refs
    cols, deep, lanes = edge.shape
    _, fine = split(deep)
    end = len(fine) - 1
    spans = [(0, sum(fine[1]))] + fine[2:]
    tail = pl.ds(*fine[end])
    lat, lon = lax.axis_index("lat"), lax.axis_index("lon")
    late = lax.rem(lon, 2) == 0
    early = jnp.logical_not(late)

    barrier = pltpu.get_barrier_semaphore()
    signal(barrier, {"lat": 1 - lat})
    before = 0
    for j in range(1, lons):
        there = lax.rem(lon + j, lons)
        before += ahead(there, lon, lons).astype(jnp.int32)

        @pl.when(jnp.logical_not(ahead(there, lon, lons)))
        def _():
            signal(barrier, {"lon": there})
            if twin:
                signal(barrier, {"lat": 1 - lat, "lon": there})
    pl.semaphore_wait(barrier, 1 + before * (2 if twin else 1))

    def remote(src, dst, send, recv, where):
        return pltpu.make_async_remote_copy(
            src_ref=src, dst_ref=dst, send_sem=send, recv_sem=recv,
            device_id=where, device_id_type=MESH)

    def face(k):
        pick = (slice(None), pl.ds(*fine[k]))
        return remote(front.at[pick], other.at[pick], face_send.at[0], face_recv.at[k - 1],
                      {"lat": 1 - lat})

    def wait_faces_sent(k, stop):
        at = fine[k][0]
        pick = (slice(None), pl.ds(at, sum(fine[stop]) - at))
        remote(front.at[pick], other.at[pick], face_send.at[0], face_recv.at[k - 1],
               {"lat": 1 - lat}).wait_send()

    def tile_copy(i):
        src = (front, front, edge, stats)[i].at[:, tail]
        dst = (tile_face, tile_face, tile_base, tile_sums)[i]
        where = {"lat": 1 - lat} if i < 2 else {}
        if i > 0:
            where["lon"] = 1 - lon
        return remote(src, dst, tile_send.at[i % 3], tile_recv.at[i // 2], where)

    def stat(part, j):
        pick = (slice(None), pl.ds(*spans[part]))
        return remote(stats.at[pick], peers.at[(j - 1,) + pick],
                      stat_send.at[j - 1], stat_recv.at[part, j - 1],
                      {"lon": lax.rem(lon + j, lons)})

    def each_stat(part, act):
        for j in range(1, lons):
            act(stat(part, j))

    @pl.when(early)
    def _():
        for k in range(1, end + 1):
            face(k).start()

    @pl.when(late)
    def _():
        for k in range(2, end if twin else end + 1):
            face(k).start()
        if twin:
            for i in (2, 0, 1):
                tile_copy(i).start()

    for j in range(1, lons):
        there = lax.rem(lon + j, lons)
        pl.when(ahead(there, lon, lons))(lambda: signal(entered, {"lon": there}))

    def finish(at, add):
        values = [edge[c, pl.ds(at, 8)] for c in range(cols)]
        if add:
            values = [v + 0.1 * other[c, pl.ds(at, 8)] for c, v in enumerate(values)]
        for c in range(cols):
            out_dens[c, pl.ds(at, 8)] = values[c]
        total, square = line_sums(values)
        stats[0, pl.ds(at, 8)] = total
        stats[1, pl.ds(at, 8)] = square

    def scale(at):
        pair = [(stats[0, pl.ds(at, 8)], stats[1, pl.ds(at, 8)])]
        for j in range(lons - 1):
            pair.append((peers[j, 0, pl.ds(at, 8)], peers[j, 1, pl.ds(at, 8)]))
        mean, gain = line_scale(pair, cols)
        for c in range(cols):
            out_scaled[c, pl.ds(at, 8)] = (out_dens[c, pl.ds(at, 8)] - mean) * gain

    def land(k):
        face(k).wait_recv()
        tiles(*fine[k], lambda at: finish(at, True))

    tiles(*fine[0], lambda at: finish(at, False))
    pl.when(late)(lambda: tiles(*fine[1], lambda at: finish(at, False)))
    pl.when(early)(lambda: land(1))
    pl.when(before < lons - 1)(lambda: pl.semaphore_wait(entered, lons - 1 - before))
    each_stat(0, lambda copy: copy.start())
    land(2)
    each_stat(0, lambda copy: copy.wait_send())
    each_stat(1, lambda copy: copy.start())
    each_stat(0, lambda copy: copy.wait_recv())
    tiles(*spans[0], scale)
    if twin:
        @pl.when(early)
        def _():
            land(end)
            tile_copy(3).start()
            tile_sums[...] = stats[:, tail]
    else:
        land(end)
        each_stat(1, lambda copy: copy.wait_send())
        each_stat(2, lambda copy: copy.start())
    each_stat(1, lambda copy: copy.wait_recv())
    tiles(*spans[1], scale)

    pl.when(early)(lambda: wait_faces_sent(1, end))
    pl.when(late)(lambda: wait_faces_sent(2, end - 1 if twin else end))
    if twin:
        each_stat(1, lambda copy: copy.wait_send())

        @pl.when(early)
        def _():
            tile_copy(3).wait_send()
            tile_copy(2).wait_recv()
            tile_copy(1).wait_recv()

        @pl.when(late)
        def _():
            tile_base[...] = edge[:, tail]
            for i in range(3):
                tile_copy(i).wait_send()
            tile_copy(3).wait_recv()
            tile_copy(0).wait_recv()
    else:
        each_stat(2, lambda copy: copy.wait_recv())
        tiles(*spans[2], scale)
        each_stat(2, lambda copy: copy.wait_send())


def write_last(lons, scaled, dens, *refs):
    twin = lons == 2
    if twin:
        tile_base, tile_face, tile_sums, _, _, out_scaled, out_dens, sems = refs[:8]
        own_scaled, own_dens, tile_sem = refs[8:]
    else:
        _, _, out_scaled, out_dens, sems = refs
    rows = out_dens.shape[0]
    cols, deep, _ = dens.shape
    _, fine = split(deep)
    last = fine[-1][0]
    late = 1 - lax.rem(lax.axis_index("lon"), 2)

    def copy(src, dst, i, begin, end):
        span = pl.ds(begin, end - begin)
        return pltpu.make_async_copy(
            src.at[:, span], dst.at[place(1, rows), :, span], sems.at[i])

    def each(act):
        act(copy(scaled, out_scaled, 0, 0, last if twin else deep))
        for moved in range(2):
            @pl.when(late == moved)
            def _():
                stop = last if twin and moved else deep
                act(copy(dens, out_dens, 1, sum(fine[moved]), stop))

    def tile_out(i):
        src, dst = ((own_scaled, out_scaled), (own_dens, out_dens))[i]
        return pltpu.make_async_copy(
            src, dst.at[place(1, rows), :, pl.ds(last, 8)], tile_sem.at[i])

    each(lambda copy: copy.start())
    if twin:
        values = [tile_base[c] + 0.1 * tile_face[c] for c in range(cols)]
        mean, gain = line_scale([line_sums(values), (tile_sums[0], tile_sums[1])], cols)

        @pl.when(late == 1)
        def _():
            for c in range(cols):
                own_dens[c] = values[c]
                own_scaled[c] = (values[c] - mean) * gain
            tile_out(1).start()

        @pl.when(late == 0)
        def _():
            for c in range(cols):
                own_scaled[c] = (dens[c, pl.ds(last, 8)] - mean) * gain

        tile_out(0).start()
        pl.when(late == 1)(lambda: tile_out(1).wait())
        tile_out(0).wait()
    each(lambda copy: copy.wait())


def in_vmem(*arrays):
    return [pltpu.with_memory_space_constraint(a, pltpu.VMEM) for a in arrays]


def all_steps(lons, levs, density, crowding):
    rows, cols, deep, lanes = density.shape
    coarse, fine = split(deep)
    sem = pltpu.SemaphoreType.DMA
    peers = max(lons - 1, 1)
    inner = pltpu.VMEM((rows - 1, cols, deep, lanes), jnp.float32)
    row = pltpu.VMEM((cols, deep, lanes), jnp.float32)
    any_space = pl.BlockSpec(memory_space=pl.ANY)
    vmem = pl.BlockSpec(memory_space=pltpu.VMEM)
    scaled, dens, edge, front = pl.pallas_call(
        functools.partial(kernel, lons, levs),
        out_shape=(inner, inner, row, row),
        in_specs=[any_space] * 2,
        out_specs=[vmem] * 4,
        scratch_shapes=[
            pltpu.VMEM((STEPS, rows + 1, cols + 2, deep + 2 * PAD, lanes), jnp.float32),
            pltpu.VMEM((rows, cols, deep, lanes), jnp.float32),
            pltpu.VMEM((rows - 1, 2, deep, lanes), jnp.float32),
            pltpu.VMEM((peers, rows - 1, 2, deep, lanes), jnp.float32),
            pltpu.SemaphoreType.REGULAR((2,)),
            sem((2,)),
            sem((len(coarse),)),
            sem((2, len(coarse))),
            sem((2 if lons > 2 else 1,)),
            sem((2, 2, 2 if lons > 2 else 1)),
            sem((2 if levs > 2 else 1,)),
            sem((2, 2, 2 if levs > 2 else 1)),
            sem((peers,)),
            sem((2, peers)),
        ],
        compiler_params=pltpu.CompilerParams(
            collective_id=0, has_side_effects=True, vmem_limit_bytes=VMEM_LIMIT
        ),
    )(density, crowding)

    out = jax.ShapeDtypeStruct(density.shape, density.dtype)
    out_scaled, out_dens, token = pl.pallas_call(
        write_inner,
        out_shape=(out, out, pltpu.VMEM((8, lanes), jnp.float32)),
        in_specs=[vmem] * 3,
        out_specs=[pl.BlockSpec(memory_space=pltpu.HBM)] * 2 + [vmem],
        scratch_shapes=[sem((3,))],
        compiler_params=pltpu.CompilerParams(vmem_limit_bytes=2**20),
    )(*in_vmem(scaled, dens, edge))

    twin = lons == 2
    tile = pltpu.VMEM((cols, 8, lanes), jnp.float32)
    extra = (tile, tile, pltpu.VMEM((2, 8, lanes), jnp.float32)) if twin else ()
    row_parts = pl.pallas_call(
        functools.partial(last_row, lons),
        out_shape=(row, row) + extra,
        in_specs=[vmem] * 3,
        out_specs=[vmem] * (2 + len(extra)),
        scratch_shapes=[
            pltpu.VMEM((cols, deep, lanes), jnp.float32),
            pltpu.VMEM((2, deep, lanes), jnp.float32),
            pltpu.VMEM((peers, 2, deep, lanes), jnp.float32),
            pltpu.SemaphoreType.REGULAR,
            sem((1,)),
            sem((len(fine) - 1,)),
            sem((peers,)),
            sem((2 if twin else 3, peers)),
            sem((3,)),
            sem((2,)),
        ],
        compiler_params=pltpu.CompilerParams(
            collective_id=1, has_side_effects=True, vmem_limit_bytes=8 * 2**20
        ),
    )(*in_vmem(edge, front, token))

    hbm = pl.BlockSpec(memory_space=pltpu.HBM)
    known = len(row_parts)
    return pl.pallas_call(
        functools.partial(write_last, lons),
        out_shape=(out, out),
        in_specs=[vmem] * known + [hbm] * 2,
        out_specs=[hbm] * 2,
        input_output_aliases={known: 0, known + 1: 1},
        scratch_shapes=[sem((2,))] + ([tile, tile, sem((2,))] if twin else []),
        compiler_params=pltpu.CompilerParams(vmem_limit_bytes=2**20),
    )(*in_vmem(*row_parts), out_scaled, out_dens)


VMEM_LIMIT = 44 * 2**20


def solution(mesh):
    lats, lons, levs = mesh.shape["lat"], mesh.shape["lon"], mesh.shape["lev"]

    def shards(density, crowding):
        rows, cols, deep, lanes = density.shape
        words = lanes * (
            STEPS * (rows + 1) * (cols + 2) * (deep + 2 * PAD)
            + 3 * rows * cols * deep
            + 2 * lons * rows * deep
        )
        fits = lats == 2 and rows > 1 and lanes == 128 and deep % 32 == 0 and 4 * words < VMEM_LIMIT
        if fits:
            return tuple(all_steps(lons, levs, density, crowding))
        return general(density, crowding)

    spec = P(("trial", "lat"), "lon", "lev", None)
    return jax.shard_map(
        shards, mesh=mesh, in_specs=(spec, spec), out_specs=(spec, spec), check_vma=False
    )
```

```python
import functools

import jax
import jax.numpy as jnp
from jax import lax
from jax.experimental import pallas as pl
from jax.experimental.pallas import tpu as pltpu
from jax.sharding import PartitionSpec as P

STEPS = 4
PAD = 8
MESH = pl.DeviceIdType.MESH


def with_halo(cells, sides, width):
    for axis, dim in sides:
        count = lax.axis_size(axis)
        ends = count - 1
        head = lax.slice_in_dim(cells, 0, width, axis=dim)
        tail = lax.slice_in_dim(cells, cells.shape[dim] - width, cells.shape[dim], axis=dim)
        cells = jnp.concatenate(
            [
                lax.ppermute(tail, axis, [(i, (i + 1) % count) for i in range(ends)]),
                cells,
                lax.ppermute(head, axis, [((i + 1) % count, i) for i in range(ends)]),
            ],
            axis=dim,
        )
    return cells


def inner_cells(values, dims):
    for dim in dims:
        values = lax.slice_in_dim(values, 1, values.shape[dim] - 1, axis=dim)
    return values


def side_cells(values, dim, start, dims):
    others = [other for other in dims if other != dim]
    values = inner_cells(values, others)
    return lax.slice_in_dim(values, start, start + values.shape[dim] - 2, axis=dim)


def advance(padded, crowding):
    middle = inner_cells(padded, (0, 1, 2))
    lower = [side_cells(padded, dim, 0, (0, 1, 2)) for dim in (0, 1, 2)]
    upper = [side_cells(padded, dim, 2, (0, 1, 2)) for dim in (0, 1, 2)]
    spread = lower[0] + upper[0] + lower[1] + upper[1] + lower[2] + upper[2] - 6.0 * middle
    return middle + 0.1 * spread + 0.2 * middle * (1.0 - middle * crowding)


def general(density, crowding):
    for step in range(STEPS):
        padded = with_halo(density, (("lat", 0), ("lon", 1), ("lev", 2)), 1)
        density = advance(padded, crowding)
    count = density.shape[1] * lax.axis_size("lon")
    moved = density - 1.0
    totals, squares = lax.psum(
        (jnp.sum(moved, axis=1, keepdims=True), jnp.sum(moved * moved, axis=1, keepdims=True)),
        "lon",
    )
    line_mean = 1.0 + totals / count
    centred = density - line_mean
    line_variance = squares / count - totals / count * (totals / count)
    return (centred * lax.rsqrt(line_variance + 0.0001), density)


def tree_sum(terms):
    terms = list(terms)
    while len(terms) > 1:
        terms = [sum(terms[i : i + 2][1:], terms[i]) for i in range(0, len(terms), 2)]
    return terms[0]


def signal(sem, where):
    pl.semaphore_signal(sem, inc=1, device_id=where, device_id_type=MESH)


def split(deep):
    half, last = deep // 2, deep - 8
    first, late = max(8, 5 * deep // 128 * 8), max(8, deep // 64 * 8)
    coarse = [(0, half), (half, half)]
    fine = [(0, first), (first, last - late - first), (last - late, late), (last, 8)]
    return coarse, fine


def place(r, rows):
    lat = lax.axis_index("lat")
    return (1 - lat) * (rows - r) + lat * (r - 1)


def tiles(first, many, act):
    def tile(i, _):
        act(pl.multiple_of(i * 8, 8))
        return 0
    lax.fori_loop(first // 8, (first + many) // 8, tile, 0)


def ahead(there, lon, lons):
    return there - lax.rem(there, 2) * lons < lon - lax.rem(lon, 2) * lons


def line_sums(values):
    cols = len(values)
    total = tree_sum(values)
    mean = total * (1.0 / cols)
    return total, tree_sum([(v - mean) * (v - mean) for v in values])


def line_scale(pair, cols):
    count = cols * len(pair)
    mean = tree_sum([p[0] for p in pair]) * (1.0 / count)
    square = tree_sum([p[1] + cols * (p[0] * (1.0 / cols) - mean) ** 2 for p in pair])
    return mean, lax.rsqrt(square * (1.0 / count) + 0.0001)


def kernel(lons, levs, dens, crowd, out_scaled, out_dens, edge, front,
           field, cap, stats, peers, entered, load_sem, face_send, face_recv,
           lon_send, lon_recv, lev_send, lev_recv, stat_send, stat_recv):
    rows, cols, deep, lanes = dens.shape
    coarse, fine = split(deep)
    lat, lon, lev = lax.axis_index("lat"), lax.axis_index("lon"), lax.axis_index("lev")
    has_left, has_right = lon > 0, lon < lons - 1
    has_down, has_up = lev > 0, lev < levs - 1
    late = lax.rem(lon, 2) == 0

    loads = [pltpu.make_async_copy(crowd, cap, load_sem.at[0])] + [
        pltpu.make_async_copy(
            dens.at[place(r, rows)],
            field.at[0, r, pl.ds(1, cols), pl.ds(PAD, deep)],
            load_sem.at[1])
        for r in range(1, rows + 1)
    ]
    all_rows = pltpu.make_async_copy(
        dens, field.at[0, pl.ds(1, rows), pl.ds(1, cols), pl.ds(PAD, deep)], load_sem.at[1])

    barrier = pltpu.get_barrier_semaphore()
    signal(barrier, {"lat": 1 - lat})
    before = 0
    for j in range(1, lons):
        there = lax.rem(lon + j, lons)
        before += ahead(there, lon, lons).astype(jnp.int32)
        pl.when(jnp.logical_not(ahead(there, lon, lons)))(lambda: signal(barrier, {"lon": there}))
    if levs > 1:
        pl.when(has_up)(lambda: signal(barrier, {"lev": lev + 1}))
    for copy in loads:
        copy.start()
    pl.semaphore_wait(barrier, 1 + before + has_down.astype(jnp.int32))

    def greet():
        for j in range(1, lons):
            there = lax.rem(lon + j, lons)
            pl.when(ahead(there, lon, lons))(lambda: signal(entered.at[0], {"lon": there}))
        if levs > 1:
            pl.when(has_down)(lambda: signal(entered.at[1], {"lev": lev - 1}))

    def wait_greeted():
        pl.when(before < lons - 1)(lambda: pl.semaphore_wait(entered.at[0], lons - 1 - before))
        if levs > 1:
            pl.when(has_up)(lambda: pl.semaphore_wait(entered.at[1], 1))

    def chunks(t):
        return fine if t == STEPS - 1 else coarse

    def face(t, k):
        at, span = chunks(t)[k]
        src = field.at[t, 1, pl.ds(1, cols), pl.ds(PAD + at, span)]
        if t == 0:
            src = dens.at[place(1, rows), :, pl.ds(at, span)]
        return pltpu.make_async_remote_copy(
            src_ref=src,
            dst_ref=field.at[t, 0, pl.ds(1, cols), pl.ds(PAD + at, span)],
            send_sem=face_send.at[k],
            recv_sem=face_recv.at[t % 2, k],
            device_id={"lat": 1 - lat},
            device_id_type=MESH,
        )

    bands = (pl.ds(1, 1), pl.ds(2, rows - 1))
    sent = []

    def way(count, forward):
        return int(forward) if count > 2 else 0

    def lon_side(t, band, right):
        own, theirs = (cols, 0) if right else (1, cols + 1)
        span = bands[band]
        return pltpu.make_async_remote_copy(
            src_ref=field.at[t, span, own, pl.ds(PAD, deep)],
            dst_ref=field.at[t, span, theirs, pl.ds(PAD, deep)],
            send_sem=lon_send.at[way(lons, right)],
            recv_sem=lon_recv.at[t % 2, band, way(lons, right)],
            device_id={"lon": lon + 1 if right else lon - 1},
            device_id_type=MESH,
        )

    def lev_side(t, band, up):
        own, theirs = (PAD + deep - 1, PAD - 1) if up else (PAD, PAD + deep)
        span = (bands[band], pl.ds(1, cols))
        return pltpu.make_async_remote_copy(
            src_ref=field.at[t, span[0], span[1], pl.ds(own, 1)],
            dst_ref=field.at[t, span[0], span[1], pl.ds(theirs, 1)],
            send_sem=lev_send.at[way(levs, up)],
            recv_sem=lev_recv.at[t % 2, band, way(levs, up)],
            device_id={"lev": lev + 1 if up else lev - 1},
            device_id_type=MESH,
        )

    def sides(t, band, act):
        if lons > 1:
            pl.when(has_right)(lambda: act(lon_side(t, band, True)))
            pl.when(has_left)(lambda: act(lon_side(t, band, False)))
        if levs > 1:
            pl.when(has_up)(lambda: act(lev_side(t, band, True)))
            pl.when(has_down)(lambda: act(lev_side(t, band, False)))

    def wait_sides_sent():
        if sent:
            sides(*sent.pop(), lambda copy: copy.wait_send())

    def start_sides(t, band):
        wait_sides_sent()
        sides(t, band, lambda copy: copy.start())
        sent.append((t, band))

    def wait_sides(t, band):
        if lons > 1:
            pl.when(has_left)(lambda: lon_side(t, band, True).wait_recv())
            pl.when(has_right)(lambda: lon_side(t, band, False).wait_recv())
        if levs > 1:
            pl.when(has_down)(lambda: lev_side(t, band, True).wait_recv())
            pl.when(has_up)(lambda: lev_side(t, band, False).wait_recv())

    stat_rows = (pl.ds(0, 1), pl.ds(1, rows - 2))

    def stat(group, j):
        return pltpu.make_async_remote_copy(
            src_ref=stats.at[stat_rows[group]],
            dst_ref=peers.at[j - 1, stat_rows[group]],
            send_sem=stat_send.at[j - 1],
            recv_sem=stat_recv.at[group, j - 1],
            device_id={"lon": lax.rem(lon + j, lons)},
            device_id_type=MESH,
        )

    for k in range(len(coarse)):
        face(0, k).start()
    greet()

    def clear_cols(at):
        for t in range(STEPS):
            def row(i, _, t=t):
                field[t, i, at, pl.ds(PAD, deep)] = jnp.zeros((deep, lanes), jnp.float32)
                return 0
            lax.fori_loop(1, rows + 1, row, 0)

    def clear_level(at):
        for t in range(STEPS):
            def row(i, _, t=t):
                def col(c, _):
                    field[t, i, c, pl.ds(at, PAD)] = jnp.zeros((PAD, lanes), jnp.float32)
                    return 0
                return lax.fori_loop(1, cols + 1, col, 0)
            lax.fori_loop(1, rows + 1, row, 0)

    pl.when(jnp.logical_not(has_left))(lambda: clear_cols(0))
    pl.when(jnp.logical_not(has_right))(lambda: clear_cols(cols + 1))
    pl.when(jnp.logical_not(has_down))(lambda: clear_level(0))
    pl.when(jnp.logical_not(has_up))(lambda: clear_level(PAD + deep))

    loads[0].wait()
    all_rows.wait()
    wait_greeted()
    start_sides(0, 1)
    start_sides(0, 0)

    def cell(t, r, c, at, span, below, above):
        here = field[t, r, c, pl.ds(PAD + at, span)]
        near = (field[t, r, c - 1, pl.ds(PAD + at, span)] + field[t, r, c + 1, pl.ds(PAD + at, span)])
        near += (field[t, r, c, pl.ds(PAD - 1 + at, span)] + field[t, r, c, pl.ds(PAD + 1 + at, span)])
        if below:
            near += field[t, r - 1, c, pl.ds(PAD + at, span)]
        if above:
            near += field[t, r + 1, c, pl.ds(PAD + at, span)]
        limit = cap[place(r, rows), c - 1, pl.ds(at, span)]
        return here * (0.6 - 0.2 * (here * limit)) + 0.1 * near

    def advance_row(t, r, at, span, last):
        def col(c, _):
            value = cell(t, r, c, at, span, True, not last)
            field[t + 1, r, c, pl.ds(PAD + at, span)] = value
            if t == STEPS - 2 and isinstance(r, int) and r == 1:
                front[c - 1, pl.ds(at, span)] = value
            return 0
        lax.fori_loop(1, cols + 1, col, 0)

    def start_face(t, k):
        def go():
            face(t - 1, k).wait_send()
            face(t, k).start()

        if t < STEPS - 1 or k == 0:
            go()
        elif k == 1:
            pl.when(late)(go)

    def finish(r, at, last):
        values = [cell(STEPS - 1, r, c, at, 8, True, not last) for c in range(1, cols + 1)]
        for c in range(cols):
            out_dens[r - 2, c, pl.ds(at, 8)] = values[c]
        total, square = line_sums(values)
        stats[r - 2, 0, pl.ds(at, 8)] = total
        stats[r - 2, 1, pl.ds(at, 8)] = square

    def scale(r, at):
        pair = [(stats[r - 2, 0, pl.ds(at, 8)], stats[r - 2, 1, pl.ds(at, 8)])]
        for j in range(lons - 1):
            pair.append((peers[j, r - 2, 0, pl.ds(at, 8)], peers[j, r - 2, 1, pl.ds(at, 8)]))
        mean, gain = line_scale(pair, cols)
        for c in range(cols):
            out_scaled[r - 2, c, pl.ds(at, 8)] = (out_dens[r - 2, c, pl.ds(at, 8)] - mean) * gain

    def each_row(first, last, act):
        def row(r, _):
            tiles(0, deep, lambda at: act(r, at))
            return 0
        lax.fori_loop(first, last, row, 0)

    def send_sums(group):
        for j in range(1, lons):
            if group == 0 and rows > 2:
                stat(1, j).wait_send()
            stat(group, j).start()

    def wait_sums(group):
        for j in range(1, lons):
            stat(group, j).wait_recv()

    for t in range(STEPS - 1):
        wait_sides(t, 1)

        def inner(r, _, t=t):
            advance_row(t, r, 0, deep, False)
            return 0

        lax.fori_loop(2, rows, inner, 0)
        advance_row(t, rows, 0, deep, True)
        start_sides(t + 1, 1)
        if t == STEPS - 2:
            wait_sides(t + 1, 1)
            if rows > 2:
                each_row(3, rows, lambda r, at: finish(r, at, False))
                tiles(0, deep, lambda at: finish(rows, at, True))
                send_sums(1)
                wait_sums(1)
                each_row(3, rows + 1, scale)
        wait_sides(t, 0)
        for k, (at, span) in enumerate(chunks(t)):
            face(t, k).wait_recv()
            advance_row(t, 1, at, span, False)
            for j, chunk in enumerate(chunks(t + 1)):
                if at < sum(chunk) <= at + span:
                    start_face(t + 1, j)
        start_sides(t + 1, 0)

    t = STEPS - 1
    tiles(0, deep, lambda at: finish(2, at, rows == 2))
    send_sums(0)
    wait_sides(t, 0)

    def base(c, _):
        edge[c - 1] = cell(t, 1, c, 0, deep, False, True)
        return 0

    lax.fori_loop(1, cols + 1, base, 0)
    wait_sums(0)
    tiles(0, deep, lambda at: scale(2, at))

    def add_face(k):
        at, span = fine[k]
        face(t, k).wait_recv()

        def col(c, _):
            edge[c, pl.ds(at, span)] += 0.1 * field[t, 0, c + 1, pl.ds(PAD + at, span)]
            return 0
        lax.fori_loop(0, cols, col, 0)

    wait_sides_sent()
    for j in range(1, lons):
        stat(0, j).wait_send()
    pl.when(jnp.logical_not(late))(lambda: face(t - 1, 1).wait_send())
    add_face(0)
    face(t, 0).wait_send()

    @pl.when(late)
    def _():
        add_face(1)
        face(t, 1).wait_send()


def write_inner(scaled, dens, edge, out_scaled, out_dens, token, sems):
    inner, cols, _, _ = scaled.shape
    waits = [pltpu.make_async_copy(edge, out_dens.at[place(1, inner + 1)], sems.at[2])]
    waits[0].start()
    for i, (src, dst) in enumerate(((scaled, out_scaled), (dens, out_dens))):
        for r in range(inner):
            pltpu.make_async_copy(src.at[r], dst.at[place(r + 2, inner + 1)], sems.at[i]).start()
        waits.append(pltpu.make_async_copy(src, dst.at[pl.ds(0, inner)], sems.at[i]))
    token[...] = jnp.zeros(token.shape, jnp.float32)
    for copy in waits:
        copy.wait()


def last_row(lons, edge, front, token, out_scaled, out_dens, *refs):
    twin = lons == 2
    tile_base, tile_face, tile_sums = refs[:3] if twin else (None,) * 3
    (other, stats, peers, entered, face_send, face_recv, stat_send, stat_recv,
     tile_send, tile_recv) = refs[3:] if twin else refs
    cols, deep, lanes = edge.shape
    _, fine = split(deep)
    end = len(fine) - 1
    spans = [(0, sum(fine[1]))] + fine[2:]
    tail = pl.ds(*fine[end])
    lat, lon = lax.axis_index("lat"), lax.axis_index("lon")
    late = lax.rem(lon, 2) == 0
    early = jnp.logical_not(late)

    barrier = pltpu.get_barrier_semaphore()
    signal(barrier, {"lat": 1 - lat})
    before = 0
    for j in range(1, lons):
        there = lax.rem(lon + j, lons)
        before += ahead(there, lon, lons).astype(jnp.int32)

        @pl.when(jnp.logical_not(ahead(there, lon, lons)))
        def _():
            signal(barrier, {"lon": there})
            if twin:
                signal(barrier, {"lat": 1 - lat, "lon": there})
    pl.semaphore_wait(barrier, 1 + before * (2 if twin else 1))

    def remote(src, dst, send, recv, where):
        return pltpu.make_async_remote_copy(
            src_ref=src, dst_ref=dst, send_sem=send, recv_sem=recv,
            device_id=where, device_id_type=MESH)

    def face(k):
        pick = (slice(None), pl.ds(*fine[k]))
        return remote(front.at[pick], other.at[pick], face_send.at[0], face_recv.at[k - 1],
                      {"lat": 1 - lat})

    def wait_faces_sent(k, stop):
        at = fine[k][0]
        pick = (slice(None), pl.ds(at, sum(fine[stop]) - at))
        remote(front.at[pick], other.at[pick], face_send.at[0], face_recv.at[k - 1],
               {"lat": 1 - lat}).wait_send()

    def tile_copy(i):
        src = (front, front, edge, stats)[i].at[:, tail]
        dst = (tile_face, tile_face, tile_base, tile_sums)[i]
        where = {"lat": 1 - lat} if i < 2 else {}
        if i > 0:
            where["lon"] = 1 - lon
        return remote(src, dst, tile_send.at[0], tile_recv.at[i // 2], where)

    def stat(part, j):
        pick = (slice(None), pl.ds(*spans[part]))
        return remote(stats.at[pick], peers.at[(j - 1,) + pick],
                      stat_send.at[j - 1], stat_recv.at[part, j - 1],
                      {"lon": lax.rem(lon + j, lons)})

    def each_stat(part, act):
        for j in range(1, lons):
            act(stat(part, j))

    @pl.when(early)
    def _():
        for k in range(1, end + 1):
            face(k).start()

    @pl.when(late)
    def _():
        for k in range(2, end if twin else end + 1):
            face(k).start()
        if twin:
            for i in (2, 0, 1):
                tile_copy(i).start()

    for j in range(1, lons):
        there = lax.rem(lon + j, lons)
        pl.when(ahead(there, lon, lons))(lambda: signal(entered, {"lon": there}))

    def finish(at, add):
        values = [edge[c, pl.ds(at, 8)] for c in range(cols)]
        if add:
            values = [v + 0.1 * other[c, pl.ds(at, 8)] for c, v in enumerate(values)]
        for c in range(cols):
            out_dens[c, pl.ds(at, 8)] = values[c]
        total, square = line_sums(values)
        stats[0, pl.ds(at, 8)] = total
        stats[1, pl.ds(at, 8)] = square

    def scale(at):
        pair = [(stats[0, pl.ds(at, 8)], stats[1, pl.ds(at, 8)])]
        for j in range(lons - 1):
            pair.append((peers[j, 0, pl.ds(at, 8)], peers[j, 1, pl.ds(at, 8)]))
        mean, gain = line_scale(pair, cols)
        for c in range(cols):
            out_scaled[c, pl.ds(at, 8)] = (out_dens[c, pl.ds(at, 8)] - mean) * gain

    def land(k):
        face(k).wait_recv()
        tiles(*fine[k], lambda at: finish(at, True))

    tiles(*fine[0], lambda at: finish(at, False))
    pl.when(late)(lambda: tiles(*fine[1], lambda at: finish(at, False)))
    pl.when(early)(lambda: land(1))
    pl.when(before < lons - 1)(lambda: pl.semaphore_wait(entered, lons - 1 - before))
    each_stat(0, lambda copy: copy.start())
    land(2)
    each_stat(0, lambda copy: copy.wait_send())
    each_stat(1, lambda copy: copy.start())
    each_stat(0, lambda copy: copy.wait_recv())
    tiles(*spans[0], scale)
    if twin:
        @pl.when(early)
        def _():
            land(end)
            tile_copy(3).start()
            tile_sums[...] = stats[:, tail]
    else:
        land(end)
        each_stat(1, lambda copy: copy.wait_send())
        each_stat(2, lambda copy: copy.start())
    each_stat(1, lambda copy: copy.wait_recv())
    tiles(*spans[1], scale)

    pl.when(early)(lambda: wait_faces_sent(1, end))
    pl.when(late)(lambda: wait_faces_sent(2, end - 1 if twin else end))
    if twin:
        each_stat(1, lambda copy: copy.wait_send())

        @pl.when(early)
        def _():
            tile_copy(3).wait_send()
            tile_copy(2).wait_recv()
            tile_copy(1).wait_recv()

        @pl.when(late)
        def _():
            tile_base[...] = edge[:, tail]
            pick = (slice(None), pl.ds(0, 24))
            remote(front.at[pick], other.at[pick], tile_send.at[0], tile_recv.at[0],
                   {"lat": 1 - lat}).wait_send()
            tile_copy(3).wait_recv()
            tile_copy(0).wait_recv()
    else:
        each_stat(2, lambda copy: copy.wait_recv())
        tiles(*spans[2], scale)
        each_stat(2, lambda copy: copy.wait_send())


def write_last(lons, scaled, dens, *refs):
    twin = lons == 2
    if twin:
        tile_base, tile_face, tile_sums, _, _, out_scaled, out_dens, sems = refs[:8]
        own_scaled, own_dens = refs[8:]
    else:
        _, _, out_scaled, out_dens, sems = refs
    rows = out_dens.shape[0]
    cols, deep, _ = dens.shape
    _, fine = split(deep)
    last = fine[-1][0]
    late = 1 - lax.rem(lax.axis_index("lon"), 2)

    def copy(src, dst, i, begin, end):
        span = pl.ds(begin, end - begin)
        return pltpu.make_async_copy(
            src.at[:, span], dst.at[place(1, rows), :, span], sems.at[i])

    def each(act, stop):
        act(copy(scaled, out_scaled, 0, 0, stop))
        for moved in range(2):
            @pl.when(late == moved)
            def _():
                act(copy(dens, out_dens, 1, sum(fine[moved]), stop if moved else deep))

    def tile_out(i):
        src, dst = ((own_scaled, out_scaled), (own_dens, out_dens))[i]
        return pltpu.make_async_copy(
            src, dst.at[place(1, rows), :, pl.ds(last, 8)], sems.at[i])

    each(lambda copy: copy.start(), last if twin else deep)
    if twin:
        values = [tile_base[c] + 0.1 * tile_face[c] for c in range(cols)]
        mean, gain = line_scale([line_sums(values), (tile_sums[0], tile_sums[1])], cols)

        @pl.when(late == 1)
        def _():
            for c in range(cols):
                own_dens[c] = values[c]
                own_scaled[c] = (values[c] - mean) * gain
            tile_out(1).start()

        @pl.when(late == 0)
        def _():
            for c in range(cols):
                own_scaled[c] = (dens[c, pl.ds(last, 8)] - mean) * gain

        tile_out(0).start()
    each(lambda copy: copy.wait(), deep)


def in_vmem(*arrays):
    return [pltpu.with_memory_space_constraint(a, pltpu.VMEM) for a in arrays]


def all_steps(lons, levs, density, crowding):
    rows, cols, deep, lanes = density.shape
    coarse, fine = split(deep)
    sem = pltpu.SemaphoreType.DMA
    peers = max(lons - 1, 1)
    inner = pltpu.VMEM((rows - 1, cols, deep, lanes), jnp.float32)
    row = pltpu.VMEM((cols, deep, lanes), jnp.float32)
    any_space = pl.BlockSpec(memory_space=pl.ANY)
    vmem = pl.BlockSpec(memory_space=pltpu.VMEM)
    scaled, dens, edge, front = pl.pallas_call(
        functools.partial(kernel, lons, levs),
        out_shape=(inner, inner, row, row),
        in_specs=[any_space] * 2,
        out_specs=[vmem] * 4,
        scratch_shapes=[
            pltpu.VMEM((STEPS, rows + 1, cols + 2, deep + 2 * PAD, lanes), jnp.float32),
            pltpu.VMEM((rows, cols, deep, lanes), jnp.float32),
            pltpu.VMEM((rows - 1, 2, deep, lanes), jnp.float32),
            pltpu.VMEM((peers, rows - 1, 2, deep, lanes), jnp.float32),
            pltpu.SemaphoreType.REGULAR((2,)),
            sem((2,)),
            sem((len(coarse),)),
            sem((2, len(coarse))),
            sem((2 if lons > 2 else 1,)),
            sem((2, 2, 2 if lons > 2 else 1)),
            sem((2 if levs > 2 else 1,)),
            sem((2, 2, 2 if levs > 2 else 1)),
            sem((peers,)),
            sem((2, peers)),
        ],
        compiler_params=pltpu.CompilerParams(
            collective_id=0, has_side_effects=True, vmem_limit_bytes=VMEM_LIMIT
        ),
    )(density, crowding)

    out = jax.ShapeDtypeStruct(density.shape, density.dtype)
    out_scaled, out_dens, token = pl.pallas_call(
        write_inner,
        out_shape=(out, out, pltpu.VMEM((8, lanes), jnp.float32)),
        in_specs=[vmem] * 3,
        out_specs=[pl.BlockSpec(memory_space=pltpu.HBM)] * 2 + [vmem],
        scratch_shapes=[sem((3,))],
        compiler_params=pltpu.CompilerParams(vmem_limit_bytes=2**20),
    )(*in_vmem(scaled, dens, edge))

    twin = lons == 2
    tile = pltpu.VMEM((cols, 8, lanes), jnp.float32)
    extra = (tile, tile, pltpu.VMEM((2, 8, lanes), jnp.float32)) if twin else ()
    row_parts = pl.pallas_call(
        functools.partial(last_row, lons),
        out_shape=(row, row) + extra,
        in_specs=[vmem] * 3,
        out_specs=[vmem] * (2 + len(extra)),
        scratch_shapes=[
            pltpu.VMEM((cols, deep, lanes), jnp.float32),
            pltpu.VMEM((2, deep, lanes), jnp.float32),
            pltpu.VMEM((peers, 2, deep, lanes), jnp.float32),
            pltpu.SemaphoreType.REGULAR,
            sem((1,)),
            sem((len(fine) - 1,)),
            sem((peers,)),
            sem((2 if twin else 3, peers)),
            sem((1,)),
            sem((2,)),
        ],
        compiler_params=pltpu.CompilerParams(
            collective_id=1, has_side_effects=True, vmem_limit_bytes=8 * 2**20
        ),
    )(*in_vmem(edge, front, token))

    hbm = pl.BlockSpec(memory_space=pltpu.HBM)
    known = len(row_parts)
    return pl.pallas_call(
        functools.partial(write_last, lons),
        out_shape=(out, out),
        in_specs=[vmem] * known + [hbm] * 2,
        out_specs=[hbm] * 2,
        input_output_aliases={known: 0, known + 1: 1},
        scratch_shapes=[sem((2,))] + ([tile, tile] if twin else []),
        compiler_params=pltpu.CompilerParams(vmem_limit_bytes=2**20),
    )(*in_vmem(*row_parts), out_scaled, out_dens)


VMEM_LIMIT = 44 * 2**20


def solution(mesh):
    lats, lons, levs = mesh.shape["lat"], mesh.shape["lon"], mesh.shape["lev"]

    def shards(density, crowding):
        rows, cols, deep, lanes = density.shape
        words = lanes * (
            STEPS * (rows + 1) * (cols + 2) * (deep + 2 * PAD)
            + 3 * rows * cols * deep
            + 2 * lons * rows * deep
        )
        fits = lats == 2 and rows > 1 and lanes == 128 and deep % 32 == 0 and 4 * words < VMEM_LIMIT
        if fits:
            return tuple(all_steps(lons, levs, density, crowding))
        return general(density, crowding)

    spec = P(("trial", "lat"), "lon", "lev", None)
    return jax.shard_map(
        shards, mesh=mesh, in_specs=(spec, spec), out_specs=(spec, spec), check_vma=False
    )
```

```python
import functools

import jax
import jax.numpy as jnp
from jax import lax
from jax.experimental import pallas as pl
from jax.experimental.pallas import tpu as pltpu
from jax.sharding import PartitionSpec as P

STEPS = 4
PAD = 8
MESH = pl.DeviceIdType.MESH


def with_halo(cells, sides, width):
    for axis, dim in sides:
        count = lax.axis_size(axis)
        ends = count - 1
        head = lax.slice_in_dim(cells, 0, width, axis=dim)
        tail = lax.slice_in_dim(cells, cells.shape[dim] - width, cells.shape[dim], axis=dim)
        cells = jnp.concatenate(
            [
                lax.ppermute(tail, axis, [(i, (i + 1) % count) for i in range(ends)]),
                cells,
                lax.ppermute(head, axis, [((i + 1) % count, i) for i in range(ends)]),
            ],
            axis=dim,
        )
    return cells


def inner_cells(values, dims):
    for dim in dims:
        values = lax.slice_in_dim(values, 1, values.shape[dim] - 1, axis=dim)
    return values


def side_cells(values, dim, start, dims):
    others = [other for other in dims if other != dim]
    values = inner_cells(values, others)
    return lax.slice_in_dim(values, start, start + values.shape[dim] - 2, axis=dim)


def advance(padded, crowding):
    middle = inner_cells(padded, (0, 1, 2))
    lower = [side_cells(padded, dim, 0, (0, 1, 2)) for dim in (0, 1, 2)]
    upper = [side_cells(padded, dim, 2, (0, 1, 2)) for dim in (0, 1, 2)]
    spread = lower[0] + upper[0] + lower[1] + upper[1] + lower[2] + upper[2] - 6.0 * middle
    return middle + 0.1 * spread + 0.2 * middle * (1.0 - middle * crowding)


def general(density, crowding):
    for step in range(STEPS):
        padded = with_halo(density, (("lat", 0), ("lon", 1), ("lev", 2)), 1)
        density = advance(padded, crowding)
    count = density.shape[1] * lax.axis_size("lon")
    moved = density - 1.0
    totals, squares = lax.psum(
        (jnp.sum(moved, axis=1, keepdims=True), jnp.sum(moved * moved, axis=1, keepdims=True)),
        "lon",
    )
    line_mean = 1.0 + totals / count
    centred = density - line_mean
    line_variance = squares / count - totals / count * (totals / count)
    return (centred * lax.rsqrt(line_variance + 0.0001), density)


def tree_sum(terms):
    terms = list(terms)
    while len(terms) > 1:
        terms = [sum(terms[i : i + 2][1:], terms[i]) for i in range(0, len(terms), 2)]
    return terms[0]


def signal(sem, where):
    pl.semaphore_signal(sem, inc=1, device_id=where, device_id_type=MESH)


def split(deep):
    half, last = deep // 2, deep - 8
    first, late = max(8, 5 * deep // 128 * 8), max(8, deep // 64 * 8)
    coarse = [(0, half), (half, half)]
    fine = [(0, first), (first, last - late - first), (last - late, late), (last, 8)]
    return coarse, fine


def place(r, rows):
    lat = lax.axis_index("lat")
    return (1 - lat) * (rows - r) + lat * (r - 1)


def tiles(first, many, act):
    def tile(i, _):
        act(pl.multiple_of(i * 8, 8))
        return 0
    lax.fori_loop(first // 8, (first + many) // 8, tile, 0)


def ahead(there, lon, lons):
    return there - lax.rem(there, 2) * lons < lon - lax.rem(lon, 2) * lons


def line_sums(values):
    cols = len(values)
    total = tree_sum(values)
    mean = total * (1.0 / cols)
    return total, tree_sum([(v - mean) * (v - mean) for v in values])


def line_scale(pair, cols):
    count = cols * len(pair)
    mean = tree_sum([p[0] for p in pair]) * (1.0 / count)
    square = tree_sum([p[1] + cols * (p[0] * (1.0 / cols) - mean) ** 2 for p in pair])
    return mean, lax.rsqrt(square * (1.0 / count) + 0.0001)


def kernel(lons, levs, dens, crowd, out_scaled, out_dens, edge, front,
           field, cap, stats, peers, entered, load_sem, face_send, face_recv,
           lon_send, lon_recv, lev_send, lev_recv, stat_send, stat_recv):
    rows, cols, deep, lanes = dens.shape
    coarse, fine = split(deep)
    lat, lon, lev = lax.axis_index("lat"), lax.axis_index("lon"), lax.axis_index("lev")
    has_left, has_right = lon > 0, lon < lons - 1
    has_down, has_up = lev > 0, lev < levs - 1
    late = lax.rem(lon, 2) == 0

    loads = [pltpu.make_async_copy(crowd, cap, load_sem.at[0])] + [
        pltpu.make_async_copy(
            dens.at[place(r, rows)],
            field.at[0, r, pl.ds(1, cols), pl.ds(PAD, deep)],
            load_sem.at[1])
        for r in range(1, rows + 1)
    ]
    all_rows = pltpu.make_async_copy(
        dens, field.at[0, pl.ds(1, rows), pl.ds(1, cols), pl.ds(PAD, deep)], load_sem.at[1])

    barrier = pltpu.get_barrier_semaphore()
    signal(barrier, {"lat": 1 - lat})
    before = 0
    for j in range(1, lons):
        there = lax.rem(lon + j, lons)
        before += ahead(there, lon, lons).astype(jnp.int32)
        pl.when(jnp.logical_not(ahead(there, lon, lons)))(lambda: signal(barrier, {"lon": there}))
    if levs > 1:
        pl.when(has_up)(lambda: signal(barrier, {"lev": lev + 1}))
    for copy in loads:
        copy.start()
    pl.semaphore_wait(barrier, 1 + before + has_down.astype(jnp.int32))

    def greet():
        for j in range(1, lons):
            there = lax.rem(lon + j, lons)
            pl.when(ahead(there, lon, lons))(lambda: signal(entered.at[0], {"lon": there}))
        if levs > 1:
            pl.when(has_down)(lambda: signal(entered.at[1], {"lev": lev - 1}))

    def wait_greeted():
        pl.when(before < lons - 1)(lambda: pl.semaphore_wait(entered.at[0], lons - 1 - before))
        if levs > 1:
            pl.when(has_up)(lambda: pl.semaphore_wait(entered.at[1], 1))

    def chunks(t):
        return fine if t == STEPS - 1 else coarse

    def face(t, k):
        at, span = chunks(t)[k]
        src = field.at[t, 1, pl.ds(1, cols), pl.ds(PAD + at, span)]
        if t == 0:
            src = dens.at[place(1, rows), :, pl.ds(at, span)]
        return pltpu.make_async_remote_copy(
            src_ref=src,
            dst_ref=field.at[t, 0, pl.ds(1, cols), pl.ds(PAD + at, span)],
            send_sem=face_send.at[k],
            recv_sem=face_recv.at[t % 2, k],
            device_id={"lat": 1 - lat},
            device_id_type=MESH,
        )

    bands = (pl.ds(1, 1), pl.ds(2, rows - 1))
    sent = []

    def way(count, forward):
        return int(forward) if count > 2 else 0

    def lon_side(t, band, right):
        own, theirs = (cols, 0) if right else (1, cols + 1)
        span = bands[band]
        return pltpu.make_async_remote_copy(
            src_ref=field.at[t, span, own, pl.ds(PAD, deep)],
            dst_ref=field.at[t, span, theirs, pl.ds(PAD, deep)],
            send_sem=lon_send.at[way(lons, right)],
            recv_sem=lon_recv.at[t % 2, band, way(lons, right)],
            device_id={"lon": lon + 1 if right else lon - 1},
            device_id_type=MESH,
        )

    def lev_side(t, band, up):
        own, theirs = (PAD + deep - 1, PAD - 1) if up else (PAD, PAD + deep)
        span = (bands[band], pl.ds(1, cols))
        return pltpu.make_async_remote_copy(
            src_ref=field.at[t, span[0], span[1], pl.ds(own, 1)],
            dst_ref=field.at[t, span[0], span[1], pl.ds(theirs, 1)],
            send_sem=lev_send.at[way(levs, up)],
            recv_sem=lev_recv.at[t % 2, band, way(levs, up)],
            device_id={"lev": lev + 1 if up else lev - 1},
            device_id_type=MESH,
        )

    def sides(t, band, act):
        if lons > 1:
            pl.when(has_right)(lambda: act(lon_side(t, band, True)))
            pl.when(has_left)(lambda: act(lon_side(t, band, False)))
        if levs > 1:
            pl.when(has_up)(lambda: act(lev_side(t, band, True)))
            pl.when(has_down)(lambda: act(lev_side(t, band, False)))

    def wait_sides_sent():
        if sent:
            sides(*sent.pop(), lambda copy: copy.wait_send())

    def start_sides(t, band):
        wait_sides_sent()
        sides(t, band, lambda copy: copy.start())
        sent.append((t, band))

    def wait_sides(t, band):
        if lons > 1:
            pl.when(has_left)(lambda: lon_side(t, band, True).wait_recv())
            pl.when(has_right)(lambda: lon_side(t, band, False).wait_recv())
        if levs > 1:
            pl.when(has_down)(lambda: lev_side(t, band, True).wait_recv())
            pl.when(has_up)(lambda: lev_side(t, band, False).wait_recv())

    stat_rows = (pl.ds(0, 1), pl.ds(1, rows - 2))

    def stat(group, j):
        return pltpu.make_async_remote_copy(
            src_ref=stats.at[stat_rows[group]],
            dst_ref=peers.at[j - 1, stat_rows[group]],
            send_sem=stat_send.at[j - 1],
            recv_sem=stat_recv.at[group, j - 1],
            device_id={"lon": lax.rem(lon + j, lons)},
            device_id_type=MESH,
        )

    for k in range(len(coarse)):
        face(0, k).start()
    greet()

    def clear_cols(at):
        for t in range(STEPS):
            def row(i, _, t=t):
                field[t, i, at, pl.ds(PAD, deep)] = jnp.zeros((deep, lanes), jnp.float32)
                return 0
            lax.fori_loop(1, rows + 1, row, 0)

    def clear_level(at):
        for t in range(STEPS):
            def row(i, _, t=t):
                def col(c, _):
                    field[t, i, c, pl.ds(at, PAD)] = jnp.zeros((PAD, lanes), jnp.float32)
                    return 0
                return lax.fori_loop(1, cols + 1, col, 0)
            lax.fori_loop(1, rows + 1, row, 0)

    pl.when(jnp.logical_not(has_left))(lambda: clear_cols(0))
    pl.when(jnp.logical_not(has_right))(lambda: clear_cols(cols + 1))
    pl.when(jnp.logical_not(has_down))(lambda: clear_level(0))
    pl.when(jnp.logical_not(has_up))(lambda: clear_level(PAD + deep))

    loads[0].wait()
    all_rows.wait()
    wait_greeted()
    start_sides(0, 1)
    start_sides(0, 0)

    def cell(t, r, c, at, span, below, above):
        here = field[t, r, c, pl.ds(PAD + at, span)]
        near = (field[t, r, c - 1, pl.ds(PAD + at, span)] + field[t, r, c + 1, pl.ds(PAD + at, span)])
        near += (field[t, r, c, pl.ds(PAD - 1 + at, span)] + field[t, r, c, pl.ds(PAD + 1 + at, span)])
        if below:
            near += field[t, r - 1, c, pl.ds(PAD + at, span)]
        if above:
            near += field[t, r + 1, c, pl.ds(PAD + at, span)]
        limit = cap[place(r, rows), c - 1, pl.ds(at, span)]
        return here * (0.6 - 0.2 * (here * limit)) + 0.1 * near

    def advance_row(t, r, at, span, last):
        def col(c, _):
            value = cell(t, r, c, at, span, True, not last)
            field[t + 1, r, c, pl.ds(PAD + at, span)] = value
            if t == STEPS - 2 and isinstance(r, int) and r == 1:
                front[c - 1, pl.ds(at, span)] = value
            return 0
        lax.fori_loop(1, cols + 1, col, 0)

    def start_face(t, k):
        def go():
            face(t - 1, k).wait_send()
            face(t, k).start()

        if t < STEPS - 1 or k == 0:
            go()
        elif k == 1:
            pl.when(late)(go)

    def finish(r, at, last):
        values = [cell(STEPS - 1, r, c, at, 8, True, not last) for c in range(1, cols + 1)]
        for c in range(cols):
            out_dens[r - 2, c, pl.ds(at, 8)] = values[c]
        total, square = line_sums(values)
        stats[r - 2, 0, pl.ds(at, 8)] = total
        stats[r - 2, 1, pl.ds(at, 8)] = square

    def scale(r, at):
        pair = [(stats[r - 2, 0, pl.ds(at, 8)], stats[r - 2, 1, pl.ds(at, 8)])]
        for j in range(lons - 1):
            pair.append((peers[j, r - 2, 0, pl.ds(at, 8)], peers[j, r - 2, 1, pl.ds(at, 8)]))
        mean, gain = line_scale(pair, cols)
        for c in range(cols):
            out_scaled[r - 2, c, pl.ds(at, 8)] = (out_dens[r - 2, c, pl.ds(at, 8)] - mean) * gain

    def each_row(first, last, act):
        def row(r, _):
            tiles(0, deep, lambda at: act(r, at))
            return 0
        lax.fori_loop(first, last, row, 0)

    def send_sums(group):
        for j in range(1, lons):
            if group == 0 and rows > 2:
                stat(1, j).wait_send()
            stat(group, j).start()

    def wait_sums(group):
        for j in range(1, lons):
            stat(group, j).wait_recv()

    for t in range(STEPS - 1):
        wait_sides(t, 1)

        def inner(r, _, t=t):
            advance_row(t, r, 0, deep, False)
            return 0

        lax.fori_loop(2, rows, inner, 0)
        advance_row(t, rows, 0, deep, True)
        start_sides(t + 1, 1)
        if t == STEPS - 2:
            wait_sides(t + 1, 1)
            if rows > 2:
                each_row(3, rows, lambda r, at: finish(r, at, False))
                tiles(0, deep, lambda at: finish(rows, at, True))
                send_sums(1)
                wait_sums(1)
                each_row(3, rows + 1, scale)
        wait_sides(t, 0)
        for k, (at, span) in enumerate(chunks(t)):
            face(t, k).wait_recv()
            advance_row(t, 1, at, span, False)
            for j, chunk in enumerate(chunks(t + 1)):
                if at < sum(chunk) <= at + span:
                    start_face(t + 1, j)
        start_sides(t + 1, 0)

    t = STEPS - 1
    tiles(0, deep, lambda at: finish(2, at, rows == 2))
    send_sums(0)
    wait_sides(t, 0)

    def base(c, _):
        edge[c - 1] = cell(t, 1, c, 0, deep, False, True)
        return 0

    lax.fori_loop(1, cols + 1, base, 0)
    wait_sums(0)
    tiles(0, deep, lambda at: scale(2, at))

    def add_face(k):
        at, span = fine[k]
        face(t, k).wait_recv()

        def col(c, _):
            edge[c, pl.ds(at, span)] += 0.1 * field[t, 0, c + 1, pl.ds(PAD + at, span)]
            return 0
        lax.fori_loop(0, cols, col, 0)

    wait_sides_sent()
    pl.when(jnp.logical_not(late))(lambda: face(t - 1, 1).wait_send())
    add_face(0)
    for j in range(1, lons):
        stat(0, j).wait_send()
    face(t, 0).wait_send()

    @pl.when(late)
    def _():
        add_face(1)
        face(t, 1).wait_send()


def write_inner(scaled, dens, edge, out_scaled, out_dens, token, sems):
    inner, cols, _, _ = scaled.shape
    waits = [pltpu.make_async_copy(edge, out_dens.at[place(1, inner + 1)], sems.at[2])]
    waits[0].start()
    for i, (src, dst) in enumerate(((scaled, out_scaled), (dens, out_dens))):
        for r in range(inner):
            pltpu.make_async_copy(src.at[r], dst.at[place(r + 2, inner + 1)], sems.at[i]).start()
        waits.append(pltpu.make_async_copy(src, dst.at[pl.ds(0, inner)], sems.at[i]))
    token[...] = jnp.zeros(token.shape, jnp.float32)
    for copy in waits:
        copy.wait()


def last_row(lons, edge, front, token, out_scaled, out_dens, *refs):
    twin = lons == 2
    tile_base, tile_face, tile_sums = refs[:3] if twin else (None,) * 3
    (other, stats, peers, entered, face_send, face_recv, stat_send, stat_recv,
     tile_send, tile_recv) = refs[3:] if twin else refs
    cols, deep, lanes = edge.shape
    _, fine = split(deep)
    end = len(fine) - 1
    spans = [(0, sum(fine[1]))] + fine[2:]
    tail = pl.ds(*fine[end])
    lat, lon = lax.axis_index("lat"), lax.axis_index("lon")
    late = lax.rem(lon, 2) == 0
    early = jnp.logical_not(late)

    barrier = pltpu.get_barrier_semaphore()
    signal(barrier, {"lat": 1 - lat})
    before = 0
    for j in range(1, lons):
        there = lax.rem(lon + j, lons)
        before += ahead(there, lon, lons).astype(jnp.int32)

        @pl.when(jnp.logical_not(ahead(there, lon, lons)))
        def _():
            signal(barrier, {"lon": there})
            if twin:
                signal(barrier, {"lat": 1 - lat, "lon": there})
    pl.semaphore_wait(barrier, 1 + before * (2 if twin else 1))

    def remote(src, dst, send, recv, where):
        return pltpu.make_async_remote_copy(
            src_ref=src, dst_ref=dst, send_sem=send, recv_sem=recv,
            device_id=where, device_id_type=MESH)

    def face(k):
        pick = (slice(None), pl.ds(*fine[k]))
        return remote(front.at[pick], other.at[pick], face_send.at[0], face_recv.at[k - 1],
                      {"lat": 1 - lat})

    def wait_faces_sent(k, stop):
        at = fine[k][0]
        pick = (slice(None), pl.ds(at, sum(fine[stop]) - at))
        remote(front.at[pick], other.at[pick], face_send.at[0], face_recv.at[k - 1],
               {"lat": 1 - lat}).wait_send()

    def tile_copy(i):
        src = (front, front, edge, stats)[i].at[:, tail]
        dst = (tile_face, tile_face, tile_base, tile_sums)[i]
        where = {"lat": 1 - lat} if i < 2 else {}
        if i > 0:
            where["lon"] = 1 - lon
        return remote(src, dst, tile_send.at[0], tile_recv.at[i // 2], where)

    def stat(part, j):
        pick = (slice(None), pl.ds(*spans[part]))
        return remote(stats.at[pick], peers.at[(j - 1,) + pick],
                      stat_send.at[j - 1], stat_recv.at[part, j - 1],
                      {"lon": lax.rem(lon + j, lons)})

    def each_stat(part, act):
        for j in range(1, lons):
            act(stat(part, j))

    @pl.when(early)
    def _():
        for k in range(1, end + 1):
            face(k).start()

    @pl.when(late)
    def _():
        for k in range(2, end if twin else end + 1):
            face(k).start()
        if twin:
            for i in (0, 1, 2):
                tile_copy(i).start()

    for j in range(1, lons):
        there = lax.rem(lon + j, lons)
        pl.when(ahead(there, lon, lons))(lambda: signal(entered, {"lon": there}))

    def finish(at, add):
        values = [edge[c, pl.ds(at, 8)] for c in range(cols)]
        if add:
            values = [v + 0.1 * other[c, pl.ds(at, 8)] for c, v in enumerate(values)]
        for c in range(cols):
            out_dens[c, pl.ds(at, 8)] = values[c]
        total, square = line_sums(values)
        stats[0, pl.ds(at, 8)] = total
        stats[1, pl.ds(at, 8)] = square

    def scale(at):
        pair = [(stats[0, pl.ds(at, 8)], stats[1, pl.ds(at, 8)])]
        for j in range(lons - 1):
            pair.append((peers[j, 0, pl.ds(at, 8)], peers[j, 1, pl.ds(at, 8)]))
        mean, gain = line_scale(pair, cols)
        for c in range(cols):
            out_scaled[c, pl.ds(at, 8)] = (out_dens[c, pl.ds(at, 8)] - mean) * gain

    def land(k):
        face(k).wait_recv()
        tiles(*fine[k], lambda at: finish(at, True))

    tiles(*fine[0], lambda at: finish(at, False))
    pl.when(late)(lambda: tiles(*fine[1], lambda at: finish(at, False)))
    pl.when(early)(lambda: land(1))
    pl.when(before < lons - 1)(lambda: pl.semaphore_wait(entered, lons - 1 - before))
    each_stat(0, lambda copy: copy.start())
    land(2)
    each_stat(0, lambda copy: copy.wait_send())
    each_stat(1, lambda copy: copy.start())
    each_stat(0, lambda copy: copy.wait_recv())
    tiles(*spans[0], scale)
    if twin:
        @pl.when(early)
        def _():
            land(end)
            tile_copy(3).start()
            tile_sums[...] = stats[:, tail]
    else:
        land(end)
        each_stat(1, lambda copy: copy.wait_send())
        each_stat(2, lambda copy: copy.start())
    each_stat(1, lambda copy: copy.wait_recv())
    tiles(*spans[1], scale)

    pl.when(early)(lambda: wait_faces_sent(1, end))
    pl.when(late)(lambda: wait_faces_sent(2, end - 1 if twin else end))
    if twin:
        each_stat(1, lambda copy: copy.wait_send())

        @pl.when(early)
        def _():
            tile_copy(3).wait_send()
            tile_copy(2).wait_recv()
            tile_copy(1).wait_recv()

        @pl.when(late)
        def _():
            tile_base[...] = edge[:, tail]
            pick = (slice(None), pl.ds(0, 24))
            remote(front.at[pick], other.at[pick], tile_send.at[0], tile_recv.at[0],
                   {"lat": 1 - lat}).wait_send()
            tile_copy(3).wait_recv()
            tile_copy(0).wait_recv()
    else:
        each_stat(2, lambda copy: copy.wait_recv())
        tiles(*spans[2], scale)
        each_stat(2, lambda copy: copy.wait_send())


def write_last(lons, scaled, dens, *refs):
    twin = lons == 2
    if twin:
        tile_base, tile_face, tile_sums, _, _, out_scaled, out_dens, sems = refs[:8]
        own_scaled, own_dens = refs[8:]
    else:
        _, _, out_scaled, out_dens, sems = refs
    rows = out_dens.shape[0]
    cols, deep, _ = dens.shape
    _, fine = split(deep)
    last = fine[-1][0]
    late = 1 - lax.rem(lax.axis_index("lon"), 2)

    def copy(src, dst, i, begin, end):
        span = pl.ds(begin, end - begin)
        return pltpu.make_async_copy(
            src.at[:, span], dst.at[place(1, rows), :, span], sems.at[i])

    def each(act, stop):
        act(copy(scaled, out_scaled, 0, 0, stop))
        for moved in range(2):
            @pl.when(late == moved)
            def _():
                act(copy(dens, out_dens, 1, sum(fine[moved]), stop if moved else deep))

    def tile_out(i):
        src, dst = ((own_scaled, out_scaled), (own_dens, out_dens))[i]
        return pltpu.make_async_copy(
            src, dst.at[place(1, rows), :, pl.ds(last, 8)], sems.at[i])

    each(lambda copy: copy.start(), last if twin else deep)
    if twin:
        values = [tile_base[c] + 0.1 * tile_face[c] for c in range(cols)]
        mean, gain = line_scale([line_sums(values), (tile_sums[0], tile_sums[1])], cols)

        @pl.when(late == 1)
        def _():
            for c in range(cols):
                own_dens[c] = values[c]
                own_scaled[c] = (values[c] - mean) * gain
            tile_out(1).start()

        @pl.when(late == 0)
        def _():
            for c in range(cols):
                own_scaled[c] = (dens[c, pl.ds(last, 8)] - mean) * gain

        tile_out(0).start()
    each(lambda copy: copy.wait(), deep)


def in_vmem(*arrays):
    return [pltpu.with_memory_space_constraint(a, pltpu.VMEM) for a in arrays]


def all_steps(lons, levs, density, crowding):
    rows, cols, deep, lanes = density.shape
    coarse, fine = split(deep)
    sem = pltpu.SemaphoreType.DMA
    peers = max(lons - 1, 1)
    inner = pltpu.VMEM((rows - 1, cols, deep, lanes), jnp.float32)
    row = pltpu.VMEM((cols, deep, lanes), jnp.float32)
    any_space = pl.BlockSpec(memory_space=pl.ANY)
    vmem = pl.BlockSpec(memory_space=pltpu.VMEM)
    scaled, dens, edge, front = pl.pallas_call(
        functools.partial(kernel, lons, levs),
        out_shape=(inner, inner, row, row),
        in_specs=[any_space] * 2,
        out_specs=[vmem] * 4,
        scratch_shapes=[
            pltpu.VMEM((STEPS, rows + 1, cols + 2, deep + 2 * PAD, lanes), jnp.float32),
            pltpu.VMEM((rows, cols, deep, lanes), jnp.float32),
            pltpu.VMEM((rows - 1, 2, deep, lanes), jnp.float32),
            pltpu.VMEM((peers, rows - 1, 2, deep, lanes), jnp.float32),
            pltpu.SemaphoreType.REGULAR((2,)),
            sem((2,)),
            sem((len(coarse),)),
            sem((2, len(coarse))),
            sem((2 if lons > 2 else 1,)),
            sem((2, 2, 2 if lons > 2 else 1)),
            sem((2 if levs > 2 else 1,)),
            sem((2, 2, 2 if levs > 2 else 1)),
            sem((peers,)),
            sem((2, peers)),
        ],
        compiler_params=pltpu.CompilerParams(
            collective_id=0, has_side_effects=True, vmem_limit_bytes=VMEM_LIMIT
        ),
    )(density, crowding)

    out = jax.ShapeDtypeStruct(density.shape, density.dtype)
    out_scaled, out_dens, token = pl.pallas_call(
        write_inner,
        out_shape=(out, out, pltpu.VMEM((8, lanes), jnp.float32)),
        in_specs=[vmem] * 3,
        out_specs=[pl.BlockSpec(memory_space=pltpu.HBM)] * 2 + [vmem],
        scratch_shapes=[sem((3,))],
        compiler_params=pltpu.CompilerParams(vmem_limit_bytes=2**20),
    )(*in_vmem(scaled, dens, edge))

    twin = lons == 2
    tile = pltpu.VMEM((cols, 8, lanes), jnp.float32)
    extra = (tile, tile, pltpu.VMEM((2, 8, lanes), jnp.float32)) if twin else ()
    row_parts = pl.pallas_call(
        functools.partial(last_row, lons),
        out_shape=(row, row) + extra,
        in_specs=[vmem] * 3,
        out_specs=[vmem] * (2 + len(extra)),
        scratch_shapes=[
            pltpu.VMEM((cols, deep, lanes), jnp.float32),
            pltpu.VMEM((2, deep, lanes), jnp.float32),
            pltpu.VMEM((peers, 2, deep, lanes), jnp.float32),
            pltpu.SemaphoreType.REGULAR,
            sem((1,)),
            sem((len(fine) - 1,)),
            sem((peers,)),
            sem((2 if twin else 3, peers)),
            sem((1,)),
            sem((2,)),
        ],
        compiler_params=pltpu.CompilerParams(
            collective_id=1, has_side_effects=True, vmem_limit_bytes=8 * 2**20
        ),
    )(*in_vmem(edge, front, token))

    hbm = pl.BlockSpec(memory_space=pltpu.HBM)
    known = len(row_parts)
    return pl.pallas_call(
        functools.partial(write_last, lons),
        out_shape=(out, out),
        in_specs=[vmem] * known + [hbm] * 2,
        out_specs=[hbm] * 2,
        input_output_aliases={known: 0, known + 1: 1},
        scratch_shapes=[sem((2,))] + ([tile, tile] if twin else []),
        compiler_params=pltpu.CompilerParams(vmem_limit_bytes=2**20),
    )(*in_vmem(*row_parts), out_scaled, out_dens)


VMEM_LIMIT = 44 * 2**20


def solution(mesh):
    lats, lons, levs = mesh.shape["lat"], mesh.shape["lon"], mesh.shape["lev"]

    def shards(density, crowding):
        rows, cols, deep, lanes = density.shape
        words = lanes * (
            STEPS * (rows + 1) * (cols + 2) * (deep + 2 * PAD)
            + 3 * rows * cols * deep
            + 2 * lons * rows * deep
        )
        fits = lats == 2 and rows > 1 and lanes == 128 and deep % 32 == 0 and 4 * words < VMEM_LIMIT
        if fits:
            return tuple(all_steps(lons, levs, density, crowding))
        return general(density, crowding)

    spec = P(("trial", "lat"), "lon", "lev", None)
    return jax.shard_map(
        shards, mesh=mesh, in_specs=(spec, spec), out_specs=(spec, spec), check_vma=False
    )
```
